32 devices in a mesh: gx: 4 (over z), gy: 4 (over y, x), gz: 2 (over core).
Axes of the slice: x: 2, y: 2, z: 4, core: 2. Of those that a mesh axis runs over, the one named last changes fastest.
Arguments:
- positions: float32 [3, 64, 64, 512], P(None, 'gx', 'gy', 'gz'), may hold values from -6 to 6
- pair_node: int32 [4, 4, 2, 32, 256], P('gx', 'gy', 'gz'), may hold values from 0 to 255
- pair_line: int32 [4, 4, 2, 32], P('gx', 'gy', 'gz'), may hold values from 0 to 255
- pair_far: int32 [4, 4, 2, 32, 256], P('gx', 'gy', 'gz'), may hold values from 0 to 261, as said below
- far_line: int32 [4, 4, 2, 32], P('gx', 'gy', 'gz'), may hold values from 0 to 483, as said below
- pair_geom: float32 [4, 4, 2, 32, 4, 256], P('gx', 'gy', 'gz'), may hold values from -4 to 4
- live_blocks: int32 [4, 4, 2], P('gx', 'gy', 'gz'), may hold values from 8 to 32, as said below
Outputs:
- corrected: float32 [3, 64, 64, 512], P(None, 'gx', 'gy', 'gz')
- sweep_history: float32 [2, 5], replicated
The draws below stay inside these ranges and needn't reach their ends.
Inputs may be any that keep to these rules, and one draw needn't show every extreme that they name: `pair_far`: together with far_line: at most one of the three coordinates of node b lies outside the owner block's own nodes; node b lies inside the whole grid; in slots below 16 node b is one of the owner block's own nodes. `far_line`: together with pair_far, as stated there. `live_blocks`: some owner block has all 32 slots live.
All inputs are finite; a program needn't handle non-finite values.
Results may differ from the reference program's by a relative error of at most 0.0001.
Values sent between devices are 32-bit elements; how exact they have to be, the bound alone decides.
A program may use at most 64 MiB of HBM per device.

```python
import jax
import jax.numpy as jnp
from jax import lax

CX = 16
CY = 16
CZ = 256
BLOCKS = 32
PAIRS_BLK = 256
RIM = 3
SWEEPS = 5
NX = 64
NY = 64
NZ = 512
PAIRS_ALL = 262144
N_GX = 4
N_GY = 4
N_GZ = 2


def far_layout(key):
    grid_x = NX // CX
    grid_y = NY // CY
    grid_z = NZ // CZ
    block_shape = (grid_x, grid_y, grid_z, BLOCKS)
    full_shape = (grid_x, grid_y, grid_z, BLOCKS, PAIRS_BLK)
    subkeys = jax.random.split(jax.random.fold_in(key, 7117), 8)
    line_x = jax.random.randint(subkeys[0], block_shape, RIM, CX + RIM)
    line_y = jax.random.randint(subkeys[1], block_shape, RIM, CY + RIM)
    coord_z = jax.random.randint(subkeys[2], full_shape, RIM, CZ + RIM)
    face_axis = jax.random.randint(subkeys[3], block_shape, 0, 3)
    high_block = jax.random.randint(subkeys[4], block_shape, 0, 2)
    layer_block = jax.random.randint(subkeys[5], block_shape, 0, RIM)
    high_pair = jax.random.randint(subkeys[6], full_shape, 0, 2)
    layer_pair = jax.random.randint(subkeys[7], full_shape, 0, RIM)
    rim_slot = lax.broadcasted_iota(jnp.int32, block_shape, 3) >= BLOCKS // 2

    def rim_coord(shape, axis_dim, extent, blocks_along, high_face, rim_layer):
        block_pos = lax.broadcasted_iota(jnp.int32, shape, axis_dim)
        low_side = jnp.where(block_pos == 0, RIM + rim_layer, rim_layer)
        high_side = jnp.where(block_pos == blocks_along - 1, extent + RIM - 1 - rim_layer, extent + RIM + rim_layer)
        return jnp.where(high_face == 1, high_side, low_side)
    line_x = jnp.where(rim_slot & (face_axis == 0), rim_coord(block_shape, 0, CX, grid_x, high_block, layer_block), line_x)
    line_y = jnp.where(rim_slot & (face_axis == 1), rim_coord(block_shape, 1, CY, grid_y, high_block, layer_block), line_y)
    z_face = (rim_slot & (face_axis == 2))[:, :, :, :, None]
    coord_z = jnp.where(z_face, rim_coord(full_shape, 2, CZ, grid_z, high_pair, layer_pair), coord_z)
    return ((line_x * (CY + 2 * RIM) + line_y).astype(jnp.int32), coord_z.astype(jnp.int32))


def draw_pair_far(key, part):
    return far_layout(key)[1]


def draw_far_line(key, part):
    return far_layout(key)[0]


def draw_live_blocks(key, part):
    grid_x = NX // CX
    grid_y = NY // CY
    grid_z = NZ // CZ
    full_shape = (grid_x, grid_y, grid_z)
    subkeys = jax.random.split(key, 3)
    base_count = jax.random.randint(subkeys[0], full_shape, BLOCKS // 4, BLOCKS // 2 + 1)
    heavy_dev = jax.random.randint(subkeys[1], full_shape, 0, 8) == 0
    chosen = jax.random.randint(subkeys[2], (), 0, grid_x * grid_y * grid_z)
    linear = (lax.broadcasted_iota(jnp.int32, full_shape, 0) * grid_y + lax.broadcasted_iota(jnp.int32, full_shape, 1)) * grid_z + lax.broadcasted_iota(jnp.int32, full_shape, 2)
    return jnp.where(heavy_dev | (linear == chosen), BLOCKS, base_count).astype(jnp.int32)


def set_ends(drawn, own_key, low, top_value):
    longest = drawn.shape.index(max(drawn.shape))
    spots = []
    for shift in (0, 1):
        where = [jax.random.randint(jax.random.fold_in(own_key, axis), (), 0, length) for axis, length in enumerate(drawn.shape)]
        where[longest] = (where[longest] + shift) % drawn.shape[longest]
        spots.append(tuple(where))
    return drawn.at[spots[0]].set(low).at[spots[1]].set(top_value)


def shard_levels(stream_key, dims, cuts, least, top_value):
    level = 1.0
    for dim, shards_of in cuts:
        steps = jax.random.uniform(jax.random.fold_in(jax.random.fold_in(stream_key, 6), dim), (shards_of,), jnp.float32, least / len(cuts), top_value / len(cuts))
        level = level * jnp.repeat(jnp.exp(steps), dims[dim] // shards_of).reshape((-1,) + (1,) * (len(dims) - 1 - dim))
    return level


def centred(own_key, shape, width, most, cuts=(), kind=jnp.bfloat16):
    gain = shard_levels(own_key, shape, cuts, -0.22, 0.18) if cuts else 1.0
    drawn = jax.random.normal(own_key, shape, jnp.float32) * width * gain
    return jnp.minimum(jnp.maximum(drawn, -most), most).astype(kind)


def setup_inputs(seed: int = 0) -> dict:
    seeds = jax.random.split(jax.random.key(seed), 8)
    return {
        "positions": centred(seeds[0], (3, NX, NY, NZ), 1.0, 6.0, ((1, 4), (2, 4), (3, 2)), jnp.float32),
        "pair_node": set_ends(jax.random.randint(seeds[1], (N_GX, N_GY, N_GZ, BLOCKS, PAIRS_BLK), 0, CZ), jax.random.fold_in(seeds[1], 1), 0, CZ - 1).astype(jnp.int32),
        "pair_line": set_ends(jax.random.randint(seeds[2], (N_GX, N_GY, N_GZ, BLOCKS), 0, CX * CY), jax.random.fold_in(seeds[2], 1), 0, (CX * CY) - 1).astype(jnp.int32),
        "pair_far": draw_pair_far(jax.random.fold_in(seeds[7], 71), 0),
        "far_line": draw_far_line(jax.random.fold_in(seeds[7], 71), 0),
        "pair_geom": centred(seeds[5], (N_GX, N_GY, N_GZ, BLOCKS, 4, PAIRS_BLK), 0.6, 4.0, ((0, 4), (1, 4), (2, 2)), jnp.float32),
        "live_blocks": draw_live_blocks(jax.random.fold_in(seeds[7], 71), 0),
    }


relax_factor = 0.9

def reference(positions, pair_node, pair_line, pair_far, far_line, pair_geom, live_blocks):
    full_shape = pair_node.shape
    block_x = lax.broadcasted_iota(jnp.int32, full_shape, 0)
    block_y = lax.broadcasted_iota(jnp.int32, full_shape, 1)
    block_z = lax.broadcasted_iota(jnp.int32, full_shape, 2)
    slot_index = lax.broadcasted_iota(jnp.int32, full_shape, 3)
    line_full = jnp.broadcast_to(pair_line[:, :, :, :, None], full_shape)
    node_x = block_x * CX + line_full // CY
    node_y = block_y * CY + line_full % CY
    node_z = block_z * CZ + pair_node
    own_flat = ((node_x * NY + node_y) * NZ + node_z).reshape(-1).astype(jnp.int32)
    ext_y = CY + 2 * RIM
    far_full = jnp.broadcast_to(far_line[:, :, :, :, None], full_shape)
    far_x = far_full // ext_y
    far_y = far_full % ext_y
    far_z = pair_far
    pad_y = NY + 2 * RIM
    pad_z = NZ + 2 * RIM
    far_flat = (((block_x * CX + far_x) * pad_y + block_y * CY + far_y) * pad_z + block_z * CZ + far_z).reshape(-1).astype(jnp.int32)
    live_mask = (slot_index < live_blocks[:, :, :, None, None]).reshape(-1)
    geometry = jnp.moveaxis(pair_geom, 4, 0).reshape(4, -1)
    node_count = NX * NY * NZ
    live_ones = jnp.where(live_mask, 1.0, 0.0).astype(jnp.float32)
    counts = jnp.zeros((node_count,), jnp.float32).at[own_flat].add(live_ones)
    current = positions.reshape(3, -1)
    energies = []
    residuals = []
    for sweep_idx in range(SWEEPS):
        padded = jnp.pad(current.reshape(3, NX, NY, NZ), ((0, 0), (RIM, RIM), (RIM, RIM), (RIM, RIM))).reshape(3, -1)
        differ = current[:, own_flat] - padded[:, far_flat]
        gap_value = lax.optimization_barrier(jnp.sum(geometry[0:3] * differ, axis=0)) - geometry[3]
        depth_value = jnp.where(live_mask, jnp.maximum(-gap_value, 0.0), 0.0)
        energy = jnp.sum(depth_value * depth_value)
        node_total = jnp.zeros((3, node_count), jnp.float32).at[:, own_flat].add(depth_value[None, :] * geometry[0:3])
        scale_factor = 1.0 / (1.0 + energy / PAIRS_ALL)
        correction = relax_factor * scale_factor * node_total / (1.0 + counts)
        current = current + correction
        residuals.append(jnp.sum(correction * correction))
        energies.append(energy)
    history = jnp.stack([jnp.sqrt(1.0 + jnp.stack(energies) / (PAIRS_BLK * BLOCKS)), jnp.sqrt(1.0 + jnp.stack(residuals) / (CX * CY * CZ))])
    return (current.reshape(3, NX, NY, NZ), history)
```

```python
import functools

import jax
import jax.numpy as jnp
from jax import lax
from jax.experimental import pallas as pl
from jax.experimental.pallas import tpu as pltpu
from jax.sharding import PartitionSpec as P

RIM = 3
SWEEPS = 5
RELAX = 0.9
AXES = ("gx", "gy", "gz")
MESH = pl.DeviceIdType.MESH
f32 = jnp.float32
bf16 = jnp.bfloat16


def split(x, parts):
    out = []
    for _ in range(parts - 1):
        hi = x.astype(bf16)
        out.append(hi)
        x = x - hi.astype(f32)
    out.append(x.astype(bf16))
    return out


def mm(a, b):
    return jnp.dot(a, b, preferred_element_type=f32)


def take_lanes(x, low, half):
    outs = []
    for h in range(0, low.shape[1], 128):
        idx = low[:, h : h + 128]
        got = jnp.take_along_axis(x[:, :128], idx, axis=1, mode="promise_in_bounds")
        for j in range(1, x.shape[1] // 128):
            more = jnp.take_along_axis(
                x[:, 128 * j : 128 * (j + 1)], idx, axis=1, mode="promise_in_bounds"
            )
            got = jnp.where(half[:, h : h + 128] == j, more, got)
        outs.append(got)
    return jnp.concatenate(outs, axis=1)


def kernel(
    sizes,
    blk,
    live_hbm,
    node_hbm,
    line_hbm,
    farpos_hbm,
    farline_hbm,
    geom_hbm,
    pos_hbm,
    acc_ref,
    hist_ref,
    live_ref,
    node_ref,
    line_ref,
    farpos_ref,
    farline_ref,
    geom_ref,
    pos_ref,
    req,
    cols,
    hot,
    two,
    amat,
    cinv,
    geo,
    low_ref,
    half_ref,
    gap,
    wcat,
    reqs,
    dsend,
    drecv,
    erecv,
    rrecv,
    in_sem,
    plane_sem,
    whole_sem,
    qs_sem,
    qr_sem,
    ds_sem,
    dr_sem,
    es_sem,
    er_sem,
    rs_sem,
    rr_sem,
):
    nx, ny, nz = sizes
    bx, by, bz = blk
    devices = nx * ny * nz
    blocks, pairs = gap.shape
    outer = blocks // 2
    lines = bx * by
    me = [lax.axis_index(a) for a in AXES]
    mine = (me[0] * ny + me[1]) * nz + me[2]
    dirs = [(a, s) for a in (1, 0, 2) for s in (1, -1)]

    def neighbour(axis, sign):
        to = list(me)
        to[axis] = lax.rem(me[axis] + sign + sizes[axis], sizes[axis])
        return tuple(to)

    def exists(axis, sign):
        return (me[axis] + sign >= 0) & (me[axis] + sign < sizes[axis])

    def coords(k):
        to = lax.rem(mine + k, devices)
        return (to // (ny * nz), lax.rem(to // nz, ny), lax.rem(to, nz))

    def moved_by(axis, k):
        to = me[axis] + k
        return jnp.where(to >= sizes[axis], to - sizes[axis], to) if k else to

    ids = [[moved_by(a, k) for k in range(sizes[a])] for a in range(3)]

    def signal_line(sem, axis):
        for k in range(1, sizes[axis]):
            to = list(me)
            to[axis] = ids[axis][k]
            pl.semaphore_signal(sem, inc=1, device_id=tuple(to), device_id_type=MESH)

    barrier = pltpu.get_barrier_semaphore()
    for axis in range(3):
        signal_line(barrier, axis)
    inputs = [
        pltpu.make_async_copy(src, dst, in_sem.at[i])
        for i, (src, dst) in enumerate(
            [
                (farline_hbm, farline_ref),
                (farpos_hbm, farpos_ref),
                (geom_hbm, geom_ref),
                (node_hbm, node_ref),
                (line_hbm, line_ref),
                (live_hbm, live_ref),
                (pos_hbm, pos_ref),
            ]
        )
    ]
    for copy in inputs:
        copy.start()
    for copy in inputs[:3]:
        copy.wait()

    def column(ref):
        row = ref[0, 0].astype(f32)
        return jnp.transpose(jnp.broadcast_to(row, (pairs, blocks)))

    wide = pairs // 128
    planes = [geom_ref[0, 0, 0, outer:, c, :] for c in range(3)]
    planes.append(farpos_ref[0, 0, 0, outer:, :].astype(f32))
    for c in range(4):
        for h in range(wide):
            req[c * wide + h] = planes[c][:, 128 * h : 128 * (h + 1)]
    cols[1] = column(farline_ref)
    req[4 * wide] = cols[1, outer:, :128]

    def ask(d, axis, sign):
        return pltpu.make_async_remote_copy(
            src_ref=req,
            dst_ref=reqs.at[d],
            send_sem=qs_sem.at[d],
            recv_sem=qr_sem.at[d],
            device_id=neighbour(axis, sign),
            device_id_type=MESH,
        )

    pl.semaphore_wait(barrier, sum(sizes) - 3)
    for d, (axis, sign) in enumerate(dirs):

        @pl.when(exists(axis, sign))
        def _():
            ask(d, axis, sign).start()

    signal_line(plane_sem, 0)
    for copy in inputs[3:6]:
        copy.wait()
    cols[0] = column(line_ref)

    for d, (axis, sign) in enumerate(dirs):

        @pl.when(jnp.logical_not(exists(axis, -sign)))
        def _():
            reqs[d] = jnp.zeros(req.shape, f32)

        @pl.when(jnp.logical_not(exists(axis, sign)))
        def _():
            for t in range(SWEEPS):
                drecv[t, d] = jnp.zeros((outer, pairs), f32)

    live = jnp.broadcast_to(live_ref[0], (blocks, pairs))
    live_rows = lax.broadcasted_iota(jnp.int32, (blocks, pairs), 0) < live
    lane_node = lax.broadcasted_iota(jnp.int32, (pairs, bz), 1).astype(f32)
    node_t = jnp.transpose(node_ref[0, 0, 0].astype(f32))
    for b in range(blocks):
        hot[pl.ds(b * pairs, pairs), :] = jnp.where(
            node_t[:, b : b + 1] == lane_node, 1.0, 0.0
        ).astype(bf16)
    row_line = line_ref[0, 0].astype(f32)
    two[...] = jnp.concatenate([row_line, row_line], axis=1)
    row_mod = lax.broadcasted_iota(jnp.int32, (blocks, blocks), 0)
    col_mod = lax.broadcasted_iota(jnp.int32, (blocks, blocks), 1)
    line_b = cols[0]
    same = line_b[:, :blocks] == row_line
    first_col = 1.0 - jnp.max(
        jnp.where(same & (col_mod < row_mod), 1.0, 0.0), axis=1, keepdims=True
    )

    def expand(stack, step):
        rows = stack.shape[0]
        which = lax.rem(lax.broadcasted_iota(jnp.int32, (rows, pairs), 0), step)
        return jnp.concatenate(
            [jnp.where(which == j, stack, 0.0).astype(bf16) for j in range(step)], axis=1
        )

    counts = []
    for g in range(blocks // 8):
        ones = jnp.where(live_rows[8 * g : 8 * g + 8], 1.0, 0.0)
        counts.append(mm(expand(ones, 8), hot[pl.ds(8 * g * pairs, 8 * pairs), :]))
    counts = jnp.concatenate(counts, axis=0).astype(bf16)

    def located(code, zpos, shift):
        e = jnp.floor((code + 0.5) / (by + 2 * RIM))
        f = code - e * (by + 2 * RIM)
        e = e - (RIM + shift[0] * bx)
        f = f - (RIM + shift[1] * by)
        z = zpos - (RIM + shift[2] * bz)
        ok_line = (e >= 0) & (e < bx) & (f >= 0) & (f < by)
        return jnp.where(ok_line, e * by + f, -1.0), z, ok_line & (z >= 0) & (z < bz)

    def setup(row, line, node, geom):
        n = line.shape[0]
        lane_line = lax.broadcasted_iota(jnp.int32, (n, lines), 1).astype(f32)
        a = jnp.where(line[:, : 2 * blocks] == two[...], 1.0, 0.0).astype(bf16)
        amat[pl.ds(row, n), :] = a
        cinv[pl.ds(row, n), :] = RELAX / (1.0 + mm(a[:, :blocks], counts))
        idx = node.astype(jnp.int32)
        low = lax.bitwise_and(idx, 127)
        half = lax.shift_right_logical(idx, 7)
        low_ref[pl.ds(row, n), :] = low
        half_ref[pl.ds(row, n), :] = half
        own = jnp.where(line == lane_line, 1.0, 0.0).astype(bf16)
        total = jnp.zeros((n, pairs), f32)
        for c in range(3):
            geo[c, pl.ds(row, n), :] = geom[c]
            vals = jnp.zeros((n, bz), f32)
            for part in split(pos_ref[c].reshape(lines, bz), 3):
                vals += mm(own, part)
            total += geom[c] * take_lanes(vals, low, half)
        return total

    def cat(parts):
        return jnp.concatenate(parts, axis=0)

    inputs[6].wait()
    for d, (axis, sign) in enumerate(dirs):

        @pl.when(exists(axis, -sign))
        def _():
            ask(d, axis, sign).wait_recv()

    if nx > 1:
        pl.semaphore_wait(plane_sem, nx - 1)
    signal_line(whole_sem, 2)
    asked = []
    for d, (axis, sign) in enumerate(dirs):
        shift = [0, 0, 0]
        shift[axis] = sign
        got = [
            jnp.concatenate([reqs[d, c * wide + h] for h in range(wide)], axis=1) for c in range(4)
        ]
        code = jnp.concatenate([reqs[d, 4 * wide]] * wide, axis=1)
        line, z, ok = located(code, got[3], shift)
        asked.append(
            [line, jnp.where(ok, z, 0.0)] + [jnp.where(ok, -got[c], 0.0) for c in range(3)]
        )
    asked = [cat([x[i] for x in asked]) for i in range(5)]
    base = asked[0].shape[0]
    rows = base + 2 * blocks

    def respond(t, total):
        for d, (axis, sign) in enumerate(dirs):
            dsend[t, d] = total[d * outer : (d + 1) * outer]
        for d, (axis, sign) in enumerate(dirs):

            @pl.when(exists(axis, -sign))
            def _():
                answer(t, d, axis, sign).start()

    def answer(t, d, axis, sign):
        return pltpu.make_async_remote_copy(
            src_ref=dsend.at[t, d],
            dst_ref=drecv.at[t, d],
            send_sem=ds_sem.at[t, d],
            recv_sem=dr_sem.at[t, d],
            device_id=neighbour(axis, -sign),
            device_id_type=MESH,
        )

    def received(t):
        for d, (axis, sign) in enumerate(dirs):

            @pl.when(exists(axis, sign))
            def _():
                answer(t, d, axis, sign).wait_recv()

        got = drecv[t, 0]
        for d in range(1, len(dirs)):
            got = got + drecv[t, d]
        return got

    respond(0, setup(0, asked[0], asked[1], asked[2:]))

    line, z, ok = located(cols[1], farpos_ref[0, 0, 0].astype(f32), (0, 0, 0))
    geom = [geom_ref[0, 0, 0, :, c, :] for c in range(4)]
    start = setup(
        base,
        cat([line_b, line]),
        cat([node_ref[0, 0, 0].astype(f32), jnp.where(ok, z, 0.0)]),
        [cat([geom[c], jnp.where(ok, -geom[c], 0.0)]) for c in range(3)],
    )
    start = start[:blocks] + start[blocks:] - geom[3]
    if nz > 1:
        pl.semaphore_wait(whole_sem, nz - 1)
    gap[0:outer, :] = start[:outer]
    gap[pl.ds(outer, outer), :] = start[outer:] + received(0)
    acc_ref[...] = jnp.zeros_like(acc_ref)

    def to_all(ref, send_sem, recv_sem):
        def send(to):
            pltpu.make_async_remote_copy(
                src_ref=ref,
                dst_ref=ref,
                send_sem=send_sem,
                recv_sem=recv_sem,
                device_id=to,
                device_id_type=MESH,
            ).start()

        if devices <= 32:
            for a in range(nx):
                for b in range(ny):
                    for c in range(nz):
                        if a or b or c:
                            send((ids[0][a], ids[1][b], ids[2][c]))
        else:

            def step(k, carry):
                send(coords(k))
                return carry

            lax.fori_loop(1, devices, step, 0)

    def lanes_sum(x):
        x = jnp.sum(x, axis=0, keepdims=True)
        out = x[:, :128]
        for j in range(1, x.shape[1] // 128):
            out = out + x[:, 128 * j : 128 * (j + 1)]
        return out

    lane = lax.broadcasted_iota(jnp.int32, (1, 128), 1)

    def apply(row, n, parts):
        both = mm(amat[row : row + n, :], parts)
        return [both[:, c * bz : (c + 1) * bz] * cinv[row : row + n, :] for c in range(3)]

    def dots(row, n, moved):
        low = low_ref[row : row + n, :]
        half = half_ref[row : row + n, :]
        total = geo[0, row : row + n] * take_lanes(moved[0], low, half)
        for c in range(1, 3):
            total += geo[c, row : row + n] * take_lanes(moved[c], low, half)
        return total

    def sweep(t, last):
        depth = jnp.where(live_rows, jnp.maximum(-gap[...], 0.0), 0.0)
        squares = lanes_sum(depth * depth)
        erecv[t, mine] = squares
        to_all(erecv.at[t, mine], es_sem.at[t], er_sem.at[t])
        for g in range(blocks // 8):
            lo, hi = 8 * g, 8 * g + 8
            terms = cat([depth[lo:hi] * geo[c, base + lo : base + hi] for c in range(3)])
            top = terms.astype(bf16).astype(f32)
            sums = mm(expand(cat([top, terms - top]), 8), hot[pl.ds(lo * pairs, 8 * pairs), :])
            sums = sums[:24] + sums[24:]
            for c in range(3):
                wcat[lo:hi, c * bz : (c + 1) * bz] = sums[8 * c : 8 * c + 8]
        parts = cat(split(wcat[...], 2))
        if not last:
            respond(t + 1, dots(0, base, apply(0, base, parts)))
        moved = apply(base, blocks if last else 2 * blocks, parts)
        near = jnp.concatenate([m[:blocks] for m in moved], axis=1)
        resid = jnp.sum(lanes_sum(near * near * first_col), axis=1, keepdims=True)
        rrecv[mine] = jnp.where(lane == t, resid, rrecv[mine])
        if last:
            to_all(rrecv.at[mine], rs_sem, rr_sem)
        else:
            step = dots(base, 2 * blocks, moved)
            step = step[:blocks] + step[blocks:]
        others = erecv.at[t, pl.ds(0, devices - 1)]
        pltpu.make_async_copy(others, others, er_sem.at[t]).wait()
        energy = jnp.sum(jnp.sum(erecv[t], axis=0), axis=1, keepdims=True)
        scale = 1.0 / (1.0 + energy / (blocks * pairs * devices))
        hist_ref[0:1, :] = jnp.where(lane == t, energy, hist_ref[0:1, :])
        hist_ref[1:2, :] = jnp.where(lane == t, scale, hist_ref[1:2, :])
        acc_ref[...] = acc_ref[...] + (scale * first_col) * near
        if not last:
            more = received(t + 1)
            gap[0:outer, :] = gap[0:outer, :] + scale * step[:outer]
            gap[pl.ds(outer, outer), :] = gap[pl.ds(outer, outer), :] + scale * (
                step[outer:] + more
            )

    rrecv[mine] = jnp.zeros((1, 128), f32)
    hist_ref[...] = jnp.zeros_like(hist_ref)

    def body(t, carry):
        sweep(t, False)
        return carry

    lax.fori_loop(0, SWEEPS - 1, body, 0)
    sweep(SWEEPS - 1, True)

    for d, (axis, sign) in enumerate(dirs):

        @pl.when(exists(axis, sign))
        def _():
            ask(d, axis, sign).wait_send()

        @pl.when(exists(axis, -sign))
        def _():
            for t in range(SWEEPS):
                answer(t, d, axis, sign).wait_send()

    others = rrecv.at[pl.ds(0, devices - 1)]
    pltpu.make_async_copy(others, others, rr_sem).wait()
    for t in range(SWEEPS):
        ref = erecv.at[t, pl.ds(0, devices - 1)]
        pltpu.make_async_copy(ref, ref, es_sem.at[t]).wait()
    others = rrecv.at[pl.ds(0, devices - 1)]
    pltpu.make_async_copy(others, others, rs_sem).wait()
    energy, scale = hist_ref[0:1, :], hist_ref[1:2, :]
    resid = jnp.sum(rrecv[...], axis=0)
    hist_ref[0:1, :] = jnp.sqrt(1.0 + energy / (blocks * pairs))
    hist_ref[1:2, :] = jnp.sqrt(1.0 + scale * scale * resid / (bx * by * bz))


def finish(acc_ref, line_ref, hist_in, pos_ref, out_ref, hist_ref):
    _, bx, by, bz = pos_ref.shape
    lines = bx * by
    row = line_ref[0, 0].astype(f32)
    row = jnp.concatenate([row, row], axis=1)
    rows = lax.broadcasted_iota(jnp.int32, (lines, row.shape[1]), 0).astype(f32)
    place = jnp.where(rows == row, 1.0, 0.0).astype(bf16)
    total = mm(place, jnp.concatenate(split(acc_ref[...], 2), axis=0))
    out_ref[0] = pos_ref[0] + total.reshape(bx, by, bz)
    hist_ref[...] = hist_in[0:2, : hist_ref.shape[1]]


def local(sizes, positions, pair_node, pair_line, pair_far, far_line, pair_geom, live_blocks):
    blocks, pairs = pair_node.shape[3:]
    blk = positions.shape[1:]
    devices = sizes[0] * sizes[1] * sizes[2]
    outer = blocks // 2
    rows = 2 * blocks + 6 * outer
    dma = pltpu.SemaphoreType.DMA
    vmem = pl.BlockSpec(memory_space=pltpu.VMEM)
    moved, hist = pl.pallas_call(
        functools.partial(kernel, sizes, blk),
        out_shape=(
            jax.ShapeDtypeStruct((blocks, 3 * blk[2]), f32),
            jax.ShapeDtypeStruct((8, 128), f32),
        ),
        in_specs=[pl.BlockSpec(memory_space=pl.ANY)] * 7,
        out_specs=(vmem, vmem),
        scratch_shapes=[
            pltpu.VMEM(live_blocks.shape, jnp.int32),
            pltpu.VMEM(pair_node.shape, jnp.int32),
            pltpu.VMEM(pair_line.shape, jnp.int32),
            pltpu.VMEM(pair_far.shape, jnp.int32),
            pltpu.VMEM(far_line.shape, jnp.int32),
            pltpu.VMEM(pair_geom.shape, f32),
            pltpu.VMEM(positions.shape, f32),
            pltpu.VMEM((4 * (pairs // 128) + 1, outer, 128), f32),
            pltpu.VMEM((2, blocks, pairs), f32),
            pltpu.VMEM((blocks * pairs, blk[2]), bf16),
            pltpu.VMEM((1, 2 * blocks), f32),
            pltpu.VMEM((rows, 2 * blocks), bf16),
            pltpu.VMEM((rows, pairs), f32),
            pltpu.VMEM((3, rows, pairs), f32),
            pltpu.VMEM((rows, pairs), jnp.int32),
            pltpu.VMEM((rows, pairs), jnp.int32),
            pltpu.VMEM((blocks, pairs), f32),
            pltpu.VMEM((blocks, 3 * blk[2]), f32),
            pltpu.VMEM((6, 4 * (pairs // 128) + 1, outer, 128), f32),
            pltpu.VMEM((SWEEPS, 6, outer, pairs), f32),
            pltpu.VMEM((SWEEPS, 6, outer, pairs), f32),
            pltpu.VMEM((SWEEPS, devices, 1, 128), f32),
            pltpu.VMEM((devices, 1, 128), f32),
            dma((7,)),
            pltpu.SemaphoreType.REGULAR,
            pltpu.SemaphoreType.REGULAR,
            dma((6,)),
            dma((6,)),
            dma((SWEEPS, 6)),
            dma((SWEEPS, 6)),
            dma((SWEEPS,)),
            dma((SWEEPS,)),
            dma,
            dma,
        ],
        compiler_params=pltpu.CompilerParams(collective_id=0, has_side_effects=True),
    )(live_blocks, pair_node, pair_line, pair_far, far_line, pair_geom, positions)
    return pl.pallas_call(
        finish,
        grid=(3,),
        out_shape=(
            jax.ShapeDtypeStruct(positions.shape, f32),
            jax.ShapeDtypeStruct((2, SWEEPS), f32),
        ),
        in_specs=[
            pl.BlockSpec((blocks, blk[2]), lambda c: (0, c)),
            pl.BlockSpec(pair_line.shape, lambda c: (0, 0, 0, 0)),
            pl.BlockSpec((8, 128), lambda c: (0, 0)),
            pl.BlockSpec((1,) + blk, lambda c: (c, 0, 0, 0)),
        ],
        out_specs=(
            pl.BlockSpec((1,) + blk, lambda c: (c, 0, 0, 0)),
            pl.BlockSpec((2, SWEEPS), lambda c: (0, 0)),
        ),
    )(moved, pair_line, hist, positions)


def solution(mesh):
    sizes = tuple(mesh.shape[a] for a in AXES)
    return jax.shard_map(
        functools.partial(local, sizes),
        mesh=mesh,
        in_specs=(
            P(None, "gx", "gy", "gz"),
            P("gx", "gy", "gz", None, None),
            P("gx", "gy", "gz", None),
            P("gx", "gy", "gz", None, None),
            P("gx", "gy", "gz", None),
            P("gx", "gy", "gz", None, None, None),
            P("gx", "gy", "gz"),
        ),
        out_specs=(P(None, "gx", "gy", "gz"), P()),
        check_vma=False,
    )
```

```python
import functools
import itertools

import jax
import jax.numpy as jnp
from jax import lax
from jax.experimental import pallas as pl
from jax.experimental.pallas import tpu as pltpu
from jax.sharding import PartitionSpec as P

RIM = 3
SWEEPS = 5
RELAX = 0.9
AXES = ("gx", "gy", "gz")
MESH = pl.DeviceIdType.MESH
f32 = jnp.float32
bf16 = jnp.bfloat16


def split(x, parts):
    out = []
    for _ in range(parts - 1):
        hi = x.astype(bf16)
        out.append(hi)
        x = x - hi.astype(f32)
    out.append(x.astype(bf16))
    return out


def mm(a, b):
    return jnp.dot(a, b, preferred_element_type=f32)


def near_radii(sizes):
    need = max(sizes[0] - 1, sizes[1] + sizes[2] - 2)
    radii = [1]
    while 2 * radii[-1] < need:
        radii.append(2 * radii[-1])
    return radii


def take_lanes(xs, low, half):
    outs = [[] for _ in xs]
    for h in range(0, low.shape[1], 128):
        idx = low[:, h : h + 128]
        got = [None] * len(xs)
        for j in range(xs[0].shape[1] // 128):
            for i, x in enumerate(xs):
                more = jnp.take_along_axis(
                    x[:, 128 * j : 128 * (j + 1)], idx, axis=1, mode="promise_in_bounds"
                )
                got[i] = jnp.where(half[:, h : h + 128] == j, more, got[i]) if j else more
        for out, x in zip(outs, got):
            out.append(x)
    return [jnp.concatenate(out, axis=1) for out in outs]


def kernel(
    sizes,
    blk,
    live_ref,
    node_hbm,
    line_hbm,
    farpos_hbm,
    farline_hbm,
    geom_hbm,
    pos_hbm,
    out_ref,
    hist_out,
    node_ref,
    line_ref,
    farpos_ref,
    farline_ref,
    geom_ref,
    pos_ref,
    acc_ref,
    hist_ref,
    step_ref,
    req,
    cols,
    hot,
    two,
    amat,
    cinv,
    geo,
    low_ref,
    half_ref,
    gap,
    wcat,
    reqs,
    dsend,
    drecv,
    erecv,
    rrecv,
    in_sem,
    near_sem,
    whole_sem,
    qs_sem,
    qr_sem,
    ds_sem,
    dr_sem,
    es_sem,
    er_sem,
    rs_sem,
    rr_sem,
):
    nx, ny, nz = sizes
    bx, by, bz = blk
    devices = nx * ny * nz
    blocks, pairs = gap.shape
    outer = blocks // 2
    lines = bx * by
    me = [lax.axis_index(a) for a in AXES]
    mine = (me[0] * ny + me[1]) * nz + me[2]
    dirs = [(a, s) for a in (1, 0, 2) for s in (1, -1)]

    def neighbour(axis, sign):
        to = list(me)
        to[axis] = lax.rem(me[axis] + sign + sizes[axis], sizes[axis])
        return tuple(to)

    def exists(axis, sign):
        return (me[axis] + sign >= 0) & (me[axis] + sign < sizes[axis])

    def coords(k):
        to = lax.rem(mine + k, devices)
        return (to // (ny * nz), lax.rem(to // nz, ny), lax.rem(to, nz))

    def moved_by(axis, k):
        to = me[axis] + k
        return jnp.where(to >= sizes[axis], to - sizes[axis], to) if k else to

    ids = [[moved_by(a, k) for k in range(sizes[a])] for a in range(3)]

    def sphere(r):
        steps = itertools.product(*[range(1 - n, n) for n in sizes])
        return [s for s in steps if sum(abs(x) for x in s) == r]

    def inside(step):
        ok = True
        for x, n, at in zip(step, sizes, me):
            if x > 0:
                ok = ok & (at < n - x)
            if x < 0:
                ok = ok & (at >= -x)
        return ok

    def signal_sphere(sem, r):
        for step in sphere(r):

            @pl.when(inside(step))
            def _():
                to = tuple(at + x for at, x in zip(me, step))
                pl.semaphore_signal(sem, inc=1, device_id=to, device_id_type=MESH)

    def wait_sphere(sem, r):
        pl.semaphore_wait(sem, sum(jnp.where(inside(s), 1, 0) for s in sphere(r)))

    radii = near_radii(sizes)
    barrier = pltpu.get_barrier_semaphore()
    signal_sphere(barrier, 1)
    inputs = [
        pltpu.make_async_copy(src, dst, in_sem.at[i])
        for i, (src, dst) in enumerate(
            [
                (farline_hbm, farline_ref),
                (farpos_hbm, farpos_ref),
                (geom_hbm, geom_ref),
                (node_hbm, node_ref),
                (line_hbm, line_ref),
                (pos_hbm, pos_ref),
            ]
        )
    ]
    for copy in inputs:
        copy.start()
    for copy in inputs[:3]:
        copy.wait()

    def column(ref):
        row = ref[0, 0].astype(f32)
        return jnp.transpose(jnp.broadcast_to(row, (pairs, blocks)))

    wide = pairs // 128
    planes = [geom_ref[0, 0, 0, outer:, c, :] for c in range(3)]
    planes.append(farpos_ref[0, 0, 0, outer:, :].astype(f32))
    for c in range(4):
        for h in range(wide):
            req[c * wide + h] = planes[c][:, 128 * h : 128 * (h + 1)]
    cols[1] = column(farline_ref)
    req[4 * wide] = cols[1, outer:, :128]

    def ask(d, axis, sign):
        return pltpu.make_async_remote_copy(
            src_ref=req,
            dst_ref=reqs.at[d],
            send_sem=qs_sem.at[d],
            recv_sem=qr_sem.at[d],
            device_id=neighbour(axis, sign),
            device_id_type=MESH,
        )

    wait_sphere(barrier, 1)
    for d, (axis, sign) in enumerate(dirs):

        @pl.when(exists(axis, sign))
        def _():
            ask(d, axis, sign).start()

    signal_sphere(near_sem.at[0], radii[0])
    for copy in inputs[3:5]:
        copy.wait()
    cols[0] = column(line_ref)

    for d, (axis, sign) in enumerate(dirs):

        @pl.when(jnp.logical_not(exists(axis, -sign)))
        def _():
            reqs[d] = jnp.zeros(req.shape, f32)

        @pl.when(jnp.logical_not(exists(axis, sign)))
        def _():
            for t in range(SWEEPS):
                drecv[t, d] = jnp.zeros((outer, pairs), f32)

    live_rows = lax.broadcasted_iota(jnp.int32, (blocks, pairs), 0) < live_ref[0, 0, 0]
    lane_node = lax.broadcasted_iota(jnp.int32, (pairs, bz), 1).astype(f32)
    node_t = jnp.transpose(node_ref[0, 0, 0].astype(f32))
    for b in range(blocks):
        if b == outer:
            wait_sphere(near_sem.at[0], radii[0])
            if len(radii) > 1:
                signal_sphere(near_sem.at[1], radii[1])
        hot[pl.ds(b * pairs, pairs), :] = jnp.where(
            node_t[:, b : b + 1] == lane_node, 1.0, 0.0
        ).astype(bf16)
    row_line = line_ref[0, 0].astype(f32)
    two[...] = jnp.concatenate([row_line, row_line], axis=1)
    row_mod = lax.broadcasted_iota(jnp.int32, (blocks, blocks), 0)
    col_mod = lax.broadcasted_iota(jnp.int32, (blocks, blocks), 1)
    line_b = cols[0]
    same = line_b[:, :blocks] == row_line
    first_col = 1.0 - jnp.max(
        jnp.where(same & (col_mod < row_mod), 1.0, 0.0), axis=1, keepdims=True
    )

    def expand(stack, step):
        rows = stack.shape[0]
        which = lax.rem(lax.broadcasted_iota(jnp.int32, (rows, pairs), 0), step)
        return jnp.concatenate(
            [jnp.where(which == j, stack, 0.0).astype(bf16) for j in range(step)], axis=1
        )

    counts = []
    for g in range(blocks // 8):
        ones = jnp.where(live_rows[8 * g : 8 * g + 8], 1.0, 0.0)
        counts.append(mm(expand(ones, 8), hot[pl.ds(8 * g * pairs, 8 * pairs), :]))
    counts = jnp.concatenate(counts, axis=0).astype(bf16)

    def located(code, zpos, shift):
        e = jnp.floor((code + 0.5) / (by + 2 * RIM))
        f = code - e * (by + 2 * RIM)
        e = e - (RIM + shift[0] * bx)
        f = f - (RIM + shift[1] * by)
        z = zpos - (RIM + shift[2] * bz)
        ok_line = (e >= 0) & (e < bx) & (f >= 0) & (f < by)
        return jnp.where(ok_line, e * by + f, -1.0), z, ok_line & (z >= 0) & (z < bz)

    def setup(row, line, node, geom):
        n = line.shape[0]
        lane_line = lax.broadcasted_iota(jnp.int32, (n, lines), 1).astype(f32)
        a = jnp.where(line[:, : 2 * blocks] == two[...], 1.0, 0.0).astype(bf16)
        amat[pl.ds(row, n), :] = a
        cinv[pl.ds(row, n), :] = RELAX / (1.0 + mm(a[:, :blocks], counts))
        idx = node.astype(jnp.int32)
        low = lax.bitwise_and(idx, 127)
        half = lax.shift_right_logical(idx, 7)
        low_ref[pl.ds(row, n), :] = low
        half_ref[pl.ds(row, n), :] = half
        own = jnp.where(line == lane_line, 1.0, 0.0).astype(bf16)
        vals = []
        for c in range(3):
            geo[c, pl.ds(row, n), :] = geom[c]
            vals.append(sum(mm(own, part) for part in split(pos_ref[c].reshape(lines, bz), 3)))
        return sum(g * x for g, x in zip(geom, take_lanes(vals, low, half)))

    def cat(parts):
        return jnp.concatenate(parts, axis=0)

    inputs[5].wait()
    for d, (axis, sign) in enumerate(dirs):

        @pl.when(exists(axis, -sign))
        def _():
            ask(d, axis, sign).wait_recv()

    asked = []
    for d, (axis, sign) in enumerate(dirs):
        shift = [0, 0, 0]
        shift[axis] = sign
        got = [
            jnp.concatenate([reqs[d, c * wide + h] for h in range(wide)], axis=1) for c in range(4)
        ]
        code = jnp.concatenate([reqs[d, 4 * wide]] * wide, axis=1)
        line, z, ok = located(code, got[3], shift)
        asked.append(
            [line, jnp.where(ok, z, 0.0)] + [jnp.where(ok, -got[c], 0.0) for c in range(3)]
        )
    asked = [cat([x[i] for x in asked]) for i in range(5)]
    base = asked[0].shape[0]
    rows = base + 2 * blocks

    def respond(t, total):
        for d, (axis, sign) in enumerate(dirs):
            dsend[t, d] = total(d * outer, outer)

            @pl.when(exists(axis, -sign))
            def _():
                answer(t, d, axis, sign).start()

    def answer(t, d, axis, sign):
        return pltpu.make_async_remote_copy(
            src_ref=dsend.at[t, d],
            dst_ref=drecv.at[t, d],
            send_sem=ds_sem.at[t, d],
            recv_sem=dr_sem.at[t, d],
            device_id=neighbour(axis, -sign),
            device_id_type=MESH,
        )

    def received(t):
        for d, (axis, sign) in enumerate(dirs):

            @pl.when(exists(axis, sign))
            def _():
                answer(t, d, axis, sign).wait_recv()

        got = drecv[t, 0]
        for d in range(1, len(dirs)):
            got = got + drecv[t, d]
        return got

    first = setup(0, asked[0], asked[1], asked[2:])
    respond(0, lambda row, n: first[row : row + n])
    for i, r in enumerate(radii[1:], 1):
        wait_sphere(near_sem.at[i], r)
        if i + 1 < len(radii):
            signal_sphere(near_sem.at[i + 1], radii[i + 1])
    for k in range(1, nx):
        to = (ids[0][k], me[1], me[2])
        pl.semaphore_signal(whole_sem, inc=1, device_id=to, device_id_type=MESH)

    line, z, ok = located(cols[1], farpos_ref[0, 0, 0].astype(f32), (0, 0, 0))
    geom = [geom_ref[0, 0, 0, :, c, :] for c in range(4)]
    start = setup(
        base,
        cat([line_b, line]),
        cat([node_ref[0, 0, 0].astype(f32), jnp.where(ok, z, 0.0)]),
        [cat([geom[c], jnp.where(ok, -geom[c], 0.0)]) for c in range(3)],
    )
    start = start[:blocks] + start[blocks:] - geom[3]
    if nx > 1:
        pl.semaphore_wait(whole_sem, nx - 1)
    gap[0:outer, :] = start[:outer]
    gap[pl.ds(outer, outer), :] = start[outer:] + received(0)
    acc_ref[...] = jnp.zeros_like(acc_ref)

    def to_all(ref, send_sem, recv_sem):
        def send(to):
            pltpu.make_async_remote_copy(
                src_ref=ref,
                dst_ref=ref,
                send_sem=send_sem,
                recv_sem=recv_sem,
                device_id=to,
                device_id_type=MESH,
            ).start()

        if devices <= 32:
            for a in range(nx):
                for b in range(ny):
                    for c in range(nz):
                        if a or b or c:
                            send((ids[0][a], ids[1][b], ids[2][c]))
        else:

            def step(k, carry):
                send(coords(k))
                return carry

            lax.fori_loop(1, devices, step, 0)

    def lanes_sum(x):
        x = jnp.sum(x, axis=0, keepdims=True)
        out = x[:, :128]
        for j in range(1, x.shape[1] // 128):
            out = out + x[:, 128 * j : 128 * (j + 1)]
        return out

    lane = lax.broadcasted_iota(jnp.int32, (1, 128), 1)
    at_line = lax.broadcasted_iota(jnp.int32, (lines, 2 * blocks), 0).astype(f32)
    place = jnp.where(at_line == two[...], 1.0, 0.0).astype(bf16)

    def placed(x):
        return mm(place, cat(split(x, 2)))

    def apply(row, n, parts):
        both = mm(amat[row : row + n, :], parts)
        return [both[:, c * bz : (c + 1) * bz] * cinv[row : row + n, :] for c in range(3)]

    def dots(row, n, moved):
        low = low_ref[row : row + n, :]
        half = half_ref[row : row + n, :]
        got = take_lanes(moved, low, half)
        return sum(geo[c, row : row + n] * got[c] for c in range(3))

    def sweep(t, last):
        depth = jnp.where(live_rows, jnp.maximum(-gap[...], 0.0), 0.0)
        squares = lanes_sum(depth * depth)
        erecv[t, mine] = squares
        to_all(erecv.at[t, mine], es_sem.at[t], er_sem.at[t])
        for g in range(blocks // 8):
            lo, hi = 8 * g, 8 * g + 8
            terms = cat([depth[lo:hi] * geo[c, base + lo : base + hi] for c in range(3)])
            top = terms.astype(bf16).astype(f32)
            sums = mm(expand(cat([top, terms - top]), 8), hot[pl.ds(lo * pairs, 8 * pairs), :])
            sums = sums[:24] + sums[24:]
            for c in range(3):
                wcat[lo:hi, c * bz : (c + 1) * bz] = sums[8 * c : 8 * c + 8]
        parts = cat(split(wcat[...], 2))
        if not last:
            far = apply(0, base, parts)
            respond(
                t + 1, lambda row, n: dots(row, n, [m[row : row + n] for m in far])
            )
        moved = apply(base, blocks if last else 2 * blocks, parts)
        near = jnp.concatenate([m[:blocks] for m in moved], axis=1)
        resid = jnp.sum(lanes_sum(near * near * first_col), axis=1, keepdims=True)
        rrecv[mine] = jnp.where(lane == t, resid, rrecv[mine])
        if last:
            to_all(rrecv.at[mine], rs_sem, rr_sem)
            for c in range(3):
                cut = slice(c * bz, (c + 1) * bz)
                done = placed(acc_ref[:, cut])
                out_ref[c] = pos_ref[c] + done.reshape(bx, by, bz)
                step_ref[c] = placed(first_col * near[:, cut]).reshape(bx, by, bz)
        else:
            step = dots(base, 2 * blocks, moved)
            step = step[:blocks] + step[blocks:]
        others = erecv.at[t, pl.ds(0, devices - 1)]
        pltpu.make_async_copy(others, others, er_sem.at[t]).wait()
        energy = jnp.sum(jnp.sum(erecv[t], axis=0), axis=1, keepdims=True)
        scale = 1.0 / (1.0 + energy / (blocks * pairs * devices))
        hist_ref[0:1, :] = jnp.where(lane == t, energy, hist_ref[0:1, :])
        hist_ref[1:2, :] = jnp.where(lane == t, scale, hist_ref[1:2, :])
        if last:
            for c in range(3):
                out_ref[c] = out_ref[c] + scale[:, :, None] * step_ref[c]
        else:
            acc_ref[...] = acc_ref[...] + (scale * first_col) * near
            more = received(t + 1)
            gap[0:outer, :] = gap[0:outer, :] + scale * step[:outer]
            gap[pl.ds(outer, outer), :] = gap[pl.ds(outer, outer), :] + scale * (
                step[outer:] + more
            )

    rrecv[mine] = jnp.zeros((1, 128), f32)
    hist_ref[...] = jnp.zeros_like(hist_ref)

    def body(t, carry):
        sweep(t, False)
        return carry

    lax.fori_loop(0, SWEEPS - 1, body, 0)
    sweep(SWEEPS - 1, True)

    for d, (axis, sign) in enumerate(dirs):

        @pl.when(exists(axis, sign))
        def _():
            ask(d, axis, sign).wait_send()

        @pl.when(exists(axis, -sign))
        def _():
            for t in range(SWEEPS):
                answer(t, d, axis, sign).wait_send()

    others = rrecv.at[pl.ds(0, devices - 1)]
    pltpu.make_async_copy(others, others, rr_sem).wait()
    for t in range(SWEEPS):
        ref = erecv.at[t, pl.ds(0, devices - 1)]
        pltpu.make_async_copy(ref, ref, es_sem.at[t]).wait()
    others = rrecv.at[pl.ds(0, devices - 1)]
    pltpu.make_async_copy(others, others, rs_sem).wait()
    energy, scale = hist_ref[0:1, :], hist_ref[1:2, :]
    resid = jnp.sum(rrecv[...], axis=0)
    hist_out[0:1, :] = jnp.sqrt(1.0 + energy / (blocks * pairs))[:, :SWEEPS]
    resid = scale * scale * resid / (bx * by * bz)
    hist_out[1:2, :] = jnp.sqrt(1.0 + resid)[:, :SWEEPS]


def finish(pos_ref, hist_ref, pos_out, hist_out, sem):
    copies = [
        pltpu.make_async_copy(pos_ref, pos_out, sem.at[0]),
        pltpu.make_async_copy(hist_ref, hist_out, sem.at[1]),
    ]
    for copy in copies:
        copy.start()
    for copy in copies:
        copy.wait()


def local(sizes, positions, pair_node, pair_line, pair_far, far_line, pair_geom, live_blocks):
    blocks, pairs = pair_node.shape[3:]
    blk = positions.shape[1:]
    devices = sizes[0] * sizes[1] * sizes[2]
    outer = blocks // 2
    rows = 2 * blocks + 6 * outer
    dma = pltpu.SemaphoreType.DMA
    vmem = pl.BlockSpec(memory_space=pltpu.VMEM)
    moved, hist = pl.pallas_call(
        functools.partial(kernel, sizes, blk),
        out_shape=(
            pltpu.VMEM(positions.shape, f32),
            pltpu.VMEM((2, SWEEPS), f32),
        ),
        in_specs=[pl.BlockSpec(memory_space=pltpu.SMEM)]
        + [pl.BlockSpec(memory_space=pltpu.HBM)] * 6,
        out_specs=(vmem, vmem),
        scratch_shapes=[
            pltpu.VMEM(pair_node.shape, jnp.int32),
            pltpu.VMEM(pair_line.shape, jnp.int32),
            pltpu.VMEM(pair_far.shape, jnp.int32),
            pltpu.VMEM(far_line.shape, jnp.int32),
            pltpu.VMEM(pair_geom.shape, f32),
            pltpu.VMEM(positions.shape, f32),
            pltpu.VMEM((blocks, 3 * blk[2]), f32),
            pltpu.VMEM((8, 128), f32),
            pltpu.VMEM(positions.shape, f32),
            pltpu.VMEM((4 * (pairs // 128) + 1, outer, 128), f32),
            pltpu.VMEM((2, blocks, pairs), f32),
            pltpu.VMEM((blocks * pairs, blk[2]), bf16),
            pltpu.VMEM((1, 2 * blocks), f32),
            pltpu.VMEM((rows, 2 * blocks), bf16),
            pltpu.VMEM((rows, pairs), f32),
            pltpu.VMEM((3, rows, pairs), f32),
            pltpu.VMEM((rows, pairs), jnp.int32),
            pltpu.VMEM((rows, pairs), jnp.int32),
            pltpu.VMEM((blocks, pairs), f32),
            pltpu.VMEM((blocks, 3 * blk[2]), f32),
            pltpu.VMEM((6, 4 * (pairs // 128) + 1, outer, 128), f32),
            pltpu.VMEM((SWEEPS, 6, outer, pairs), f32),
            pltpu.VMEM((SWEEPS, 6, outer, pairs), f32),
            pltpu.VMEM((SWEEPS, devices, 1, 128), f32),
            pltpu.VMEM((devices, 1, 128), f32),
            dma((6,)),
            pltpu.SemaphoreType.REGULAR((len(near_radii(sizes)),)),
            pltpu.SemaphoreType.REGULAR,
            dma((6,)),
            dma((6,)),
            dma((SWEEPS, 6)),
            dma((SWEEPS, 6)),
            dma((SWEEPS,)),
            dma((SWEEPS,)),
            dma,
            dma,
        ],
        compiler_params=pltpu.CompilerParams(
            collective_id=0, has_side_effects=True, vmem_limit_bytes=40 << 20
        ),
    )(
        live_blocks,
        *[
            pltpu.with_memory_space_constraint(x, pltpu.HBM)
            for x in (
                pair_node,
                pair_line,
                pair_far,
                far_line,
                pair_geom,
                positions,
            )
        ]
    )
    return pl.pallas_call(
        finish,
        out_shape=(
            jax.ShapeDtypeStruct(positions.shape, f32),
            jax.ShapeDtypeStruct((2, SWEEPS), f32),
        ),
        in_specs=[vmem] * 2,
        out_specs=[pl.BlockSpec(memory_space=pl.ANY)] * 2,
        scratch_shapes=[dma((2,))],
        compiler_params=pltpu.CompilerParams(vmem_limit_bytes=1 << 20),
    )(moved, hist)


def solution(mesh):
    sizes = tuple(mesh.shape[a] for a in AXES)
    return jax.shard_map(
        functools.partial(local, sizes),
        mesh=mesh,
        in_specs=(
            P(None, "gx", "gy", "gz"),
            P("gx", "gy", "gz", None, None),
            P("gx", "gy", "gz", None),
            P("gx", "gy", "gz", None, None),
            P("gx", "gy", "gz", None),
            P("gx", "gy", "gz", None, None, None),
            P("gx", "gy", "gz"),
        ),
        out_specs=(P(None, "gx", "gy", "gz"), P()),
        check_vma=False,
    )
```

```python
import functools
import itertools

import jax
import jax.numpy as jnp
from jax import lax
from jax.experimental import pallas as pl
from jax.experimental.pallas import tpu as pltpu
from jax.sharding import PartitionSpec as P

RIM = 3
SWEEPS = 5
RELAX = 0.9
AXES = ("gx", "gy", "gz")
MESH = pl.DeviceIdType.MESH
f32 = jnp.float32
bf16 = jnp.bfloat16


def split(x, parts):
    out = []
    for _ in range(parts - 1):
        hi = x.astype(bf16)
        out.append(hi)
        x = x - hi.astype(f32)
    out.append(x.astype(bf16))
    return out


def mm(a, b):
    return jnp.dot(a, b, preferred_element_type=f32)


def near_radii(sizes):
    need = max(sizes[0] - 1, sizes[1] + sizes[2] - 2)
    radii = [1]
    while 2 * radii[-1] < need:
        radii.append(2 * radii[-1])
    return radii


def take_lanes(xs, low, half):
    outs = [[] for _ in xs]
    for h in range(0, low.shape[1], 128):
        idx = low[:, h : h + 128]
        got = [None] * len(xs)
        for j in range(xs[0].shape[1] // 128):
            for i, x in enumerate(xs):
                more = jnp.take_along_axis(
                    x[:, 128 * j : 128 * (j + 1)], idx, axis=1, mode="promise_in_bounds"
                )
                got[i] = jnp.where(half[:, h : h + 128] == j, more, got[i]) if j else more
        for out, x in zip(outs, got):
            out.append(x)
    return [jnp.concatenate(out, axis=1) for out in outs]


def kernel(
    sizes,
    blk,
    live_ref,
    node_hbm,
    line_hbm,
    farpos_hbm,
    farline_hbm,
    geom_hbm,
    pos_hbm,
    out_ref,
    hist_out,
    node_ref,
    line_ref,
    farpos_ref,
    farline_ref,
    geom_ref,
    pos_ref,
    acc_ref,
    near_ref,
    step_ref,
    pos3,
    code,
    codes,
    lsend,
    lrecv,
    req,
    cols,
    hot,
    two,
    amat,
    cinv,
    geo,
    low_ref,
    half_ref,
    gap,
    terms,
    sums,
    reqs,
    dsend,
    drecv,
    erecv,
    rrecv,
    in_sem,
    near_sem,
    whole_sem,
    ds_sem,
    dr_sem,
    es_sem,
    er_sem,
):
    nx, ny, nz = sizes
    bx, by, bz = blk
    devices = nx * ny * nz
    blocks, pairs = gap.shape
    outer = blocks // 2
    lines = bx * by
    me = [lax.axis_index(a) for a in AXES]
    mine = (me[0] * ny + me[1]) * nz + me[2]
    dirs = [(a, s) for a in (1, 0, 2) for s in (1, -1)]

    def neighbour(axis, sign):
        to = list(me)
        to[axis] = lax.rem(me[axis] + sign + sizes[axis], sizes[axis])
        return tuple(to)

    def exists(axis, sign):
        return (me[axis] + sign >= 0) & (me[axis] + sign < sizes[axis])

    def coords(k):
        to = lax.rem(mine + k, devices)
        return (to // (ny * nz), lax.rem(to // nz, ny), lax.rem(to, nz))

    def moved_by(axis, k):
        to = me[axis] + k
        return jnp.where(to >= sizes[axis], to - sizes[axis], to) if k else to

    ids = [[moved_by(a, k) for k in range(sizes[a])] for a in range(3)]

    def sphere(r):
        steps = itertools.product(*[range(1 - n, n) for n in sizes])
        return [s for s in steps if sum(abs(x) for x in s) == r]

    def inside(step):
        ok = True
        for x, n, at in zip(step, sizes, me):
            if x > 0:
                ok = ok & (at < n - x)
            if x < 0:
                ok = ok & (at >= -x)
        return ok

    def signal_sphere(sem, r):
        for step in sphere(r):

            @pl.when(inside(step))
            def _():
                to = tuple(at + x for at, x in zip(me, step))
                pl.semaphore_signal(sem, inc=1, device_id=to, device_id_type=MESH)

    def wait_sphere(sem, r):
        pl.semaphore_wait(sem, sum(jnp.where(inside(s), 1, 0) for s in sphere(r)))

    radii = near_radii(sizes)
    barrier = pltpu.get_barrier_semaphore()
    signal_sphere(barrier, 1)
    inputs = [
        pltpu.make_async_copy(src, dst, in_sem.at[i])
        for i, (src, dst) in enumerate(
            [
                (farline_hbm, farline_ref),
                (farpos_hbm, farpos_ref),
                (geom_hbm, geom_ref),
                (node_hbm, node_ref),
                (line_hbm, line_ref),
                (pos_hbm, pos_ref),
            ]
        )
    ]
    for copy in inputs:
        copy.start()
    for copy in inputs[:3]:
        copy.wait()

    def column(ref):
        row = ref[0, 0].astype(f32)
        return jnp.transpose(jnp.broadcast_to(row, (pairs, blocks)))

    wide = pairs // 128
    planes = [geom_ref[0, 0, 0, outer:, c, :] for c in range(3)]
    planes.append(farpos_ref[0, 0, 0, outer:, :].astype(f32))
    for c in range(4):
        for h in range(wide):
            req[c * wide + h] = planes[c][:, 128 * h : 128 * (h + 1)]
    cols[1] = column(farline_ref)
    code[...] = cols[1, outer:, :128]

    def remote(src, dst, slot, d, to):
        return pltpu.make_async_remote_copy(
            src_ref=src,
            dst_ref=dst,
            send_sem=ds_sem.at[slot, d],
            recv_sem=dr_sem.at[slot, d],
            device_id=neighbour(*to),
            device_id_type=MESH,
        )

    def ask_line(d, axis, sign):
        return remote(code, codes.at[d], 2, d, (axis, sign))

    def ask_pairs(d, axis, sign):
        return remote(req, reqs.at[d], 3, d, (axis, sign))

    def line_back(d, axis, sign):
        return remote(lsend.at[d], lrecv.at[d], 0, d, (axis, -sign))

    def answer(t, d, axis, sign):
        return remote(dsend.at[t, d], drecv.at[t, d], t % 2, d, (axis, -sign))

    wait_sphere(barrier, 1)
    for ask in (ask_line, ask_pairs):
        for d, (axis, sign) in enumerate(dirs):

            @pl.when(exists(axis, sign))
            def _():
                ask(d, axis, sign).start()

    signal_sphere(near_sem.at[0], radii[0])
    for copy in inputs[3:5]:
        copy.wait()
    cols[0] = column(line_ref)

    for d, (axis, sign) in enumerate(dirs):

        @pl.when(jnp.logical_not(exists(axis, -sign)))
        def _():
            codes[d] = jnp.zeros(code.shape, f32)
            reqs[d] = jnp.zeros(req.shape, f32)

        @pl.when(jnp.logical_not(exists(axis, sign)))
        def _():
            lrecv[d] = jnp.zeros((3, outer, bz), f32)
            for t in range(1, SWEEPS):
                drecv[t, d] = jnp.zeros((outer, pairs), f32)

    def at_lanes(z):
        z = z.astype(jnp.int32)
        return lax.bitwise_and(z, 127), lax.shift_right_arithmetic(z, 7)

    live_rows = lax.broadcasted_iota(jnp.int32, (blocks, pairs), 0) < live_ref[0, 0, 0]
    node_low, node_half = at_lanes(node_ref[0, 0, 0])
    lane_node = lax.broadcasted_iota(jnp.int32, (pairs, 128), 1).astype(f32)
    node_t = jnp.transpose(node_low.astype(f32))
    group = terms.shape[1] // blocks
    terms[...] = jnp.zeros_like(terms)
    for b in range(blocks):
        if b == outer:
            wait_sphere(near_sem.at[0], radii[0])
            if len(radii) > 1:
                signal_sphere(near_sem.at[1], radii[1])
        hot[pl.ds(b * pairs, pairs), :] = jnp.where(
            node_t[:, b : b + 1] == lane_node, 1.0, 0.0
        ).astype(bf16)
    row_line = line_ref[0, 0].astype(f32)
    two[...] = jnp.concatenate([row_line, row_line], axis=1)
    row_mod = lax.broadcasted_iota(jnp.int32, (blocks, blocks), 0)
    col_mod = lax.broadcasted_iota(jnp.int32, (blocks, blocks), 1)
    line_b = cols[0]
    same = line_b[:, :blocks] == row_line
    first_col = 1.0 - jnp.max(
        jnp.where(same & (col_mod < row_mod), 1.0, 0.0), axis=1, keepdims=True
    )

    def cat(parts, axis=0):
        return jnp.concatenate(parts, axis=axis)

    def scatter(values):
        n = len(values)
        for h in range(bz // 128):
            for c in range(n):
                x = jnp.where(node_half == h, values[c], 0.0)
                for j in range(wide):
                    cut = x[:, 128 * j : 128 * (j + 1)]
                    terms[j, pl.ds(h * n + c, blocks, stride=group), :] = cut
        for b in range(blocks):
            slot = cat([terms[j, pl.ds(b * group, group), :] for j in range(wide)], 1)
            both = cat(split(slot, 2))
            both = mm(both, hot[pl.ds(b * pairs, pairs), :])
            sums[pl.ds(b * group, group), :] = both[:group] + both[group:]
        return [
            cat([sums[pl.ds(h * n + c, blocks, stride=group), :] for h in range(bz // 128)], 1)
            for c in range(n)
        ]

    ones = jnp.where(live_rows, 1.0, 0.0)
    counts = scatter([ones, jnp.zeros_like(ones), jnp.zeros_like(ones)])[0].astype(bf16)

    def located(code, zpos, shift):
        e = jnp.floor((code + 0.5) / (by + 2 * RIM))
        f = code - e * (by + 2 * RIM)
        e = e - (RIM + shift[0] * bx)
        f = f - (RIM + shift[1] * by)
        z = zpos - (RIM + shift[2] * bz)
        ok_line = (e >= 0) & (e < bx) & (f >= 0) & (f < by)
        return jnp.where(ok_line, e * by + f, -1.0), z, ok_line & (z >= 0) & (z < bz)

    def setup(row, line, node, geom):
        n = line.shape[0]
        a = jnp.where(line[:, : 2 * blocks] == two[...], 1.0, 0.0).astype(bf16)
        amat[pl.ds(row, n), :] = a
        cinv[pl.ds(row, n), :] = RELAX / (1.0 + mm(a[:, :blocks], counts))
        low, half = at_lanes(node)
        low_ref[pl.ds(row, n), :] = low
        half_ref[pl.ds(row, n), :] = half
        for c in range(3):
            geo[c, pl.ds(row, n), :] = geom[c]

    def fetch(line):
        lane_line = lax.broadcasted_iota(jnp.int32, (line.shape[0], lines), 1).astype(f32)
        own = jnp.where(line == lane_line, 1.0, 0.0).astype(bf16)
        return [sum(mm(own, pos3[c, k]) for k in range(3)) for c in range(3)]

    base = len(dirs) * outer
    rows = base + 2 * blocks
    node = node_ref[0, 0, 0].astype(f32)
    far = farpos_ref[0, 0, 0].astype(f32)
    geom = [geom_ref[0, 0, 0, :, c, :] for c in range(4)]
    line, z, ok = located(cols[1], far, (0, 0, 0))
    setup(
        base,
        cat([line_b, line]),
        cat([node, jnp.where(ok, z, 0.0)]),
        [cat([geom[c], jnp.where(ok, -geom[c], 0.0)]) for c in range(3)],
    )
    inputs[5].wait()
    for c in range(3):
        for k, part in enumerate(split(pos_ref[c].reshape(lines, bz), 3)):
            pos3[c, k] = part
    vals = fetch(cat([line_b, line]))

    for d, (axis, sign) in enumerate(dirs):

        @pl.when(exists(axis, -sign))
        def _():
            ask_line(d, axis, sign).wait_recv()

    shifts = []
    for axis, sign in dirs:
        shifts.append([sign if a == axis else 0 for a in range(3)])
    asked = []
    for d in range(len(dirs)):
        there = jnp.concatenate([codes[d]] * wide, axis=1)
        asked.append(located(there, 0.0, shifts[d])[0])
    back = fetch(cat(asked))
    for d, (axis, sign) in enumerate(dirs):
        for c in range(3):
            lsend[d, c] = back[c][d * outer : (d + 1) * outer]

        @pl.when(exists(axis, -sign))
        def _():
            line_back(d, axis, sign).start()

    for i, r in enumerate(radii[1:], 1):
        wait_sphere(near_sem.at[i], r)
        if i + 1 < len(radii):
            signal_sphere(near_sem.at[i + 1], radii[i + 1])
    for k in range(1, nx):
        to = (ids[0][k], me[1], me[2])
        pl.semaphore_signal(whole_sem, inc=1, device_id=to, device_id_type=MESH)

    start = take_lanes([v[:blocks] for v in vals], *at_lanes(node))
    inner = take_lanes([v[blocks : blocks + outer] for v in vals], *at_lanes(z[:outer]))
    gap[...] = sum(geom[c] * start[c] for c in range(3)) - geom[3]
    gap[0:outer, :] = gap[0:outer, :] - sum(geom[c][:outer] * inner[c] for c in range(3))

    for d, (axis, sign) in enumerate(dirs):

        @pl.when(exists(axis, -sign))
        def _():
            ask_pairs(d, axis, sign).wait_recv()

    pairs_in = []
    for d in range(len(dirs)):
        got = [
            jnp.concatenate([reqs[d, c * wide + h] for h in range(wide)], axis=1) for c in range(4)
        ]
        there = jnp.concatenate([codes[d]] * wide, axis=1)
        _, at, ok = located(there, got[3], shifts[d])
        pairs_in.append([jnp.where(ok, at, 0.0)] + [jnp.where(ok, -got[c], 0.0) for c in range(3)])
    pairs_in = [cat([x[i] for x in pairs_in]) for i in range(4)]
    setup(0, cat(asked), pairs_in[0], pairs_in[1:])

    for d, (axis, sign) in enumerate(dirs):

        @pl.when(exists(axis, sign))
        def _():
            line_back(d, axis, sign).wait_recv()

    low, half = at_lanes(far[outer:] - RIM)
    reach = []
    for c in range(3):
        line = vals[c][blocks + outer :]
        for d, (axis, sign) in enumerate(dirs):
            if axis < 2:
                line = line + lrecv[d, c]
        below = lrecv[dirs.index((2, -1)), c][:, bz - 128 :]
        above = lrecv[dirs.index((2, 1)), c][:, :128]
        reach.append(jnp.concatenate([below, line, above], axis=1))
    reach = take_lanes(reach, low, half + 1)
    if nx > 1:
        pl.semaphore_wait(whole_sem, nx - 1)
    gap[pl.ds(outer, outer), :] = gap[pl.ds(outer, outer), :] - sum(
        geom[c][outer:] * reach[c] for c in range(3)
    )
    for d, (axis, sign) in enumerate(dirs):

        @pl.when(exists(axis, sign))
        def _():
            ask_line(d, axis, sign).wait_send()
            ask_pairs(d, axis, sign).wait_send()

        @pl.when(exists(axis, -sign))
        def _():
            line_back(d, axis, sign).wait_send()

    def respond(t, total):
        for d, (axis, sign) in enumerate(dirs):
            dsend[t, d] = total(d * outer, outer)

            @pl.when(exists(axis, -sign))
            def _():
                answer(t, d, axis, sign).start()

    def responded(t):
        for d, (axis, sign) in enumerate(dirs):

            @pl.when(exists(axis, -sign))
            def _():
                answer(t, d, axis, sign).wait_send()

    def received(t):
        for d, (axis, sign) in enumerate(dirs):

            @pl.when(exists(axis, sign))
            def _():
                answer(t, d, axis, sign).wait_recv()

        got = drecv[t, 0]
        for d in range(1, len(dirs)):
            got = got + drecv[t, d]
        return got

    acc_ref[...] = jnp.zeros_like(acc_ref)

    def to_all(ref, send_sem, recv_sem):
        def send(to):
            pltpu.make_async_remote_copy(
                src_ref=ref,
                dst_ref=ref,
                send_sem=send_sem,
                recv_sem=recv_sem,
                device_id=to,
                device_id_type=MESH,
            ).start()

        if devices <= 32:
            for a in range(nx):
                for b in range(ny):
                    for c in range(nz):
                        if a or b or c:
                            send((ids[0][a], ids[1][b], ids[2][c]))
        else:

            def step(k, carry):
                send(coords(k))
                return carry

            lax.fori_loop(1, devices, step, 0)

    def lanes_sum(x):
        x = jnp.sum(x, axis=0, keepdims=True)
        out = x[:, :128]
        for j in range(1, x.shape[1] // 128):
            out = out + x[:, 128 * j : 128 * (j + 1)]
        return out

    lane = lax.broadcasted_iota(jnp.int32, (1, 128), 1)
    at_line = lax.broadcasted_iota(jnp.int32, (lines, 2 * blocks), 0).astype(f32)
    place = jnp.where(at_line == two[...], 1.0, 0.0).astype(bf16)

    def placed(x):
        return mm(place, cat(split(x, 2)))

    def apply(row, n, parts):
        both = mm(amat[row : row + n, :], parts)
        return [both[:, c * bz : (c + 1) * bz] * cinv[row : row + n, :] for c in range(3)]

    def dots(row, n, moved):
        low = low_ref[row : row + n, :]
        half = half_ref[row : row + n, :]
        got = take_lanes(moved, low, half)
        return sum(geo[c, row : row + n] * got[c] for c in range(3))

    def wait_all(ref, sem):
        others = ref.at[pl.ds(0, devices - 1)]
        pltpu.make_async_copy(others, others, sem).wait()

    def settle(scale):
        acc_ref[...] = acc_ref[...] + (scale * first_col) * near_ref[...]

    rrecv[mine] = jnp.zeros((1, 128), f32)
    energies, scales = [], []
    for t in range(SWEEPS):
        last, slot = t == SWEEPS - 1, t % 2
        depth = jnp.where(live_rows, jnp.maximum(-gap[...], 0.0), 0.0)
        erecv[t, mine] = lanes_sum(depth * depth)
        to_all(erecv.at[t, mine], es_sem.at[slot], er_sem.at[slot])
        own = scatter([depth * geo[c, base : base + blocks] for c in range(3)])
        parts = cat(split(cat(own, 1), 2))
        if t:
            wait_all(erecv.at[t - 1], es_sem.at[1 - slot])
            responded(t)
            settle(scales[-1])
        if not last:
            far = apply(0, base, parts)
            respond(t + 1, lambda row, n: dots(row, n, [m[row : row + n] for m in far]))
        moved = apply(base, blocks if last else 2 * blocks, parts)
        near = cat([m[:blocks] for m in moved], 1)
        near_ref[...] = near
        resid = jnp.sum(lanes_sum(near * near * first_col), axis=1, keepdims=True)
        rrecv[mine] = jnp.where(lane == t, resid, rrecv[mine])
        if last:
            to_all(rrecv.at[mine], es_sem.at[2], er_sem.at[2])
            for c in range(3):
                cut = slice(c * bz, (c + 1) * bz)
                done = placed(acc_ref[:, cut])
                out_ref[c] = pos_ref[c] + done.reshape(bx, by, bz)
                step_ref[c] = placed(first_col * near[:, cut]).reshape(bx, by, bz)
        else:
            step = dots(base, 2 * blocks, moved)
            step = step[:blocks] + step[blocks:]
            more = received(t + 1)
        wait_all(erecv.at[t], er_sem.at[slot])
        energy = jnp.sum(jnp.sum(erecv[t], axis=0), axis=1, keepdims=True)
        scale = 1.0 / (1.0 + energy / (blocks * pairs * devices))
        energies.append(energy)
        scales.append(scale)
        if last:
            for c in range(3):
                out_ref[c] = out_ref[c] + scale[:, :, None] * step_ref[c]
        else:
            gap[0:outer, :] = gap[0:outer, :] + scale * step[:outer]
            gap[pl.ds(outer, outer), :] = gap[pl.ds(outer, outer), :] + scale * (
                step[outer:] + more
            )

    wait_all(erecv.at[SWEEPS - 1], es_sem.at[(SWEEPS - 1) % 2])
    energy, scale = jnp.zeros((1, 128), f32), jnp.zeros((1, 128), f32)
    for t in range(SWEEPS):
        energy = jnp.where(lane == t, energies[t], energy)
        scale = jnp.where(lane == t, scales[t], scale)
    hist_out[0:1, :] = jnp.sqrt(1.0 + energy / (blocks * pairs))[:, :SWEEPS]
    factor = scale * scale / (bx * by * bz)
    wait_all(rrecv, er_sem.at[2])
    resid = factor * jnp.sum(rrecv[...], axis=0)
    hist_out[1:2, :] = jnp.sqrt(1.0 + resid)[:, :SWEEPS]
    wait_all(rrecv, es_sem.at[2])


def finish(pos_ref, hist_ref, pos_out, hist_out, sem):
    copies = [
        pltpu.make_async_copy(pos_ref, pos_out, sem.at[0]),
        pltpu.make_async_copy(hist_ref, hist_out, sem.at[1]),
    ]
    for copy in copies:
        copy.start()
    for copy in copies:
        copy.wait()


def local(sizes, positions, pair_node, pair_line, pair_far, far_line, pair_geom, live_blocks):
    blocks, pairs = pair_node.shape[3:]
    blk = positions.shape[1:]
    devices = sizes[0] * sizes[1] * sizes[2]
    outer = blocks // 2
    rows = 2 * blocks + 6 * outer
    group = -(-3 * (blk[2] // 128) // 8) * 8
    dma = pltpu.SemaphoreType.DMA
    vmem = pl.BlockSpec(memory_space=pltpu.VMEM)
    moved, hist = pl.pallas_call(
        functools.partial(kernel, sizes, blk),
        out_shape=(
            pltpu.VMEM(positions.shape, f32),
            pltpu.VMEM((2, SWEEPS), f32),
        ),
        in_specs=[pl.BlockSpec(memory_space=pltpu.SMEM)]
        + [pl.BlockSpec(memory_space=pltpu.HBM)] * 6,
        out_specs=(vmem, vmem),
        scratch_shapes=[
            pltpu.VMEM(pair_node.shape, jnp.int32),
            pltpu.VMEM(pair_line.shape, jnp.int32),
            pltpu.VMEM(pair_far.shape, jnp.int32),
            pltpu.VMEM(far_line.shape, jnp.int32),
            pltpu.VMEM(pair_geom.shape, f32),
            pltpu.VMEM(positions.shape, f32),
            pltpu.VMEM((blocks, 3 * blk[2]), f32),
            pltpu.VMEM((blocks, 3 * blk[2]), f32),
            pltpu.VMEM(positions.shape, f32),
            pltpu.VMEM((3, 3, blk[0] * blk[1], blk[2]), bf16),
            pltpu.VMEM((outer, 128), f32),
            pltpu.VMEM((6, outer, 128), f32),
            pltpu.VMEM((6, 3, outer, blk[2]), f32),
            pltpu.VMEM((6, 3, outer, blk[2]), f32),
            pltpu.VMEM((4 * (pairs // 128), outer, 128), f32),
            pltpu.VMEM((2, blocks, pairs), f32),
            pltpu.VMEM((blocks * pairs, 128), bf16),
            pltpu.VMEM((1, 2 * blocks), f32),
            pltpu.VMEM((rows, 2 * blocks), bf16),
            pltpu.VMEM((rows, pairs), f32),
            pltpu.VMEM((3, rows, pairs), f32),
            pltpu.VMEM((rows, pairs), jnp.int32),
            pltpu.VMEM((rows, pairs), jnp.int32),
            pltpu.VMEM((blocks, pairs), f32),
            pltpu.VMEM((pairs // 128, blocks * group, 128), f32),
            pltpu.VMEM((blocks * group, 128), f32),
            pltpu.VMEM((6, 4 * (pairs // 128), outer, 128), f32),
            pltpu.VMEM((SWEEPS, 6, outer, pairs), f32),
            pltpu.VMEM((SWEEPS, 6, outer, pairs), f32),
            pltpu.VMEM((SWEEPS, devices, 1, 128), f32),
            pltpu.VMEM((devices, 1, 128), f32),
            dma((6,)),
            pltpu.SemaphoreType.REGULAR((len(near_radii(sizes)),)),
            pltpu.SemaphoreType.REGULAR,
            dma((4, 6)),
            dma((4, 6)),
            dma((3,)),
            dma((3,)),
        ],
        compiler_params=pltpu.CompilerParams(
            collective_id=0, has_side_effects=True, vmem_limit_bytes=40 << 20
        ),
    )(
        live_blocks,
        *[
            pltpu.with_memory_space_constraint(x, pltpu.HBM)
            for x in (
                pair_node,
                pair_line,
                pair_far,
                far_line,
                pair_geom,
                positions,
            )
        ]
    )
    return pl.pallas_call(
        finish,
        out_shape=(
            jax.ShapeDtypeStruct(positions.shape, f32),
            jax.ShapeDtypeStruct((2, SWEEPS), f32),
        ),
        in_specs=[vmem] * 2,
        out_specs=[pl.BlockSpec(memory_space=pl.ANY)] * 2,
        scratch_shapes=[dma((2,))],
        compiler_params=pltpu.CompilerParams(vmem_limit_bytes=1 << 20),
    )(moved, hist)


def solution(mesh):
    sizes = tuple(mesh.shape[a] for a in AXES)
    return jax.shard_map(
        functools.partial(local, sizes),
        mesh=mesh,
        in_specs=(
            P(None, "gx", "gy", "gz"),
            P("gx", "gy", "gz", None, None),
            P("gx", "gy", "gz", None),
            P("gx", "gy", "gz", None, None),
            P("gx", "gy", "gz", None),
            P("gx", "gy", "gz", None, None, None),
            P("gx", "gy", "gz"),
        ),
        out_specs=(P(None, "gx", "gy", "gz"), P()),
        check_vma=False,
    )
```

```python
import functools
import itertools

import jax
import jax.numpy as jnp
from jax import lax
from jax.experimental import pallas as pl
from jax.experimental.pallas import tpu as pltpu
from jax.sharding import PartitionSpec as P

RIM = 3
SWEEPS = 5
RELAX = 0.9
AXES = ("gx", "gy", "gz")
MESH = pl.DeviceIdType.MESH
f32 = jnp.float32
bf16 = jnp.bfloat16


def split(x, parts):
    out = []
    for _ in range(parts - 1):
        hi = x.astype(bf16)
        out.append(hi)
        x = x - hi.astype(f32)
    out.append(x.astype(bf16))
    return out


def mm(a, b):
    return jnp.dot(a, b, preferred_element_type=f32)


def near_radii(sizes):
    need = max(sizes[0] - 1, sizes[1] + sizes[2] - 2)
    radii = [1]
    while 2 * radii[-1] < need:
        radii.append(2 * radii[-1])
    return radii


def take_lanes(xs, low, half):
    outs = [[] for _ in xs]
    for h in range(0, low.shape[1], 128):
        idx = low[:, h : h + 128]
        got = [None] * len(xs)
        for j in range(xs[0].shape[1] // 128):
            for i, x in enumerate(xs):
                more = jnp.take_along_axis(
                    x[:, 128 * j : 128 * (j + 1)], idx, axis=1, mode="promise_in_bounds"
                )
                got[i] = jnp.where(half[:, h : h + 128] == j, more, got[i]) if j else more
        for out, x in zip(outs, got):
            out.append(x)
    return [jnp.concatenate(out, axis=1) for out in outs]


def kernel(
    sizes,
    blk,
    live_ref,
    node_hbm,
    line_hbm,
    farpos_hbm,
    farline_hbm,
    geom_hbm,
    pos_hbm,
    out_ref,
    hist_out,
    node_ref,
    line_ref,
    farpos_ref,
    farline_ref,
    geom_ref,
    pos_ref,
    acc_ref,
    near_ref,
    step_ref,
    pos3,
    code,
    codes,
    there,
    lsend,
    lrecv,
    req,
    cols,
    hot,
    two,
    amat,
    cinv,
    geo,
    low_ref,
    half_ref,
    gap,
    terms,
    sums,
    reqs,
    dsend,
    drecv,
    erecv,
    rrecv,
    near_sem,
    whole_sem,
    ds_sem,
    dr_sem,
    es_sem,
    er_sem,
):
    nx, ny, nz = sizes
    bx, by, bz = blk
    devices = nx * ny * nz
    blocks, pairs = gap.shape
    outer = blocks // 2
    lines = bx * by
    me = [lax.axis_index(a) for a in AXES]
    mine = (me[0] * ny + me[1]) * nz + me[2]
    dirs = [(a, s) for a in (1, 0, 2) for s in (1, -1)]

    def neighbour(axis, sign):
        to = list(me)
        to[axis] = lax.rem(me[axis] + sign + sizes[axis], sizes[axis])
        return tuple(to)

    def exists(axis, sign):
        return (me[axis] + sign >= 0) & (me[axis] + sign < sizes[axis])

    def coords(k):
        to = lax.rem(mine + k, devices)
        return (to // (ny * nz), lax.rem(to // nz, ny), lax.rem(to, nz))

    def moved_by(axis, k):
        to = me[axis] + k
        return jnp.where(to >= sizes[axis], to - sizes[axis], to) if k else to

    ids = [[moved_by(a, k) for k in range(sizes[a])] for a in range(3)]

    def sphere(r):
        steps = itertools.product(*[range(1 - n, n) for n in sizes])
        return [s for s in steps if sum(abs(x) for x in s) == r]

    def inside(step):
        ok = True
        for x, n, at in zip(step, sizes, me):
            if x > 0:
                ok = ok & (at < n - x)
            if x < 0:
                ok = ok & (at >= -x)
        return ok

    def signal_sphere(sem, r):
        for step in sphere(r):

            @pl.when(inside(step))
            def _():
                to = tuple(at + x for at, x in zip(me, step))
                pl.semaphore_signal(sem, inc=1, device_id=to, device_id_type=MESH)

    def wait_sphere(sem, r):
        pl.semaphore_wait(sem, sum(jnp.where(inside(s), 1, 0) for s in sphere(r)))

    radii = near_radii(sizes)
    barrier = pltpu.get_barrier_semaphore()
    signal_sphere(barrier, 1)
    inputs = [
        pltpu.make_async_copy(*copy)
        for copy in [
            (farline_hbm, farline_ref, ds_sem.at[0, 0]),
            (farpos_hbm, farpos_ref, ds_sem.at[0, 1]),
            (geom_hbm, geom_ref, ds_sem.at[0, 2]),
            (node_hbm, node_ref, es_sem.at[0]),
            (line_hbm, line_ref, es_sem.at[1]),
            (pos_hbm, pos_ref, es_sem.at[2]),
        ]
    ]
    for copy in inputs:
        copy.start()
    for copy in inputs[:3]:
        copy.wait()

    def column(ref):
        row = ref[0, 0].astype(f32)
        return jnp.transpose(jnp.broadcast_to(row, (pairs, blocks)))

    wide = pairs // 128
    planes = [geom_ref[0, 0, 0, outer:, c, :] for c in range(3)]
    planes.append(farpos_ref[0, 0, 0, outer:, :].astype(f32))
    for c in range(4):
        for h in range(wide):
            req[c * wide + h] = planes[c][:, 128 * h : 128 * (h + 1)]
    cols[1] = column(farline_ref)
    row = farline_ref[0, 0].astype(f32)
    code[...] = jnp.concatenate([row] * (128 // blocks), axis=1)

    def remote(src, dst, send_sem, recv_sem, to):
        return pltpu.make_async_remote_copy(
            src_ref=src,
            dst_ref=dst,
            send_sem=send_sem,
            recv_sem=recv_sem,
            device_id=neighbour(*to),
            device_id_type=MESH,
        )

    def ask_line(d, axis, sign):
        return remote(code, codes.at[pl.ds(d, 1), :], ds_sem.at[1, d], dr_sem.at[1, d], (axis, sign))

    def ask_pairs(d, axis, sign):
        return remote(req, reqs.at[d], ds_sem.at[0, d], dr_sem.at[2, d], (axis, sign))

    def line_back(d, axis, sign):
        sems = ds_sem.at[1, d], dr_sem.at[0, d]
        return remote(lsend.at[d], lrecv.at[d], *sems, (axis, -sign))

    def answer(t, d, axis, sign):
        sems = ds_sem.at[t % 2, d], dr_sem.at[t % 2, d]
        return remote(dsend.at[t, d], drecv.at[t, d], *sems, (axis, -sign))

    def first_side(side):
        odd = lax.rem(me[1], 2) == 1
        return odd if side > 0 else jnp.logical_not(odd)

    def start_two(copy, way):
        for first in (True, False):
            for d in range(2):
                axis, sign = dirs[d]
                turn = first_side(way * sign)
                turn = turn if first else jnp.logical_not(turn)

                @pl.when(exists(axis, way * sign) & turn)
                def _():
                    copy(d, axis, sign).start()

    def start_rest(copy, way, d):
        axis, sign = dirs[d]

        @pl.when(exists(axis, way * sign))
        def _():
            copy(d, axis, sign).start()

    wait_sphere(barrier, 1)
    for ask in (ask_line, ask_pairs):
        start_two(ask, 1)
        for d in range(2, len(dirs)):
            start_rest(ask, 1, d)

    signal_sphere(near_sem.at[0], radii[0])
    for copy in inputs[3:5]:
        copy.wait()
    cols[0] = column(line_ref)

    codes[len(dirs) :] = jnp.zeros((8 - len(dirs), 128), f32)
    for d, (axis, sign) in enumerate(dirs):

        @pl.when(jnp.logical_not(exists(axis, -sign)))
        def _():
            codes[pl.ds(d, 1), :] = jnp.zeros(code.shape, f32)
            reqs[d] = jnp.zeros(req.shape, f32)

        @pl.when(jnp.logical_not(exists(axis, sign)))
        def _():
            lrecv[d] = jnp.zeros((3, outer, bz), f32)
            for t in range(1, SWEEPS):
                drecv[t, d] = jnp.zeros((outer, pairs), f32)

    def at_lanes(z):
        z = z.astype(jnp.int32)
        return lax.bitwise_and(z, 127), lax.shift_right_arithmetic(z, 7)

    live_rows = lax.broadcasted_iota(jnp.int32, (blocks, pairs), 0) < live_ref[0, 0, 0]
    node_low, node_half = at_lanes(node_ref[0, 0, 0])
    lane_node = lax.broadcasted_iota(jnp.int32, (pairs, 128), 1).astype(f32)
    node_t = jnp.transpose(node_low.astype(f32))
    group = terms.shape[1] // blocks
    terms[...] = jnp.zeros_like(terms)
    for b in range(blocks):
        if b == outer:
            wait_sphere(near_sem.at[0], radii[0])
            if len(radii) > 1:
                signal_sphere(near_sem.at[1], radii[1])
        hot[pl.ds(b * pairs, pairs), :] = jnp.where(
            node_t[:, b : b + 1] == lane_node, 1.0, 0.0
        ).astype(bf16)
    row_line = line_ref[0, 0].astype(f32)
    two[...] = jnp.concatenate([row_line, row_line], axis=1)
    row_mod = lax.broadcasted_iota(jnp.int32, (blocks, blocks), 0)
    col_mod = lax.broadcasted_iota(jnp.int32, (blocks, blocks), 1)
    line_b = cols[0]
    same = line_b[:, :blocks] == row_line
    first_col = 1.0 - jnp.max(
        jnp.where(same & (col_mod < row_mod), 1.0, 0.0), axis=1, keepdims=True
    )

    def cat(parts, axis=0):
        return jnp.concatenate(parts, axis=axis)

    def scatter(values):
        n = len(values)
        for h in range(bz // 128):
            for c in range(n):
                x = jnp.where(node_half == h, values[c], 0.0)
                for j in range(wide):
                    cut = x[:, 128 * j : 128 * (j + 1)]
                    terms[j, pl.ds(h * n + c, blocks, stride=group), :] = cut
        for b in range(blocks):
            slot = cat([terms[j, pl.ds(b * group, group), :] for j in range(wide)], 1)
            both = cat(split(slot, 2))
            both = mm(both, hot[pl.ds(b * pairs, pairs), :])
            sums[pl.ds(b * group, group), :] = both[:group] + both[group:]
        return [
            cat([sums[pl.ds(h * n + c, blocks, stride=group), :] for h in range(bz // 128)], 1)
            for c in range(n)
        ]

    ones = jnp.where(live_rows, 1.0, 0.0)
    counts = scatter([ones, jnp.zeros_like(ones), jnp.zeros_like(ones)])[0].astype(bf16)

    def located(code, zpos, shift):
        e = jnp.floor((code + 0.5) / (by + 2 * RIM))
        f = code - e * (by + 2 * RIM)
        e = e - (RIM + shift[0] * bx)
        f = f - (RIM + shift[1] * by)
        z = zpos - (RIM + shift[2] * bz)
        ok_line = (e >= 0) & (e < bx) & (f >= 0) & (f < by)
        return jnp.where(ok_line, e * by + f, -1.0), z, ok_line & (z >= 0) & (z < bz)

    def setup(row, line, node, geom):
        n = line.shape[0]
        a = jnp.where(line[:, : 2 * blocks] == two[...], 1.0, 0.0).astype(bf16)
        amat[pl.ds(row, n), :] = a
        cinv[pl.ds(row, n), :] = RELAX / (1.0 + mm(a[:, :blocks], counts))
        low, half = at_lanes(node)
        low_ref[pl.ds(row, n), :] = low
        half_ref[pl.ds(row, n), :] = half
        for c in range(3):
            geo[c, pl.ds(row, n), :] = geom[c]

    def fetch(line):
        lane_line = lax.broadcasted_iota(jnp.int32, (line.shape[0], lines), 1).astype(f32)
        own = jnp.where(line == lane_line, 1.0, 0.0).astype(bf16)
        return [sum(mm(own, pos3[c, k]) for k in range(3)) for c in range(3)]

    base = len(dirs) * outer
    rows = base + 2 * blocks
    node = node_ref[0, 0, 0].astype(f32)
    far = farpos_ref[0, 0, 0].astype(f32)
    geom = [geom_ref[0, 0, 0, :, c, :] for c in range(4)]
    line, z, ok = located(cols[1], far, (0, 0, 0))
    setup(
        base,
        cat([line_b, line]),
        cat([node, jnp.where(ok, z, 0.0)]),
        [cat([geom[c], jnp.where(ok, -geom[c], 0.0)]) for c in range(3)],
    )
    inputs[5].wait()
    for c in range(3):
        for k, part in enumerate(split(pos_ref[c].reshape(lines, bz), 3)):
            pos3[c, k] = part
    vals = fetch(cat([line_b, line]))

    for d, (axis, sign) in enumerate(dirs):

        @pl.when(exists(axis, -sign))
        def _():
            ask_line(d, axis, sign).wait_recv()

    shifts = []
    for axis, sign in dirs:
        shifts.append([sign if a == axis else 0 for a in range(3)])
    turned = jnp.transpose(codes[...])[outer:blocks]
    asked = []
    for d in range(len(dirs)):
        there[d] = jnp.broadcast_to(turned[:, d : d + 1], (outer, pairs))
        asked.append(located(there[d], 0.0, shifts[d])[0])
    back = fetch(cat(asked))
    for d in range(len(dirs)):
        for c in range(3):
            lsend[d, c] = back[c][d * outer : (d + 1) * outer]
    for d, (axis, sign) in enumerate(dirs):

        @pl.when(exists(axis, sign))
        def _():
            ask_line(d, axis, sign).wait_send()

    start_two(line_back, -1)
    for d in range(2, len(dirs)):
        start_rest(line_back, -1, d)

    for i, r in enumerate(radii[1:], 1):
        wait_sphere(near_sem.at[i], r)
        if i + 1 < len(radii):
            signal_sphere(near_sem.at[i + 1], radii[i + 1])
    for k in range(1, nx):
        to = (ids[0][k], me[1], me[2])
        pl.semaphore_signal(whole_sem, inc=1, device_id=to, device_id_type=MESH)

    start = take_lanes([v[:blocks] for v in vals], *at_lanes(node))
    inner = take_lanes([v[blocks : blocks + outer] for v in vals], *at_lanes(z[:outer]))
    gap[...] = sum(geom[c] * start[c] for c in range(3)) - geom[3]
    gap[0:outer, :] = gap[0:outer, :] - sum(geom[c][:outer] * inner[c] for c in range(3))

    for d, (axis, sign) in enumerate(dirs):

        @pl.when(exists(axis, -sign))
        def _():
            ask_pairs(d, axis, sign).wait_recv()

    pairs_in = []
    for d in range(len(dirs)):
        got = [
            jnp.concatenate([reqs[d, c * wide + h] for h in range(wide)], axis=1) for c in range(4)
        ]
        _, at, ok = located(there[d], got[3], shifts[d])
        pairs_in.append([jnp.where(ok, at, 0.0)] + [jnp.where(ok, -got[c], 0.0) for c in range(3)])
    pairs_in = [cat([x[i] for x in pairs_in]) for i in range(4)]
    setup(0, cat(asked), pairs_in[0], pairs_in[1:])

    for d, (axis, sign) in enumerate(dirs):

        @pl.when(exists(axis, sign))
        def _():
            line_back(d, axis, sign).wait_recv()

    low, half = at_lanes(far[outer:] - RIM)
    reach = []
    for c in range(3):
        line = vals[c][blocks + outer :]
        for d, (axis, sign) in enumerate(dirs):
            if axis < 2:
                line = line + lrecv[d, c]
        below = lrecv[dirs.index((2, -1)), c][:, bz - 128 :]
        above = lrecv[dirs.index((2, 1)), c][:, :128]
        reach.append(jnp.concatenate([below, line, above], axis=1))
    reach = take_lanes(reach, low, half + 1)
    if nx > 1:
        pl.semaphore_wait(whole_sem, nx - 1)
    gap[pl.ds(outer, outer), :] = gap[pl.ds(outer, outer), :] - sum(
        geom[c][outer:] * reach[c] for c in range(3)
    )
    for d, (axis, sign) in enumerate(dirs):

        @pl.when(exists(axis, sign))
        def _():
            ask_pairs(d, axis, sign).wait_send()

        @pl.when(exists(axis, -sign))
        def _():
            line_back(d, axis, sign).wait_send()

    def respond(t, total):
        send = functools.partial(answer, t)
        for d in range(len(dirs)):
            dsend[t, d] = total(d * outer, outer)
            if d == 1:
                start_two(send, -1)
            if d > 1:
                start_rest(send, -1, d)

    def responded(t):
        for d, (axis, sign) in enumerate(dirs):

            @pl.when(exists(axis, -sign))
            def _():
                answer(t, d, axis, sign).wait_send()

    def received(t):
        for d, (axis, sign) in enumerate(dirs):

            @pl.when(exists(axis, sign))
            def _():
                answer(t, d, axis, sign).wait_recv()

        got = drecv[t, 0]
        for d in range(1, len(dirs)):
            got = got + drecv[t, d]
        return got

    acc_ref[...] = jnp.zeros_like(acc_ref)

    def to_all(ref, send_sem, recv_sem):
        def send(to):
            pltpu.make_async_remote_copy(
                src_ref=ref,
                dst_ref=ref,
                send_sem=send_sem,
                recv_sem=recv_sem,
                device_id=to,
                device_id_type=MESH,
            ).start()

        if devices <= 32:
            for a in range(nx):
                for b in range(ny):
                    for c in range(nz):
                        if a or b or c:
                            send((ids[0][a], ids[1][b], ids[2][c]))
        else:

            def step(k, carry):
                send(coords(k))
                return carry

            lax.fori_loop(1, devices, step, 0)

    def lanes_sum(x):
        x = jnp.sum(x, axis=0, keepdims=True)
        out = x[:, :128]
        for j in range(1, x.shape[1] // 128):
            out = out + x[:, 128 * j : 128 * (j + 1)]
        return out

    lane = lax.broadcasted_iota(jnp.int32, (1, 128), 1)
    at_line = lax.broadcasted_iota(jnp.int32, (lines, 2 * blocks), 0).astype(f32)
    place = jnp.where(at_line == two[...], 1.0, 0.0).astype(bf16)

    def placed(x):
        return mm(place, cat(split(x, 2)))

    def apply(row, n, parts):
        both = mm(amat[row : row + n, :], parts)
        return [both[:, c * bz : (c + 1) * bz] * cinv[row : row + n, :] for c in range(3)]

    def dots(row, n, moved):
        low = low_ref[row : row + n, :]
        half = half_ref[row : row + n, :]
        got = take_lanes(moved, low, half)
        return sum(geo[c, row : row + n] * got[c] for c in range(3))

    def wait_all(ref, sem):
        others = ref.at[pl.ds(0, devices - 1)]
        pltpu.make_async_copy(others, others, sem).wait()

    def settle(scale):
        acc_ref[...] = acc_ref[...] + (scale * first_col) * near_ref[...]

    rrecv[mine] = jnp.zeros((1, 128), f32)
    energies, scales = [], []
    for t in range(SWEEPS):
        last, slot = t == SWEEPS - 1, t % 2
        depth = jnp.where(live_rows, jnp.maximum(-gap[...], 0.0), 0.0)
        erecv[t, mine] = lanes_sum(depth * depth)
        to_all(erecv.at[t, mine], es_sem.at[slot], er_sem.at[slot])
        own = scatter([depth * geo[c, base : base + blocks] for c in range(3)])
        parts = cat(split(cat(own, 1), 2))
        if t:
            wait_all(erecv.at[t - 1], es_sem.at[1 - slot])
            responded(t)
            settle(scales[-1])
        if not last:
            far = apply(0, base, parts)
            respond(t + 1, lambda row, n: dots(row, n, [m[row : row + n] for m in far]))
        moved = apply(base, blocks if last else 2 * blocks, parts)
        near = cat([m[:blocks] for m in moved], 1)
        near_ref[...] = near
        resid = jnp.sum(lanes_sum(near * near * first_col), axis=1, keepdims=True)
        rrecv[mine] = jnp.where(lane == t, resid, rrecv[mine])
        if last:
            to_all(rrecv.at[mine], es_sem.at[2], er_sem.at[2])
            for c in range(3):
                cut = slice(c * bz, (c + 1) * bz)
                done = placed(acc_ref[:, cut])
                out_ref[c] = pos_ref[c] + done.reshape(bx, by, bz)
                step_ref[c] = placed(first_col * near[:, cut]).reshape(bx, by, bz)
        else:
            step = dots(base, 2 * blocks, moved)
            step = step[:blocks] + step[blocks:]
            more = received(t + 1)
        wait_all(erecv.at[t], er_sem.at[slot])
        energy = jnp.sum(jnp.sum(erecv[t], axis=0), axis=1, keepdims=True)
        scale = 1.0 / (1.0 + energy / (blocks * pairs * devices))
        energies.append(energy)
        scales.append(scale)
        if last:
            for c in range(3):
                out_ref[c] = out_ref[c] + scale[:, :, None] * step_ref[c]
        else:
            gap[0:outer, :] = gap[0:outer, :] + scale * step[:outer]
            gap[pl.ds(outer, outer), :] = gap[pl.ds(outer, outer), :] + scale * (
                step[outer:] + more
            )

    wait_all(erecv.at[SWEEPS - 1], es_sem.at[(SWEEPS - 1) % 2])
    energy, scale = jnp.zeros((1, 128), f32), jnp.zeros((1, 128), f32)
    for t in range(SWEEPS):
        energy = jnp.where(lane == t, energies[t], energy)
        scale = jnp.where(lane == t, scales[t], scale)
    hist_out[0:1, :] = jnp.sqrt(1.0 + energy / (blocks * pairs))[:, :SWEEPS]
    factor = scale * scale / (bx * by * bz)
    wait_all(rrecv, er_sem.at[2])
    resid = factor * jnp.sum(rrecv[...], axis=0)
    hist_out[1:2, :] = jnp.sqrt(1.0 + resid)[:, :SWEEPS]
    wait_all(rrecv, es_sem.at[2])


def finish(pos_ref, hist_ref, pos_out, hist_out, sem):
    copies = [
        pltpu.make_async_copy(pos_ref, pos_out, sem.at[0]),
        pltpu.make_async_copy(hist_ref, hist_out, sem.at[1]),
    ]
    for copy in copies:
        copy.start()
    for copy in copies:
        copy.wait()


def local(sizes, positions, pair_node, pair_line, pair_far, far_line, pair_geom, live_blocks):
    blocks, pairs = pair_node.shape[3:]
    blk = positions.shape[1:]
    devices = sizes[0] * sizes[1] * sizes[2]
    outer = blocks // 2
    rows = 2 * blocks + 6 * outer
    group = -(-3 * (blk[2] // 128) // 8) * 8
    dma = pltpu.SemaphoreType.DMA
    vmem = pl.BlockSpec(memory_space=pltpu.VMEM)
    moved, hist = pl.pallas_call(
        functools.partial(kernel, sizes, blk),
        out_shape=(
            pltpu.VMEM(positions.shape, f32),
            pltpu.VMEM((2, SWEEPS), f32),
        ),
        in_specs=[pl.BlockSpec(memory_space=pltpu.SMEM)]
        + [pl.BlockSpec(memory_space=pltpu.HBM)] * 6,
        out_specs=(vmem, vmem),
        scratch_shapes=[
            pltpu.VMEM(pair_node.shape, jnp.int32),
            pltpu.VMEM(pair_line.shape, jnp.int32),
            pltpu.VMEM(pair_far.shape, jnp.int32),
            pltpu.VMEM(far_line.shape, jnp.int32),
            pltpu.VMEM(pair_geom.shape, f32),
            pltpu.VMEM(positions.shape, f32),
            pltpu.VMEM((blocks, 3 * blk[2]), f32),
            pltpu.VMEM((blocks, 3 * blk[2]), f32),
            pltpu.VMEM(positions.shape, f32),
            pltpu.VMEM((3, 3, blk[0] * blk[1], blk[2]), bf16),
            pltpu.VMEM((1, 128), f32),
            pltpu.VMEM((8, 128), f32),
            pltpu.VMEM((6, outer, pairs), f32),
            pltpu.VMEM((6, 3, outer, blk[2]), f32),
            pltpu.VMEM((6, 3, outer, blk[2]), f32),
            pltpu.VMEM((4 * (pairs // 128), outer, 128), f32),
            pltpu.VMEM((2, blocks, pairs), f32),
            pltpu.VMEM((blocks * pairs, 128), bf16),
            pltpu.VMEM((1, 2 * blocks), f32),
            pltpu.VMEM((rows, 2 * blocks), bf16),
            pltpu.VMEM((rows, pairs), f32),
            pltpu.VMEM((3, rows, pairs), f32),
            pltpu.VMEM((rows, pairs), jnp.int32),
            pltpu.VMEM((rows, pairs), jnp.int32),
            pltpu.VMEM((blocks, pairs), f32),
            pltpu.VMEM((pairs // 128, blocks * group, 128), f32),
            pltpu.VMEM((blocks * group, 128), f32),
            pltpu.VMEM((6, 4 * (pairs // 128), outer, 128), f32),
            pltpu.VMEM((SWEEPS, 6, outer, pairs), f32),
            pltpu.VMEM((SWEEPS, 6, outer, pairs), f32),
            pltpu.VMEM((SWEEPS, devices, 1, 128), f32),
            pltpu.VMEM((devices, 1, 128), f32),
            pltpu.SemaphoreType.REGULAR((len(near_radii(sizes)),)),
            pltpu.SemaphoreType.REGULAR,
            dma((2, 6)),
            dma((3, 6)),
            dma((3,)),
            dma((3,)),
        ],
        compiler_params=pltpu.CompilerParams(
            collective_id=0, has_side_effects=True, vmem_limit_bytes=40 << 20
        ),
    )(
        live_blocks,
        *[
            pltpu.with_memory_space_constraint(x, pltpu.HBM)
            for x in (
                pair_node,
                pair_line,
                pair_far,
                far_line,
                pair_geom,
                positions,
            )
        ]
    )
    return pl.pallas_call(
        finish,
        out_shape=(
            jax.ShapeDtypeStruct(positions.shape, f32),
            jax.ShapeDtypeStruct((2, SWEEPS), f32),
        ),
        in_specs=[vmem] * 2,
        out_specs=[pl.BlockSpec(memory_space=pl.ANY)] * 2,
        scratch_shapes=[dma((2,))],
        compiler_params=pltpu.CompilerParams(vmem_limit_bytes=1 << 20),
    )(moved, hist)


def solution(mesh):
    sizes = tuple(mesh.shape[a] for a in AXES)
    return jax.shard_map(
        functools.partial(local, sizes),
        mesh=mesh,
        in_specs=(
            P(None, "gx", "gy", "gz"),
            P("gx", "gy", "gz", None, None),
            P("gx", "gy", "gz", None),
            P("gx", "gy", "gz", None, None),
            P("gx", "gy", "gz", None),
            P("gx", "gy", "gz", None, None, None),
            P("gx", "gy", "gz"),
        ),
        out_specs=(P(None, "gx", "gy", "gz"), P()),
        check_vma=False,
    )
```

```python
import functools
import itertools

import jax
import jax.numpy as jnp
from jax import lax
from jax.experimental import pallas as pl
from jax.experimental.pallas import tpu as pltpu
from jax.sharding import PartitionSpec as P

RIM = 3
SWEEPS = 5
RELAX = 0.9
AXES = ("gx", "gy", "gz")
MESH = pl.DeviceIdType.MESH
f32 = jnp.float32
bf16 = jnp.bfloat16


def split(x, parts):
    out = []
    for _ in range(parts - 1):
        hi = x.astype(bf16)
        out.append(hi)
        x = x - hi.astype(f32)
    out.append(x.astype(bf16))
    return out


def mm(a, b):
    return jnp.dot(a, b, preferred_element_type=f32)


def near_radii(sizes):
    need = max(sizes[0] - 1, sizes[1] + sizes[2] - 2)
    radii = [1]
    while 2 * radii[-1] < need:
        radii.append(2 * radii[-1])
    return radii


def take_lanes(xs, low, half):
    outs = [[] for _ in xs]
    for h in range(0, low.shape[1], 128):
        idx = low[:, h : h + 128]
        got = [None] * len(xs)
        for j in range(xs[0].shape[1] // 128):
            for i, x in enumerate(xs):
                more = jnp.take_along_axis(
                    x[:, 128 * j : 128 * (j + 1)], idx, axis=1, mode="promise_in_bounds"
                )
                got[i] = jnp.where(half[:, h : h + 128] == j, more, got[i]) if j else more
        for out, x in zip(outs, got):
            out.append(x)
    return [jnp.concatenate(out, axis=1) for out in outs]


def kernel(
    sizes,
    blk,
    live_ref,
    node_hbm,
    line_hbm,
    farpos_hbm,
    farline_hbm,
    geom_hbm,
    pos_hbm,
    out_ref,
    hist_out,
    node_ref,
    line_ref,
    farpos_ref,
    farline_ref,
    geom_ref,
    pos_ref,
    acc_ref,
    near_ref,
    step_ref,
    pos3,
    code,
    codes,
    there,
    lsend,
    lrecv,
    req,
    cols,
    hot,
    two,
    amat,
    cinv,
    geo,
    low_ref,
    half_ref,
    gap,
    terms,
    sums,
    reqs,
    dsend,
    drecv,
    erecv,
    rrecv,
    near_sem,
    whole_sem,
    ds_sem,
    dr_sem,
    es_sem,
    er_sem,
):
    nx, ny, nz = sizes
    bx, by, bz = blk
    devices = nx * ny * nz
    blocks, pairs = gap.shape
    outer = blocks // 2
    lines = bx * by
    me = [lax.axis_index(a) for a in AXES]
    mine = (me[0] * ny + me[1]) * nz + me[2]
    dirs = [(a, s) for a in (1, 0, 2) for s in (1, -1)]

    def neighbour(axis, sign):
        to = list(me)
        to[axis] = lax.rem(me[axis] + sign + sizes[axis], sizes[axis])
        return tuple(to)

    def exists(axis, sign):
        return (me[axis] + sign >= 0) & (me[axis] + sign < sizes[axis])

    def coords(k):
        to = lax.rem(mine + k, devices)
        return (to // (ny * nz), lax.rem(to // nz, ny), lax.rem(to, nz))

    def moved_by(axis, k):
        if sizes[axis] & (sizes[axis] - 1) == 0:
            return lax.bitwise_xor(me[axis], k)
        to = me[axis] + k
        return jnp.where(to >= sizes[axis], to - sizes[axis], to)

    ids = [[moved_by(a, k) for k in range(sizes[a])] for a in range(3)]

    def sphere(r):
        steps = itertools.product(*[range(1 - n, n) for n in sizes])
        return [s for s in steps if sum(abs(x) for x in s) == r]

    def inside(step):
        ok = True
        for x, n, at in zip(step, sizes, me):
            if x > 0:
                ok = ok & (at < n - x)
            if x < 0:
                ok = ok & (at >= -x)
        return ok

    def signal_sphere(sem, r):
        for step in sphere(r):

            @pl.when(inside(step))
            def _():
                to = tuple(at + x for at, x in zip(me, step))
                pl.semaphore_signal(sem, inc=1, device_id=to, device_id_type=MESH)

    def wait_sphere(sem, r):
        pl.semaphore_wait(sem, sum(jnp.where(inside(s), 1, 0) for s in sphere(r)))

    radii = near_radii(sizes)
    barrier = pltpu.get_barrier_semaphore()
    signal_sphere(barrier, 1)
    inputs = [
        pltpu.make_async_copy(*copy)
        for copy in [
            (farline_hbm, farline_ref, ds_sem.at[0]),
            (farpos_hbm, farpos_ref, ds_sem.at[1]),
            (geom_hbm, geom_ref, es_sem.at[0]),
            (node_hbm, node_ref, es_sem.at[1]),
            (line_hbm, line_ref, es_sem.at[2]),
            (pos_hbm, pos_ref, ds_sem.at[2]),
        ]
    ]
    for copy in inputs:
        copy.start()
    for copy in inputs[:3]:
        copy.wait()

    def column(ref):
        row = ref[0, 0].astype(f32)
        return jnp.transpose(jnp.broadcast_to(row, (pairs, blocks)))

    wide = pairs // 128
    planes = [geom_ref[0, 0, 0, outer:, c, :] for c in range(3)]
    planes.append(farpos_ref[0, 0, 0, outer:, :].astype(f32))
    for c in range(4):
        for h in range(wide):
            req[c * wide + h] = planes[c][:, 128 * h : 128 * (h + 1)]
    cols[1] = column(farline_ref)
    row = farline_ref[0, 0].astype(f32)
    code[...] = jnp.concatenate([row] * (128 // blocks), axis=1)

    def remote(src, dst, send_sem, recv_sem, to):
        return pltpu.make_async_remote_copy(
            src_ref=src,
            dst_ref=dst,
            send_sem=send_sem,
            recv_sem=recv_sem,
            device_id=neighbour(*to),
            device_id_type=MESH,
        )

    def ask_line(d, axis, sign):
        return remote(code, codes.at[pl.ds(d, 1), :], ds_sem.at[1], dr_sem.at[1], (axis, sign))

    def ask_pairs(d, axis, sign):
        return remote(req, reqs.at[d], ds_sem.at[0], dr_sem.at[2], (axis, sign))

    def line_back(d, axis, sign):
        return remote(lsend.at[d], lrecv.at[d], ds_sem.at[1], dr_sem.at[0], (axis, -sign))

    def answer(t, d, axis, sign):
        sems = ds_sem.at[t % 2], dr_sem.at[t % 2]
        return remote(dsend.at[t, d], drecv.at[t, d], *sems, (axis, -sign))

    count = sum(jnp.where(exists(axis, sign), 1, 0) for axis, sign in dirs)

    def wait_each(ref, sem):
        for k in range(1, len(dirs) + 1):

            @pl.when(count == k)
            def _():
                some = ref.at[pl.ds(0, k)]
                pltpu.make_async_copy(some, some, sem).wait()

    def first_side(side):
        odd = lax.rem(me[1], 2) == 1
        return odd if side > 0 else jnp.logical_not(odd)

    def start_two(copy, way):
        for first in (True, False):
            for d in range(2):
                axis, sign = dirs[d]
                turn = first_side(way * sign)
                turn = turn if first else jnp.logical_not(turn)

                @pl.when(exists(axis, way * sign) & turn)
                def _():
                    copy(d, axis, sign).start()

    def start_rest(copy, way, d):
        axis, sign = dirs[d]

        @pl.when(exists(axis, way * sign))
        def _():
            copy(d, axis, sign).start()

    wait_sphere(barrier, 1)
    for ask in (ask_line, ask_pairs):
        start_two(ask, 1)
        for d in range(2, len(dirs)):
            start_rest(ask, 1, d)

    signal_sphere(near_sem.at[0], radii[0])
    for copy in inputs[3:5]:
        copy.wait()
    cols[0] = column(line_ref)

    codes[len(dirs) :] = jnp.zeros((8 - len(dirs), 128), f32)
    for d, (axis, sign) in enumerate(dirs):

        @pl.when(jnp.logical_not(exists(axis, -sign)))
        def _():
            codes[pl.ds(d, 1), :] = jnp.zeros(code.shape, f32)
            reqs[d] = jnp.zeros(req.shape, f32)

        @pl.when(jnp.logical_not(exists(axis, sign)))
        def _():
            lrecv[d] = jnp.zeros((3, outer, bz), f32)
            for t in range(1, SWEEPS):
                drecv[t, d] = jnp.zeros((outer, pairs), f32)

    def at_lanes(z):
        z = z.astype(jnp.int32)
        return lax.bitwise_and(z, 127), lax.shift_right_arithmetic(z, 7)

    live_rows = lax.broadcasted_iota(jnp.int32, (blocks, pairs), 0) < live_ref[0, 0, 0]
    node_low, node_half = at_lanes(node_ref[0, 0, 0])
    lane_node = lax.broadcasted_iota(jnp.int32, (pairs, 128), 1).astype(f32)
    node_t = jnp.transpose(node_low.astype(f32))
    group = terms.shape[1] // blocks
    terms[...] = jnp.zeros_like(terms)
    for b in range(blocks):
        if b == outer:
            wait_sphere(near_sem.at[0], radii[0])
            if len(radii) > 1:
                signal_sphere(near_sem.at[1], radii[1])
        hot[pl.ds(b * pairs, pairs), :] = jnp.where(
            node_t[:, b : b + 1] == lane_node, 1.0, 0.0
        ).astype(bf16)
    row_line = line_ref[0, 0].astype(f32)
    two[...] = jnp.concatenate([row_line, row_line], axis=1)
    row_mod = lax.broadcasted_iota(jnp.int32, (blocks, blocks), 0)
    col_mod = lax.broadcasted_iota(jnp.int32, (blocks, blocks), 1)
    line_b = cols[0]
    same = line_b[:, :blocks] == row_line
    first_col = 1.0 - jnp.max(
        jnp.where(same & (col_mod < row_mod), 1.0, 0.0), axis=1, keepdims=True
    )

    def cat(parts, axis=0):
        return jnp.concatenate(parts, axis=axis)

    def scatter(values):
        n = len(values)
        for h in range(bz // 128):
            for c in range(n):
                x = jnp.where(node_half == h, values[c], 0.0)
                for j in range(wide):
                    cut = x[:, 128 * j : 128 * (j + 1)]
                    terms[j, pl.ds(h * n + c, blocks, stride=group), :] = cut
        for b in range(blocks):
            slot = cat([terms[j, pl.ds(b * group, group), :] for j in range(wide)], 1)
            both = cat(split(slot, 2))
            both = mm(both, hot[pl.ds(b * pairs, pairs), :])
            sums[pl.ds(b * group, group), :] = both[:group] + both[group:]
        return [
            cat([sums[pl.ds(h * n + c, blocks, stride=group), :] for h in range(bz // 128)], 1)
            for c in range(n)
        ]

    ones = jnp.where(live_rows, 1.0, 0.0)
    counts = scatter([ones, jnp.zeros_like(ones), jnp.zeros_like(ones)])[0].astype(bf16)

    def located(code, zpos, shift):
        e = jnp.floor((code + 0.5) / (by + 2 * RIM))
        f = code - e * (by + 2 * RIM)
        e = e - (RIM + shift[0] * bx)
        f = f - (RIM + shift[1] * by)
        z = zpos - (RIM + shift[2] * bz)
        ok_line = (e >= 0) & (e < bx) & (f >= 0) & (f < by)
        return jnp.where(ok_line, e * by + f, -1.0), z, ok_line & (z >= 0) & (z < bz)

    def setup(row, line, node, geom):
        n = line.shape[0]
        a = jnp.where(line[:, : 2 * blocks] == two[...], 1.0, 0.0).astype(bf16)
        amat[pl.ds(row, n), :] = a
        cinv[pl.ds(row, n), :] = RELAX / (1.0 + mm(a[:, :blocks], counts))
        low, half = at_lanes(node)
        low_ref[pl.ds(row, n), :] = low
        half_ref[pl.ds(row, n), :] = half
        for c in range(3):
            geo[c, pl.ds(row, n), :] = geom[c]

    def fetch(line):
        lane_line = lax.broadcasted_iota(jnp.int32, (line.shape[0], lines), 1).astype(f32)
        own = jnp.where(line == lane_line, 1.0, 0.0).astype(bf16)
        return [sum(mm(own, pos3[c, k]) for k in range(3)) for c in range(3)]

    base = len(dirs) * outer
    rows = base + 2 * blocks
    node = node_ref[0, 0, 0].astype(f32)
    far = farpos_ref[0, 0, 0].astype(f32)
    geom = [geom_ref[0, 0, 0, :, c, :] for c in range(4)]
    line, z, ok = located(cols[1], far, (0, 0, 0))
    setup(
        base,
        cat([line_b, line]),
        cat([node, jnp.where(ok, z, 0.0)]),
        [cat([geom[c], jnp.where(ok, -geom[c], 0.0)]) for c in range(3)],
    )
    inputs[5].wait()
    for c in range(3):
        for k, part in enumerate(split(pos_ref[c].reshape(lines, bz), 3)):
            pos3[c, k] = part
    vals = fetch(cat([line_b, line]))

    wait_each(codes, dr_sem.at[1])
    shifts = []
    for axis, sign in dirs:
        shifts.append([sign if a == axis else 0 for a in range(3)])
    turned = jnp.transpose(codes[...])[outer:blocks]
    asked = []
    for d in range(len(dirs)):
        there[d] = jnp.broadcast_to(turned[:, d : d + 1], (outer, pairs))
        asked.append(located(there[d], 0.0, shifts[d])[0])
    back = fetch(cat(asked))
    for d in range(len(dirs)):
        for c in range(3):
            lsend[d, c] = back[c][d * outer : (d + 1) * outer]
    wait_each(codes, ds_sem.at[1])
    start_two(line_back, -1)
    for d in range(2, len(dirs)):
        start_rest(line_back, -1, d)

    for i, r in enumerate(radii[1:], 1):
        wait_sphere(near_sem.at[i], r)
        if i + 1 < len(radii):
            signal_sphere(near_sem.at[i + 1], radii[i + 1])
    for k in range(1, nx):
        to = (ids[0][k], me[1], me[2])
        pl.semaphore_signal(whole_sem, inc=1, device_id=to, device_id_type=MESH)

    start = take_lanes([v[:blocks] for v in vals], *at_lanes(node))
    inner = take_lanes([v[blocks : blocks + outer] for v in vals], *at_lanes(z[:outer]))
    gap[...] = sum(geom[c] * start[c] for c in range(3)) - geom[3]
    gap[0:outer, :] = gap[0:outer, :] - sum(geom[c][:outer] * inner[c] for c in range(3))

    wait_each(reqs, dr_sem.at[2])
    pairs_in = []
    for d in range(len(dirs)):
        got = [
            jnp.concatenate([reqs[d, c * wide + h] for h in range(wide)], axis=1) for c in range(4)
        ]
        _, at, ok = located(there[d], got[3], shifts[d])
        pairs_in.append([jnp.where(ok, at, 0.0)] + [jnp.where(ok, -got[c], 0.0) for c in range(3)])
    pairs_in = [cat([x[i] for x in pairs_in]) for i in range(4)]
    setup(0, cat(asked), pairs_in[0], pairs_in[1:])

    wait_each(lrecv, dr_sem.at[0])
    low, half = at_lanes(far[outer:] - RIM)
    reach = []
    for c in range(3):
        line = vals[c][blocks + outer :]
        for d, (axis, sign) in enumerate(dirs):
            if axis < 2:
                line = line + lrecv[d, c]
        below = lrecv[dirs.index((2, -1)), c][:, bz - 128 :]
        above = lrecv[dirs.index((2, 1)), c][:, :128]
        reach.append(jnp.concatenate([below, line, above], axis=1))
    reach = take_lanes(reach, low, half + 1)
    if nx > 1:
        pl.semaphore_wait(whole_sem, nx - 1)
    gap[pl.ds(outer, outer), :] = gap[pl.ds(outer, outer), :] - sum(
        geom[c][outer:] * reach[c] for c in range(3)
    )
    def respond(t, total):
        send = functools.partial(answer, t)
        for d in range(len(dirs)):
            dsend[t, d] = total(d * outer, outer)
            if d == 1:
                start_two(send, -1)
            if d > 1:
                start_rest(send, -1, d)

    def responded(t):
        wait_each(dsend.at[t], ds_sem.at[t % 2])

    def received(t):
        wait_each(drecv.at[t], dr_sem.at[t % 2])
        got = drecv[t, 0]
        for d in range(1, len(dirs)):
            got = got + drecv[t, d]
        return got

    acc_ref[...] = jnp.zeros_like(acc_ref)

    def to_all(ref, send_sem, recv_sem):
        def send(to):
            pltpu.make_async_remote_copy(
                src_ref=ref,
                dst_ref=ref,
                send_sem=send_sem,
                recv_sem=recv_sem,
                device_id=to,
                device_id_type=MESH,
            ).start()

        if devices <= 32:
            for a in reversed(range(nx)):
                for b in reversed(range(ny)):
                    for c in range(nz):
                        if a or b or c:
                            send((ids[0][a], ids[1][b], ids[2][c]))
        else:

            def step(k, carry):
                send(coords(k))
                return carry

            lax.fori_loop(1, devices, step, 0)

    def lanes_sum(x):
        x = jnp.sum(x, axis=0, keepdims=True)
        out = x[:, :128]
        for j in range(1, x.shape[1] // 128):
            out = out + x[:, 128 * j : 128 * (j + 1)]
        return out

    lane = lax.broadcasted_iota(jnp.int32, (1, 128), 1)
    at_line = lax.broadcasted_iota(jnp.int32, (lines, 2 * blocks), 0).astype(f32)
    place = jnp.where(at_line == two[...], 1.0, 0.0).astype(bf16)

    def placed(x):
        return mm(place, cat(split(x, 2)))

    def apply(row, n, parts):
        both = mm(amat[row : row + n, :], parts)
        return [both[:, c * bz : (c + 1) * bz] * cinv[row : row + n, :] for c in range(3)]

    def dots(row, n, moved):
        low = low_ref[row : row + n, :]
        half = half_ref[row : row + n, :]
        got = take_lanes(moved, low, half)
        return sum(geo[c, row : row + n] * got[c] for c in range(3))

    def wait_all(ref, sem):
        others = ref.at[pl.ds(0, devices - 1)]
        pltpu.make_async_copy(others, others, sem).wait()

    def settle(scale):
        acc_ref[...] = acc_ref[...] + (scale * first_col) * near_ref[...]

    rrecv[mine] = jnp.zeros((1, 128), f32)
    energies, scales = [], []
    for t in range(SWEEPS):
        last, slot = t == SWEEPS - 1, t % 2
        depth = jnp.where(live_rows, jnp.maximum(-gap[...], 0.0), 0.0)
        erecv[t, mine] = lanes_sum(depth * depth)
        to_all(erecv.at[t, mine], es_sem.at[slot], er_sem.at[slot])
        own = scatter([depth * geo[c, base : base + blocks] for c in range(3)])
        parts = cat(split(cat(own, 1), 2))
        if not t:
            wait_each(lrecv, ds_sem.at[1])
        if not last:
            far = apply(0, base, parts)
            respond(t + 1, lambda row, n: dots(row, n, [m[row : row + n] for m in far]))
        moved = apply(base, blocks if last else 2 * blocks, parts)
        near = cat([m[:blocks] for m in moved], 1)
        resid = jnp.sum(lanes_sum(near * near * first_col), axis=1, keepdims=True)
        rrecv[mine] = jnp.where(lane == t, resid, rrecv[mine])
        if last:
            to_all(rrecv.at[mine], es_sem.at[2], er_sem.at[2])
        if t:
            wait_all(erecv.at[t - 1], es_sem.at[1 - slot])
            responded(t)
            settle(scales[-1])
        else:
            wait_each(reqs, ds_sem.at[0])
        near_ref[...] = near
        if last:
            for c in range(3):
                cut = slice(c * bz, (c + 1) * bz)
                done = placed(acc_ref[:, cut])
                out_ref[c] = pos_ref[c] + done.reshape(bx, by, bz)
                step_ref[c] = placed(first_col * near[:, cut]).reshape(bx, by, bz)
        else:
            step = dots(base, 2 * blocks, moved)
            step = step[:blocks] + step[blocks:]
            more = received(t + 1)
        wait_all(erecv.at[t], er_sem.at[slot])
        energy = jnp.sum(jnp.sum(erecv[t], axis=0), axis=1, keepdims=True)
        scale = 1.0 / (1.0 + energy / (blocks * pairs * devices))
        energies.append(energy)
        scales.append(scale)
        if last:
            for c in range(3):
                out_ref[c] = out_ref[c] + scale[:, :, None] * step_ref[c]
        else:
            gap[0:outer, :] = gap[0:outer, :] + scale * step[:outer]
            gap[pl.ds(outer, outer), :] = gap[pl.ds(outer, outer), :] + scale * (
                step[outer:] + more
            )

    wait_all(erecv.at[SWEEPS - 1], es_sem.at[(SWEEPS - 1) % 2])
    energy, scale = jnp.zeros((1, 128), f32), jnp.zeros((1, 128), f32)
    for t in range(SWEEPS):
        energy = jnp.where(lane == t, energies[t], energy)
        scale = jnp.where(lane == t, scales[t], scale)
    hist_out[0:1, :] = jnp.sqrt(1.0 + energy / (blocks * pairs))[:, :SWEEPS]
    factor = scale * scale / (bx * by * bz)
    wait_all(rrecv, er_sem.at[2])
    resid = factor * jnp.sum(rrecv[...], axis=0)
    hist_out[1:2, :] = jnp.sqrt(1.0 + resid)[:, :SWEEPS]
    wait_all(rrecv, es_sem.at[2])


def finish(pos_ref, hist_ref, pos_out, hist_out, sem):
    copies = [
        pltpu.make_async_copy(pos_ref, pos_out, sem.at[0]),
        pltpu.make_async_copy(hist_ref, hist_out, sem.at[1]),
    ]
    for copy in copies:
        copy.start()
    for copy in copies:
        copy.wait()


def local(sizes, positions, pair_node, pair_line, pair_far, far_line, pair_geom, live_blocks):
    blocks, pairs = pair_node.shape[3:]
    blk = positions.shape[1:]
    devices = sizes[0] * sizes[1] * sizes[2]
    outer = blocks // 2
    rows = 2 * blocks + 6 * outer
    group = -(-3 * (blk[2] // 128) // 8) * 8
    dma = pltpu.SemaphoreType.DMA
    vmem = pl.BlockSpec(memory_space=pltpu.VMEM)
    moved, hist = pl.pallas_call(
        functools.partial(kernel, sizes, blk),
        out_shape=(
            pltpu.VMEM(positions.shape, f32),
            pltpu.VMEM((2, SWEEPS), f32),
        ),
        in_specs=[pl.BlockSpec(memory_space=pltpu.SMEM)]
        + [pl.BlockSpec(memory_space=pltpu.HBM)] * 6,
        out_specs=(vmem, vmem),
        scratch_shapes=[
            pltpu.VMEM(pair_node.shape, jnp.int32),
            pltpu.VMEM(pair_line.shape, jnp.int32),
            pltpu.VMEM(pair_far.shape, jnp.int32),
            pltpu.VMEM(far_line.shape, jnp.int32),
            pltpu.VMEM(pair_geom.shape, f32),
            pltpu.VMEM(positions.shape, f32),
            pltpu.VMEM((blocks, 3 * blk[2]), f32),
            pltpu.VMEM((blocks, 3 * blk[2]), f32),
            pltpu.VMEM(positions.shape, f32),
            pltpu.VMEM((3, 3, blk[0] * blk[1], blk[2]), bf16),
            pltpu.VMEM((1, 128), f32),
            pltpu.VMEM((8, 128), f32),
            pltpu.VMEM((6, outer, pairs), f32),
            pltpu.VMEM((6, 3, outer, blk[2]), f32),
            pltpu.VMEM((6, 3, outer, blk[2]), f32),
            pltpu.VMEM((4 * (pairs // 128), outer, 128), f32),
            pltpu.VMEM((2, blocks, pairs), f32),
            pltpu.VMEM((blocks * pairs, 128), bf16),
            pltpu.VMEM((1, 2 * blocks), f32),
            pltpu.VMEM((rows, 2 * blocks), bf16),
            pltpu.VMEM((rows, pairs), f32),
            pltpu.VMEM((3, rows, pairs), f32),
            pltpu.VMEM((rows, pairs), jnp.int32),
            pltpu.VMEM((rows, pairs), jnp.int32),
            pltpu.VMEM((blocks, pairs), f32),
            pltpu.VMEM((pairs // 128, blocks * group, 128), f32),
            pltpu.VMEM((blocks * group, 128), f32),
            pltpu.VMEM((6, 4 * (pairs // 128), outer, 128), f32),
            pltpu.VMEM((SWEEPS, 6, outer, pairs), f32),
            pltpu.VMEM((SWEEPS, 6, outer, pairs), f32),
            pltpu.VMEM((SWEEPS, devices, 1, 128), f32),
            pltpu.VMEM((devices, 1, 128), f32),
            pltpu.SemaphoreType.REGULAR((len(near_radii(sizes)),)),
            pltpu.SemaphoreType.REGULAR,
            dma((3,)),
            dma((3,)),
            dma((3,)),
            dma((3,)),
        ],
        compiler_params=pltpu.CompilerParams(
            collective_id=0, has_side_effects=True, vmem_limit_bytes=40 << 20
        ),
    )(
        live_blocks,
        *[
            pltpu.with_memory_space_constraint(x, pltpu.HBM)
            for x in (
                pair_node,
                pair_line,
                pair_far,
                far_line,
                pair_geom,
                positions,
            )
        ]
    )
    return pl.pallas_call(
        finish,
        out_shape=(
            jax.ShapeDtypeStruct(positions.shape, f32),
            jax.ShapeDtypeStruct((2, SWEEPS), f32),
        ),
        in_specs=[vmem] * 2,
        out_specs=[pl.BlockSpec(memory_space=pl.ANY)] * 2,
        scratch_shapes=[dma((2,))],
        compiler_params=pltpu.CompilerParams(vmem_limit_bytes=1 << 20),
    )(moved, hist)


def solution(mesh):
    sizes = tuple(mesh.shape[a] for a in AXES)
    return jax.shard_map(
        functools.partial(local, sizes),
        mesh=mesh,
        in_specs=(
            P(None, "gx", "gy", "gz"),
            P("gx", "gy", "gz", None, None),
            P("gx", "gy", "gz", None),
            P("gx", "gy", "gz", None, None),
            P("gx", "gy", "gz", None),
            P("gx", "gy", "gz", None, None, None),
            P("gx", "gy", "gz"),
        ),
        out_specs=(P(None, "gx", "gy", "gz"), P()),
        check_vma=False,
    )
```

```python
import functools
import itertools

import jax
import jax.numpy as jnp
from jax import lax
from jax.experimental import pallas as pl
from jax.experimental.pallas import tpu as pltpu
from jax.sharding import PartitionSpec as P

RIM = 3
SWEEPS = 5
RELAX = 0.9
AXES = ("gx", "gy", "gz")
MESH = pl.DeviceIdType.MESH
f32 = jnp.float32
bf16 = jnp.bfloat16


def split(x, parts):
    out = []
    for _ in range(parts - 1):
        hi = x.astype(bf16)
        out.append(hi)
        x = x - hi.astype(f32)
    out.append(x.astype(bf16))
    return out


def mm(a, b):
    return jnp.dot(a, b, preferred_element_type=f32)


def near_radii(sizes):
    need = max(sizes[0] - 1, sizes[1] + sizes[2] - 2)
    radii = [1]
    while 2 * radii[-1] < need:
        radii.append(2 * radii[-1])
    return radii


def take_lanes(xs, low, half):
    outs = [[] for _ in xs]
    for h in range(0, low.shape[1], 128):
        idx = low[:, h : h + 128]
        got = [None] * len(xs)
        for j in range(xs[0].shape[1] // 128):
            for i, x in enumerate(xs):
                more = jnp.take_along_axis(
                    x[:, 128 * j : 128 * (j + 1)], idx, axis=1, mode="promise_in_bounds"
                )
                got[i] = jnp.where(half[:, h : h + 128] == j, more, got[i]) if j else more
        for out, x in zip(outs, got):
            out.append(x)
    return [jnp.concatenate(out, axis=1) for out in outs]


def kernel(
    sizes,
    blk,
    live_ref,
    node_hbm,
    line_hbm,
    farpos_hbm,
    farline_ref,
    geom_hbm,
    pos_hbm,
    out_ref,
    hist_out,
    node_ref,
    line_ref,
    farpos_ref,
    geom_ref,
    pos_ref,
    acc_ref,
    near_ref,
    step_ref,
    pos3,
    code,
    codes,
    there,
    lsend,
    lrecv,
    req,
    cols,
    hot,
    two,
    amat,
    cinv,
    geo,
    low_ref,
    half_ref,
    gap,
    terms,
    sums,
    reqs,
    dsend,
    drecv,
    erecv,
    rrecv,
    near_sem,
    whole_sem,
    ds_sem,
    dr_sem,
    es_sem,
    er_sem,
):
    nx, ny, nz = sizes
    bx, by, bz = blk
    devices = nx * ny * nz
    blocks, pairs = gap.shape
    outer = blocks // 2
    lines = bx * by
    me = [lax.axis_index(a) for a in AXES]
    mine = (me[0] * ny + me[1]) * nz + me[2]
    dirs = [(a, s) for a in (1, 0, 2) for s in (1, -1)]

    def neighbour(axis, sign):
        to = list(me)
        to[axis] = lax.rem(me[axis] + sign + sizes[axis], sizes[axis])
        return tuple(to)

    def exists(axis, sign):
        return (me[axis] + sign >= 0) & (me[axis] + sign < sizes[axis])

    def coords(k):
        to = lax.rem(mine + k, devices)
        return (to // (ny * nz), lax.rem(to // nz, ny), lax.rem(to, nz))

    def moved_by(axis, k):
        if sizes[axis] & (sizes[axis] - 1) == 0:
            return lax.bitwise_xor(me[axis], k)
        to = me[axis] + k
        return jnp.where(to >= sizes[axis], to - sizes[axis], to)

    ids = [[moved_by(a, k) for k in range(sizes[a])] for a in range(3)]

    def sphere(r):
        steps = itertools.product(*[range(1 - n, n) for n in sizes])
        return [s for s in steps if sum(abs(x) for x in s) == r]

    def inside(step):
        ok = True
        for x, n, at in zip(step, sizes, me):
            if x > 0:
                ok = ok & (at < n - x)
            if x < 0:
                ok = ok & (at >= -x)
        return ok

    def signal_sphere(sem, r):
        for step in sphere(r):

            @pl.when(inside(step))
            def _():
                to = tuple(at + x for at, x in zip(me, step))
                pl.semaphore_signal(sem, inc=1, device_id=to, device_id_type=MESH)

    def wait_sphere(sem, r):
        pl.semaphore_wait(sem, sum(jnp.where(inside(s), 1, 0) for s in sphere(r)))

    radii = near_radii(sizes)
    barrier = pltpu.get_barrier_semaphore()
    signal_sphere(barrier, 1)
    inputs = [
        pltpu.make_async_copy(*copy)
        for copy in [
            (farpos_hbm, farpos_ref, ds_sem.at[0]),
            (geom_hbm, geom_ref, es_sem.at[0]),
            (node_hbm, node_ref, es_sem.at[1]),
            (line_hbm, line_ref, es_sem.at[2]),
            (pos_hbm, pos_ref, ds_sem.at[2]),
        ]
    ]
    for copy in inputs:
        copy.start()
    def column(ref):
        row = ref[0, 0].astype(f32)
        return jnp.transpose(jnp.broadcast_to(row, (pairs, blocks)))

    row = farline_ref[0, 0].astype(f32)
    code[...] = jnp.concatenate([row] * (128 // blocks), axis=1)

    def remote(src, dst, send_sem, recv_sem, to):
        return pltpu.make_async_remote_copy(
            src_ref=src,
            dst_ref=dst,
            send_sem=send_sem,
            recv_sem=recv_sem,
            device_id=neighbour(*to),
            device_id_type=MESH,
        )

    def ask_line(d, axis, sign):
        return remote(code, codes.at[pl.ds(d, 1), :], ds_sem.at[1], dr_sem.at[1], (axis, sign))

    def ask_pairs(d, axis, sign):
        return remote(req, reqs.at[d], ds_sem.at[0], dr_sem.at[2], (axis, sign))

    def line_back(d, axis, sign):
        return remote(lsend.at[d], lrecv.at[d], ds_sem.at[1], dr_sem.at[0], (axis, -sign))

    def answer(t, d, axis, sign):
        sems = ds_sem.at[t % 2], dr_sem.at[t % 2]
        return remote(dsend.at[t, d], drecv.at[t, d], *sems, (axis, -sign))

    count = sum(jnp.where(exists(axis, sign), 1, 0) for axis, sign in dirs)

    def wait_each(ref, sem):
        for k in range(1, len(dirs) + 1):

            @pl.when(count == k)
            def _():
                some = ref.at[pl.ds(0, k)]
                pltpu.make_async_copy(some, some, sem).wait()

    def first_side(side):
        odd = lax.rem(me[1], 2) == 1
        return odd if side > 0 else jnp.logical_not(odd)

    def start_two(copy, way):
        for first in (True, False):
            for d in range(2):
                axis, sign = dirs[d]
                turn = first_side(way * sign)
                turn = turn if first else jnp.logical_not(turn)

                @pl.when(exists(axis, way * sign) & turn)
                def _():
                    copy(d, axis, sign).start()

    def start_rest(copy, way, d):
        axis, sign = dirs[d]

        @pl.when(exists(axis, way * sign))
        def _():
            copy(d, axis, sign).start()

    wait_sphere(barrier, 1)
    start_two(ask_line, 1)
    for d in range(2, len(dirs)):
        start_rest(ask_line, 1, d)
    for copy in inputs[:2]:
        copy.wait()
    wide = pairs // 128
    planes = [geom_ref[0, 0, 0, outer:, c, :] for c in range(3)]
    planes.append(farpos_ref[0, 0, 0, outer:, :].astype(f32))
    for c in range(4):
        for h in range(wide):
            req[c * wide + h] = planes[c][:, 128 * h : 128 * (h + 1)]
    start_two(ask_pairs, 1)
    for d in range(2, len(dirs)):
        start_rest(ask_pairs, 1, d)

    signal_sphere(near_sem.at[0], radii[0])
    for copy in inputs[2:4]:
        copy.wait()
    cols[0] = column(line_ref)
    cols[1] = column(farline_ref)

    codes[len(dirs) :] = jnp.zeros((8 - len(dirs), 128), f32)
    for d, (axis, sign) in enumerate(dirs):

        @pl.when(jnp.logical_not(exists(axis, -sign)))
        def _():
            codes[pl.ds(d, 1), :] = jnp.zeros(code.shape, f32)
            reqs[d] = jnp.zeros(req.shape, f32)

        @pl.when(jnp.logical_not(exists(axis, sign)))
        def _():
            lrecv[d] = jnp.zeros((3, outer, bz), f32)
            for t in range(1, SWEEPS):
                drecv[t, d] = jnp.zeros((outer, pairs), f32)

    def at_lanes(z):
        z = z.astype(jnp.int32)
        return lax.bitwise_and(z, 127), lax.shift_right_arithmetic(z, 7)

    live_rows = lax.broadcasted_iota(jnp.int32, (blocks, pairs), 0) < live_ref[0, 0, 0]
    node_low, node_half = at_lanes(node_ref[0, 0, 0])
    lane_node = lax.broadcasted_iota(jnp.int32, (pairs, 128), 1).astype(f32)
    node_t = jnp.transpose(node_low.astype(f32))
    group = terms.shape[1] // blocks
    terms[...] = jnp.zeros_like(terms)

    def mark(slots):
        for b in slots:
            hot[pl.ds(b * pairs, pairs), :] = jnp.where(
                node_t[:, b : b + 1] == lane_node, 1.0, 0.0
            ).astype(bf16)

    mark(range(outer))
    wait_sphere(near_sem.at[0], radii[0])
    if len(radii) > 1:
        signal_sphere(near_sem.at[1], radii[1])
    inputs[4].wait()
    for c in range(3):
        for k, part in enumerate(split(pos_ref[c].reshape(lines, bz), 3)):
            pos3[c, k] = part
    row_line = line_ref[0, 0].astype(f32)
    two[...] = jnp.concatenate([row_line, row_line], axis=1)
    row_mod = lax.broadcasted_iota(jnp.int32, (blocks, blocks), 0)
    col_mod = lax.broadcasted_iota(jnp.int32, (blocks, blocks), 1)
    line_b = cols[0]
    same = line_b[:, :blocks] == row_line
    first_col = 1.0 - jnp.max(
        jnp.where(same & (col_mod < row_mod), 1.0, 0.0), axis=1, keepdims=True
    )

    def cat(parts, axis=0):
        return jnp.concatenate(parts, axis=axis)

    def scatter(values):
        n = len(values)
        for h in range(bz // 128):
            for c in range(n):
                x = jnp.where(node_half == h, values[c], 0.0)
                for j in range(wide):
                    cut = x[:, 128 * j : 128 * (j + 1)]
                    terms[j, pl.ds(h * n + c, blocks, stride=group), :] = cut
        for b in range(blocks):
            slot = cat([terms[j, pl.ds(b * group, group), :] for j in range(wide)], 1)
            both = cat(split(slot, 2))
            both = mm(both, hot[pl.ds(b * pairs, pairs), :])
            sums[pl.ds(b * group, group), :] = both[:group] + both[group:]
        return [
            cat([sums[pl.ds(h * n + c, blocks, stride=group), :] for h in range(bz // 128)], 1)
            for c in range(n)
        ]

    def located(code, zpos, shift):
        e = jnp.floor((code + 0.5) / (by + 2 * RIM))
        f = code - e * (by + 2 * RIM)
        e = e - (RIM + shift[0] * bx)
        f = f - (RIM + shift[1] * by)
        z = zpos - (RIM + shift[2] * bz)
        ok_line = (e >= 0) & (e < bx) & (f >= 0) & (f < by)
        return jnp.where(ok_line, e * by + f, -1.0), z, ok_line & (z >= 0) & (z < bz)

    def setup(row, line, node, geom):
        n = line.shape[0]
        a = jnp.where(line[:, : 2 * blocks] == two[...], 1.0, 0.0).astype(bf16)
        amat[pl.ds(row, n), :] = a
        cinv[pl.ds(row, n), :] = RELAX / (1.0 + mm(a[:, :blocks], counts))
        low, half = at_lanes(node)
        low_ref[pl.ds(row, n), :] = low
        half_ref[pl.ds(row, n), :] = half
        for c in range(3):
            geo[c, pl.ds(row, n), :] = geom[c]

    def fetch(line):
        lane_line = lax.broadcasted_iota(jnp.int32, (line.shape[0], lines), 1).astype(f32)
        own = jnp.where(line == lane_line, 1.0, 0.0).astype(bf16)
        return [sum(mm(own, pos3[c, k]) for k in range(3)) for c in range(3)]

    base = len(dirs) * outer
    rows = base + 2 * blocks
    node = node_ref[0, 0, 0].astype(f32)
    far = farpos_ref[0, 0, 0].astype(f32)
    geom = [geom_ref[0, 0, 0, :, c, :] for c in range(4)]
    wait_each(codes, dr_sem.at[1])
    shifts = []
    for axis, sign in dirs:
        shifts.append([sign if a == axis else 0 for a in range(3)])
    turned = jnp.transpose(codes[...])[outer:blocks]
    asked = []
    for d in range(len(dirs)):
        there[d] = jnp.broadcast_to(turned[:, d : d + 1], (outer, pairs))
        asked.append(located(there[d], 0.0, shifts[d])[0])
    back = fetch(cat(asked))
    for d in range(len(dirs)):
        for c in range(3):
            lsend[d, c] = back[c][d * outer : (d + 1) * outer]
    wait_each(codes, ds_sem.at[1])
    start_two(line_back, -1)
    for d in range(2, len(dirs)):
        start_rest(line_back, -1, d)

    for i, r in enumerate(radii[1:], 1):
        wait_sphere(near_sem.at[i], r)
        if i + 1 < len(radii):
            signal_sphere(near_sem.at[i + 1], radii[i + 1])
    for k in range(1, nx):
        to = (ids[0][k], me[1], me[2])
        pl.semaphore_signal(whole_sem, inc=1, device_id=to, device_id_type=MESH)

    mark(range(outer, blocks))
    ones = jnp.where(live_rows, 1.0, 0.0)
    counts = scatter([ones, jnp.zeros_like(ones), jnp.zeros_like(ones)])[0].astype(bf16)
    line, z, ok = located(cols[1], far, (0, 0, 0))
    setup(
        base,
        cat([line_b, line]),
        cat([node, jnp.where(ok, z, 0.0)]),
        [cat([geom[c], jnp.where(ok, -geom[c], 0.0)]) for c in range(3)],
    )
    vals = fetch(cat([line_b, line]))
    start = take_lanes([v[:blocks] for v in vals], *at_lanes(node))
    inner = take_lanes([v[blocks : blocks + outer] for v in vals], *at_lanes(z[:outer]))
    gap[...] = sum(geom[c] * start[c] for c in range(3)) - geom[3]
    gap[0:outer, :] = gap[0:outer, :] - sum(geom[c][:outer] * inner[c] for c in range(3))

    wait_each(reqs, dr_sem.at[2])
    pairs_in = []
    for d in range(len(dirs)):
        got = [
            jnp.concatenate([reqs[d, c * wide + h] for h in range(wide)], axis=1) for c in range(4)
        ]
        _, at, ok = located(there[d], got[3], shifts[d])
        pairs_in.append([jnp.where(ok, at, 0.0)] + [jnp.where(ok, -got[c], 0.0) for c in range(3)])
    pairs_in = [cat([x[i] for x in pairs_in]) for i in range(4)]
    setup(0, cat(asked), pairs_in[0], pairs_in[1:])

    wait_each(lrecv, dr_sem.at[0])
    low, half = at_lanes(far[outer:] - RIM)
    reach = []
    for c in range(3):
        line = vals[c][blocks + outer :]
        for d, (axis, sign) in enumerate(dirs):
            if axis < 2:
                line = line + lrecv[d, c]
        below = lrecv[dirs.index((2, -1)), c][:, bz - 128 :]
        above = lrecv[dirs.index((2, 1)), c][:, :128]
        reach.append(jnp.concatenate([below, line, above], axis=1))
    reach = take_lanes(reach, low, half + 1)
    if nx > 1:
        pl.semaphore_wait(whole_sem, nx - 1)
    gap[pl.ds(outer, outer), :] = gap[pl.ds(outer, outer), :] - sum(
        geom[c][outer:] * reach[c] for c in range(3)
    )
    def respond(t, total):
        send = functools.partial(answer, t)
        for d in range(len(dirs)):
            dsend[t, d] = total(d * outer, outer)
            if d == 1:
                start_two(send, -1)
            if d > 1:
                start_rest(send, -1, d)

    def responded(t):
        wait_each(dsend.at[t], ds_sem.at[t % 2])

    def received(t):
        wait_each(drecv.at[t], dr_sem.at[t % 2])
        got = drecv[t, 0]
        for d in range(1, len(dirs)):
            got = got + drecv[t, d]
        return got

    acc_ref[...] = jnp.zeros_like(acc_ref)

    def to_all(ref, send_sem, recv_sem):
        def send(to):
            pltpu.make_async_remote_copy(
                src_ref=ref,
                dst_ref=ref,
                send_sem=send_sem,
                recv_sem=recv_sem,
                device_id=to,
                device_id_type=MESH,
            ).start()

        if devices <= 32:
            for a in reversed(range(nx)):
                for b in reversed(range(ny)):
                    for c in range(nz):
                        if a or b or c:
                            send((ids[0][a], ids[1][b], ids[2][c]))
        else:

            def step(k, carry):
                send(coords(k))
                return carry

            lax.fori_loop(1, devices, step, 0)

    def lanes_sum(x):
        x = jnp.sum(x, axis=0, keepdims=True)
        out = x[:, :128]
        for j in range(1, x.shape[1] // 128):
            out = out + x[:, 128 * j : 128 * (j + 1)]
        return out

    lane = lax.broadcasted_iota(jnp.int32, (1, 128), 1)
    at_line = lax.broadcasted_iota(jnp.int32, (lines, 2 * blocks), 0).astype(f32)
    place = jnp.where(at_line == two[...], 1.0, 0.0).astype(bf16)

    def placed(x):
        return mm(place, cat(split(x, 2)))

    def apply(row, n, parts):
        both = mm(amat[row : row + n, :], parts)
        return [both[:, c * bz : (c + 1) * bz] * cinv[row : row + n, :] for c in range(3)]

    def dots(row, n, moved):
        low = low_ref[row : row + n, :]
        half = half_ref[row : row + n, :]
        got = take_lanes(moved, low, half)
        return sum(geo[c, row : row + n] * got[c] for c in range(3))

    def wait_all(ref, sem):
        others = ref.at[pl.ds(0, devices - 1)]
        pltpu.make_async_copy(others, others, sem).wait()

    def settle(scale):
        acc_ref[...] = acc_ref[...] + (scale * first_col) * near_ref[...]

    rrecv[mine] = jnp.zeros((1, 128), f32)
    energies, scales = [], []
    for t in range(SWEEPS):
        last, slot = t == SWEEPS - 1, t % 2
        depth = jnp.where(live_rows, jnp.maximum(-gap[...], 0.0), 0.0)
        erecv[t, mine] = lanes_sum(depth * depth)
        to_all(erecv.at[t, mine], es_sem.at[slot], er_sem.at[slot])
        own = scatter([depth * geo[c, base : base + blocks] for c in range(3)])
        parts = cat(split(cat(own, 1), 2))
        if not t:
            wait_each(lrecv, ds_sem.at[1])
        if not last:
            far = apply(0, base, parts)
            respond(t + 1, lambda row, n: dots(row, n, [m[row : row + n] for m in far]))
        moved = apply(base, blocks if last else 2 * blocks, parts)
        near = cat([m[:blocks] for m in moved], 1)
        resid = jnp.sum(lanes_sum(near * near * first_col), axis=1, keepdims=True)
        rrecv[mine] = jnp.where(lane == t, resid, rrecv[mine])
        if last:
            to_all(rrecv.at[mine], es_sem.at[2], er_sem.at[2])
        if t:
            wait_all(erecv.at[t - 1], es_sem.at[1 - slot])
            responded(t)
            settle(scales[-1])
        else:
            wait_each(reqs, ds_sem.at[0])
        near_ref[...] = near
        if last:
            for c in range(3):
                cut = slice(c * bz, (c + 1) * bz)
                done = placed(acc_ref[:, cut])
                out_ref[c] = pos_ref[c] + done.reshape(bx, by, bz)
                step_ref[c] = placed(first_col * near[:, cut]).reshape(bx, by, bz)
        else:
            step = dots(base, 2 * blocks, moved)
            step = step[:blocks] + step[blocks:]
            more = received(t + 1)
        wait_all(erecv.at[t], er_sem.at[slot])
        energy = jnp.sum(jnp.sum(erecv[t], axis=0), axis=1, keepdims=True)
        scale = 1.0 / (1.0 + energy / (blocks * pairs * devices))
        energies.append(energy)
        scales.append(scale)
        if last:
            for c in range(3):
                out_ref[c] = out_ref[c] + scale[:, :, None] * step_ref[c]
        else:
            gap[0:outer, :] = gap[0:outer, :] + scale * step[:outer]
            gap[pl.ds(outer, outer), :] = gap[pl.ds(outer, outer), :] + scale * (
                step[outer:] + more
            )

    wait_all(erecv.at[SWEEPS - 1], es_sem.at[(SWEEPS - 1) % 2])
    energy, scale = jnp.zeros((1, 128), f32), jnp.zeros((1, 128), f32)
    for t in range(SWEEPS):
        energy = jnp.where(lane == t, energies[t], energy)
        scale = jnp.where(lane == t, scales[t], scale)
    hist_out[0:1, :] = jnp.sqrt(1.0 + energy / (blocks * pairs))[:, :SWEEPS]
    factor = scale * scale / (bx * by * bz)
    wait_all(rrecv, er_sem.at[2])
    resid = factor * jnp.sum(rrecv[...], axis=0)
    hist_out[1:2, :] = jnp.sqrt(1.0 + resid)[:, :SWEEPS]
    wait_all(rrecv, es_sem.at[2])


def finish(pos_ref, hist_ref, pos_out, hist_out, sem):
    copies = [
        pltpu.make_async_copy(pos_ref, pos_out, sem.at[0]),
        pltpu.make_async_copy(hist_ref, hist_out, sem.at[1]),
    ]
    for copy in copies:
        copy.start()
    for copy in copies:
        copy.wait()


def local(sizes, positions, pair_node, pair_line, pair_far, far_line, pair_geom, live_blocks):
    blocks, pairs = pair_node.shape[3:]
    blk = positions.shape[1:]
    devices = sizes[0] * sizes[1] * sizes[2]
    outer = blocks // 2
    rows = 2 * blocks + 6 * outer
    group = -(-3 * (blk[2] // 128) // 8) * 8
    dma = pltpu.SemaphoreType.DMA
    vmem = pl.BlockSpec(memory_space=pltpu.VMEM)
    hbm = functools.partial(pltpu.with_memory_space_constraint, memory_space=pltpu.HBM)
    moved, hist = pl.pallas_call(
        functools.partial(kernel, sizes, blk),
        out_shape=(
            pltpu.VMEM(positions.shape, f32),
            pltpu.VMEM((2, SWEEPS), f32),
        ),
        in_specs=[pl.BlockSpec(memory_space=pltpu.SMEM)]
        + [pl.BlockSpec(memory_space=pltpu.HBM)] * 3
        + [vmem]
        + [pl.BlockSpec(memory_space=pltpu.HBM)] * 2,
        out_specs=(vmem, vmem),
        scratch_shapes=[
            pltpu.VMEM(pair_node.shape, jnp.int32),
            pltpu.VMEM(pair_line.shape, jnp.int32),
            pltpu.VMEM(pair_far.shape, jnp.int32),
            pltpu.VMEM(pair_geom.shape, f32),
            pltpu.VMEM(positions.shape, f32),
            pltpu.VMEM((blocks, 3 * blk[2]), f32),
            pltpu.VMEM((blocks, 3 * blk[2]), f32),
            pltpu.VMEM(positions.shape, f32),
            pltpu.VMEM((3, 3, blk[0] * blk[1], blk[2]), bf16),
            pltpu.VMEM((1, 128), f32),
            pltpu.VMEM((8, 128), f32),
            pltpu.VMEM((6, outer, pairs), f32),
            pltpu.VMEM((6, 3, outer, blk[2]), f32),
            pltpu.VMEM((6, 3, outer, blk[2]), f32),
            pltpu.VMEM((4 * (pairs // 128), outer, 128), f32),
            pltpu.VMEM((2, blocks, pairs), f32),
            pltpu.VMEM((blocks * pairs, 128), bf16),
            pltpu.VMEM((1, 2 * blocks), f32),
            pltpu.VMEM((rows, 2 * blocks), bf16),
            pltpu.VMEM((rows, pairs), f32),
            pltpu.VMEM((3, rows, pairs), f32),
            pltpu.VMEM((rows, pairs), jnp.int32),
            pltpu.VMEM((rows, pairs), jnp.int32),
            pltpu.VMEM((blocks, pairs), f32),
            pltpu.VMEM((pairs // 128, blocks * group, 128), f32),
            pltpu.VMEM((blocks * group, 128), f32),
            pltpu.VMEM((6, 4 * (pairs // 128), outer, 128), f32),
            pltpu.VMEM((SWEEPS, 6, outer, pairs), f32),
            pltpu.VMEM((SWEEPS, 6, outer, pairs), f32),
            pltpu.VMEM((SWEEPS, devices, 1, 128), f32),
            pltpu.VMEM((devices, 1, 128), f32),
            pltpu.SemaphoreType.REGULAR((len(near_radii(sizes)),)),
            pltpu.SemaphoreType.REGULAR,
            dma((3,)),
            dma((3,)),
            dma((3,)),
            dma((3,)),
        ],
        compiler_params=pltpu.CompilerParams(
            collective_id=0, has_side_effects=True, vmem_limit_bytes=40 << 20
        ),
    )(
        live_blocks,
        hbm(pair_node),
        hbm(pair_line),
        hbm(pair_far),
        pltpu.with_memory_space_constraint(far_line, pltpu.VMEM),
        hbm(pair_geom),
        hbm(positions),
    )
    return pl.pallas_call(
        finish,
        out_shape=(
            jax.ShapeDtypeStruct(positions.shape, f32),
            jax.ShapeDtypeStruct((2, SWEEPS), f32),
        ),
        in_specs=[vmem] * 2,
        out_specs=[pl.BlockSpec(memory_space=pl.ANY)] * 2,
        scratch_shapes=[dma((2,))],
        compiler_params=pltpu.CompilerParams(vmem_limit_bytes=1 << 20),
    )(moved, hist)


def solution(mesh):
    sizes = tuple(mesh.shape[a] for a in AXES)
    return jax.shard_map(
        functools.partial(local, sizes),
        mesh=mesh,
        in_specs=(
            P(None, "gx", "gy", "gz"),
            P("gx", "gy", "gz", None, None),
            P("gx", "gy", "gz", None),
            P("gx", "gy", "gz", None, None),
            P("gx", "gy", "gz", None),
            P("gx", "gy", "gz", None, None, None),
            P("gx", "gy", "gz"),
        ),
        out_specs=(P(None, "gx", "gy", "gz"), P()),
        check_vma=False,
    )
```

```python
import functools
import itertools

import jax
import jax.numpy as jnp
from jax import lax
from jax.experimental import pallas as pl
from jax.experimental.pallas import tpu as pltpu
from jax.sharding import PartitionSpec as P

RIM = 3
SWEEPS = 5
RELAX = 0.9
AXES = ("gx", "gy", "gz")
MESH = pl.DeviceIdType.MESH
f32 = jnp.float32
bf16 = jnp.bfloat16


def split(x, parts):
    out = []
    for _ in range(parts - 1):
        hi = x.astype(bf16)
        out.append(hi)
        x = x - hi.astype(f32)
    out.append(x.astype(bf16))
    return out


def mm(a, b):
    return jnp.dot(a, b, preferred_element_type=f32)


def near_radii(sizes):
    need = max(sizes[0] - 1, sizes[1] + sizes[2] - 2)
    radii = [1]
    while 2 * radii[-1] < need:
        radii.append(2 * radii[-1])
    return radii


def take_lanes(xs, low, half):
    outs = [[] for _ in xs]
    for h in range(0, low.shape[1], 128):
        idx = low[:, h : h + 128]
        got = [None] * len(xs)
        for j in range(xs[0].shape[1] // 128):
            for i, x in enumerate(xs):
                more = jnp.take_along_axis(
                    x[:, 128 * j : 128 * (j + 1)], idx, axis=1, mode="promise_in_bounds"
                )
                got[i] = jnp.where(half[:, h : h + 128] == j, more, got[i]) if j else more
        for out, x in zip(outs, got):
            out.append(x)
    return [jnp.concatenate(out, axis=1) for out in outs]


def kernel(
    sizes,
    blk,
    live_ref,
    node_hbm,
    line_hbm,
    farpos_hbm,
    farline_ref,
    geom_hbm,
    pos_hbm,
    out_ref,
    hist_out,
    node_ref,
    line_ref,
    farpos_ref,
    geom_ref,
    pos_ref,
    acc_ref,
    near_ref,
    step_ref,
    pos3,
    code,
    codes,
    lsend,
    lrecv,
    req,
    cols,
    hot,
    two,
    amat,
    cinv,
    geo,
    low_ref,
    half_ref,
    gap,
    terms,
    sums,
    reqs,
    dsend,
    drecv,
    erecv,
    rrecv,
    near_sem,
    whole_sem,
    ds_sem,
    dr_sem,
    es_sem,
    er_sem,
):
    nx, ny, nz = sizes
    bx, by, bz = blk
    devices = nx * ny * nz
    blocks, pairs = gap.shape
    outer = blocks // 2
    lines = bx * by
    me = [lax.axis_index(a) for a in AXES]
    mine = (me[0] * ny + me[1]) * nz + me[2]
    dirs = [(a, s) for a in (1, 0, 2) for s in (1, -1)]

    def neighbour(axis, sign):
        to = list(me)
        to[axis] = lax.rem(me[axis] + sign + sizes[axis], sizes[axis])
        return tuple(to)

    def exists(axis, sign):
        return (me[axis] + sign >= 0) & (me[axis] + sign < sizes[axis])

    def coords(k):
        to = lax.rem(mine + k, devices)
        return (to // (ny * nz), lax.rem(to // nz, ny), lax.rem(to, nz))

    def moved_by(axis, k):
        if sizes[axis] & (sizes[axis] - 1) == 0:
            return lax.bitwise_xor(me[axis], k)
        to = me[axis] + k
        return jnp.where(to >= sizes[axis], to - sizes[axis], to)

    ids = [[moved_by(a, k) for k in range(sizes[a])] for a in range(3)]

    def sphere(r):
        steps = itertools.product(*[range(1 - n, n) for n in sizes])
        steps = [s for s in steps if sum(abs(x) for x in s) == r]
        return sorted(steps, key=lambda s: -abs(s[1]))

    def inside(step):
        ok = True
        for x, n, at in zip(step, sizes, me):
            if x > 0:
                ok = ok & (at < n - x)
            if x < 0:
                ok = ok & (at >= -x)
        return ok

    def signal_sphere(sem, r):
        for step in sphere(r):

            @pl.when(inside(step))
            def _():
                to = tuple(at + x for at, x in zip(me, step))
                pl.semaphore_signal(sem, inc=1, device_id=to, device_id_type=MESH)

    def wait_sphere(sem, r):
        pl.semaphore_wait(sem, sum(jnp.where(inside(s), 1, 0) for s in sphere(r)))

    radii = near_radii(sizes)
    barrier = pltpu.get_barrier_semaphore()
    signal_sphere(barrier, 1)
    inputs = [
        pltpu.make_async_copy(*copy)
        for copy in [
            (farpos_hbm, farpos_ref, ds_sem.at[0]),
            (geom_hbm, geom_ref, es_sem.at[0]),
            (node_hbm, node_ref, es_sem.at[1]),
            (line_hbm, line_ref, es_sem.at[2]),
            (pos_hbm, pos_ref, ds_sem.at[2]),
        ]
    ]
    for copy in inputs:
        copy.start()
    def column(ref):
        row = ref[0, 0].astype(f32)
        return jnp.transpose(jnp.broadcast_to(row, (pairs, blocks)))

    cols[1] = column(farline_ref)
    code[...] = cols[1, outer:, :128]

    def remote(src, dst, send_sem, recv_sem, to):
        return pltpu.make_async_remote_copy(
            src_ref=src,
            dst_ref=dst,
            send_sem=send_sem,
            recv_sem=recv_sem,
            device_id=neighbour(*to),
            device_id_type=MESH,
        )

    def ask_line(d, axis, sign):
        return remote(code, codes.at[d], ds_sem.at[1], dr_sem.at[1], (axis, sign))

    def ask_pairs(d, axis, sign):
        return remote(req, reqs.at[d], ds_sem.at[0], dr_sem.at[2], (axis, sign))

    def line_back(d, axis, sign):
        return remote(lsend.at[d], lrecv.at[d], ds_sem.at[1], dr_sem.at[0], (axis, -sign))

    def answer(t, d, axis, sign):
        sems = ds_sem.at[t % 2], dr_sem.at[t % 2]
        return remote(dsend.at[t, d], drecv.at[t, d], *sems, (axis, -sign))

    count = sum(jnp.where(exists(axis, sign), 1, 0) for axis, sign in dirs)

    def wait_each(ref, sem):
        for k in range(1, len(dirs) + 1):

            @pl.when(count == k)
            def _():
                some = ref.at[pl.ds(0, k)]
                pltpu.make_async_copy(some, some, sem).wait()

    def first_side(side):
        odd = lax.rem(me[1], 2) == 1
        return odd if side > 0 else jnp.logical_not(odd)

    def start_two(copy, way):
        for first in (True, False):
            for d in range(2):
                axis, sign = dirs[d]
                turn = first_side(way * sign)
                turn = turn if first else jnp.logical_not(turn)

                @pl.when(exists(axis, way * sign) & turn)
                def _():
                    copy(d, axis, sign).start()

    def start_rest(copy, way, d):
        axis, sign = dirs[d]

        @pl.when(exists(axis, way * sign))
        def _():
            copy(d, axis, sign).start()

    wait_sphere(barrier, 1)
    start_two(ask_line, 1)
    for d in range(2, len(dirs)):
        start_rest(ask_line, 1, d)
    for copy in inputs[:2]:
        copy.wait()
    wide = pairs // 128
    planes = [geom_ref[0, 0, 0, outer:, c, :] for c in range(3)]
    planes.append(farpos_ref[0, 0, 0, outer:, :].astype(f32))
    for c in range(4):
        for h in range(wide):
            req[c * wide + h] = planes[c][:, 128 * h : 128 * (h + 1)]
    start_two(ask_pairs, 1)
    for d in range(2, len(dirs)):
        start_rest(ask_pairs, 1, d)

    signal_sphere(near_sem.at[0], radii[0])
    for copy in inputs[2:4]:
        copy.wait()
    cols[0] = column(line_ref)

    for d, (axis, sign) in enumerate(dirs):

        @pl.when(jnp.logical_not(exists(axis, -sign)))
        def _():
            codes[d] = jnp.zeros(code.shape, f32)
            reqs[d] = jnp.zeros(req.shape, f32)

        @pl.when(jnp.logical_not(exists(axis, sign)))
        def _():
            lrecv[d] = jnp.zeros((3, outer, bz), f32)
            for t in range(1, SWEEPS):
                drecv[t, d] = jnp.zeros((outer, pairs), f32)

    def at_lanes(z):
        z = z.astype(jnp.int32)
        return lax.bitwise_and(z, 127), lax.shift_right_arithmetic(z, 7)

    live_rows = lax.broadcasted_iota(jnp.int32, (blocks, pairs), 0) < live_ref[0, 0, 0]
    node_low, node_half = at_lanes(node_ref[0, 0, 0])
    lane_node = lax.broadcasted_iota(jnp.int32, (pairs, 128), 1).astype(f32)
    node_t = jnp.transpose(node_low.astype(f32))
    group = terms.shape[1] // blocks
    terms[...] = jnp.zeros_like(terms)

    def mark(slots):
        for b in slots:
            hot[pl.ds(b * pairs, pairs), :] = jnp.where(
                node_t[:, b : b + 1] == lane_node, 1.0, 0.0
            ).astype(bf16)

    mark(range(outer))
    wait_sphere(near_sem.at[0], radii[0])
    if len(radii) > 1:
        signal_sphere(near_sem.at[1], radii[1])
    inputs[4].wait()
    for c in range(3):
        for k, part in enumerate(split(pos_ref[c].reshape(lines, bz), 3)):
            pos3[c, k] = part
    row_line = line_ref[0, 0].astype(f32)
    two[...] = jnp.concatenate([row_line, row_line], axis=1)
    row_mod = lax.broadcasted_iota(jnp.int32, (blocks, blocks), 0)
    col_mod = lax.broadcasted_iota(jnp.int32, (blocks, blocks), 1)
    line_b = cols[0]
    same = line_b[:, :blocks] == row_line
    first_col = 1.0 - jnp.max(
        jnp.where(same & (col_mod < row_mod), 1.0, 0.0), axis=1, keepdims=True
    )

    def cat(parts, axis=0):
        return jnp.concatenate(parts, axis=axis)

    def scatter(values):
        n = len(values)
        for h in range(bz // 128):
            for c in range(n):
                x = jnp.where(node_half == h, values[c], 0.0)
                for j in range(wide):
                    cut = x[:, 128 * j : 128 * (j + 1)]
                    terms[j, pl.ds(h * n + c, blocks, stride=group), :] = cut
        for b in range(blocks):
            slot = cat([terms[j, pl.ds(b * group, group), :] for j in range(wide)], 1)
            both = cat(split(slot, 2))
            both = mm(both, hot[pl.ds(b * pairs, pairs), :])
            sums[pl.ds(b * group, group), :] = both[:group] + both[group:]
        return [
            cat([sums[pl.ds(h * n + c, blocks, stride=group), :] for h in range(bz // 128)], 1)
            for c in range(n)
        ]

    def located(code, zpos, shift):
        e = jnp.floor((code + 0.5) / (by + 2 * RIM))
        f = code - e * (by + 2 * RIM)
        e = e - (RIM + shift[0] * bx)
        f = f - (RIM + shift[1] * by)
        z = zpos - (RIM + shift[2] * bz)
        ok_line = (e >= 0) & (e < bx) & (f >= 0) & (f < by)
        return jnp.where(ok_line, e * by + f, -1.0), z, ok_line & (z >= 0) & (z < bz)

    def setup(row, line, node, geom):
        n = line.shape[0]
        a = jnp.where(line[:, : 2 * blocks] == two[...], 1.0, 0.0).astype(bf16)
        amat[pl.ds(row, n), :] = a
        cinv[pl.ds(row, n), :] = RELAX / (1.0 + mm(a[:, :blocks], counts))
        low, half = at_lanes(node)
        low_ref[pl.ds(row, n), :] = low
        half_ref[pl.ds(row, n), :] = half
        for c in range(3):
            geo[c, pl.ds(row, n), :] = geom[c]

    def fetch(line):
        lane_line = lax.broadcasted_iota(jnp.int32, (line.shape[0], lines), 1).astype(f32)
        own = jnp.where(line == lane_line, 1.0, 0.0).astype(bf16)
        return [sum(mm(own, pos3[c, k]) for k in range(3)) for c in range(3)]

    base = len(dirs) * outer
    rows = base + 2 * blocks
    node = node_ref[0, 0, 0].astype(f32)
    far = farpos_ref[0, 0, 0].astype(f32)
    geom = [geom_ref[0, 0, 0, :, c, :] for c in range(4)]
    wait_each(codes, dr_sem.at[1])
    shifts = []
    for axis, sign in dirs:
        shifts.append([sign if a == axis else 0 for a in range(3)])
    asked = []
    for d in range(len(dirs)):
        there = jnp.concatenate([codes[d]] * wide, axis=1)
        asked.append(located(there, 0.0, shifts[d])[0])
    back = fetch(cat(asked))
    for d in range(len(dirs)):
        for c in range(3):
            lsend[d, c] = back[c][d * outer : (d + 1) * outer]
    wait_each(codes, ds_sem.at[1])
    start_two(line_back, -1)
    for d in range(2, len(dirs)):
        start_rest(line_back, -1, d)

    for i, r in enumerate(radii[1:], 1):
        wait_sphere(near_sem.at[i], r)
        if i + 1 < len(radii):
            signal_sphere(near_sem.at[i + 1], radii[i + 1])
    for k in range(1, nx):
        to = (ids[0][k], me[1], me[2])
        pl.semaphore_signal(whole_sem, inc=1, device_id=to, device_id_type=MESH)

    mark(range(outer, blocks))
    ones = jnp.where(live_rows, 1.0, 0.0)
    counts = scatter([ones, jnp.zeros_like(ones), jnp.zeros_like(ones)])[0].astype(bf16)
    line, z, ok = located(cols[1], far, (0, 0, 0))
    setup(
        base,
        cat([line_b, line]),
        cat([node, jnp.where(ok, z, 0.0)]),
        [cat([geom[c], jnp.where(ok, -geom[c], 0.0)]) for c in range(3)],
    )
    vals = fetch(cat([line_b, line]))
    start = take_lanes([v[:blocks] for v in vals], *at_lanes(node))
    inner = take_lanes([v[blocks : blocks + outer] for v in vals], *at_lanes(z[:outer]))
    gap[...] = sum(geom[c] * start[c] for c in range(3)) - geom[3]
    gap[0:outer, :] = gap[0:outer, :] - sum(geom[c][:outer] * inner[c] for c in range(3))

    wait_each(reqs, dr_sem.at[2])
    pairs_in = []
    for d in range(len(dirs)):
        got = [
            jnp.concatenate([reqs[d, c * wide + h] for h in range(wide)], axis=1) for c in range(4)
        ]
        there = jnp.concatenate([codes[d]] * wide, axis=1)
        _, at, ok = located(there, got[3], shifts[d])
        pairs_in.append([jnp.where(ok, at, 0.0)] + [jnp.where(ok, -got[c], 0.0) for c in range(3)])
    pairs_in = [cat([x[i] for x in pairs_in]) for i in range(4)]
    setup(0, cat(asked), pairs_in[0], pairs_in[1:])

    wait_each(lrecv, dr_sem.at[0])
    low, half = at_lanes(far[outer:] - RIM)
    reach = []
    for c in range(3):
        line = vals[c][blocks + outer :]
        for d, (axis, sign) in enumerate(dirs):
            if axis < 2:
                line = line + lrecv[d, c]
        below = lrecv[dirs.index((2, -1)), c][:, bz - 128 :]
        above = lrecv[dirs.index((2, 1)), c][:, :128]
        reach.append(jnp.concatenate([below, line, above], axis=1))
    reach = take_lanes(reach, low, half + 1)
    if nx > 1:
        pl.semaphore_wait(whole_sem, nx - 1)
    gap[pl.ds(outer, outer), :] = gap[pl.ds(outer, outer), :] - sum(
        geom[c][outer:] * reach[c] for c in range(3)
    )
    def respond(t, total):
        send = functools.partial(answer, t)
        for d in range(len(dirs)):
            dsend[t, d] = total(d * outer, outer)
            if d == 1:
                start_two(send, -1)
            if d > 1:
                start_rest(send, -1, d)

    def responded(t):
        wait_each(dsend.at[t], ds_sem.at[t % 2])

    def received(t):
        wait_each(drecv.at[t], dr_sem.at[t % 2])
        got = drecv[t, 0]
        for d in range(1, len(dirs)):
            got = got + drecv[t, d]
        return got

    acc_ref[...] = jnp.zeros_like(acc_ref)

    def to_all(ref, send_sem, recv_sem):
        def send(to):
            pltpu.make_async_remote_copy(
                src_ref=ref,
                dst_ref=ref,
                send_sem=send_sem,
                recv_sem=recv_sem,
                device_id=to,
                device_id_type=MESH,
            ).start()

        if devices <= 32:
            for a in reversed(range(nx)):
                for b in reversed(range(ny)):
                    for c in range(nz):
                        if a or b or c:
                            send((ids[0][a], ids[1][b], ids[2][c]))
        else:

            def step(k, carry):
                send(coords(k))
                return carry

            lax.fori_loop(1, devices, step, 0)

    def lanes_sum(x):
        x = jnp.sum(x, axis=0, keepdims=True)
        out = x[:, :128]
        for j in range(1, x.shape[1] // 128):
            out = out + x[:, 128 * j : 128 * (j + 1)]
        return out

    lane = lax.broadcasted_iota(jnp.int32, (1, 128), 1)
    at_line = lax.broadcasted_iota(jnp.int32, (lines, 2 * blocks), 0).astype(f32)
    place = jnp.where(at_line == two[...], 1.0, 0.0).astype(bf16)

    def placed(x):
        return mm(place, cat(split(x, 2)))

    def apply(row, n, parts):
        both = mm(amat[row : row + n, :], parts)
        return [both[:, c * bz : (c + 1) * bz] * cinv[row : row + n, :] for c in range(3)]

    def dots(row, n, moved):
        low = low_ref[row : row + n, :]
        half = half_ref[row : row + n, :]
        got = take_lanes(moved, low, half)
        return sum(geo[c, row : row + n] * got[c] for c in range(3))

    def wait_all(ref, sem):
        others = ref.at[pl.ds(0, devices - 1)]
        pltpu.make_async_copy(others, others, sem).wait()

    def settle(scale):
        acc_ref[...] = acc_ref[...] + (scale * first_col) * near_ref[...]

    rrecv[mine] = jnp.zeros((1, 128), f32)
    energies, scales = [], []
    for t in range(SWEEPS):
        last, slot = t == SWEEPS - 1, t % 2
        depth = jnp.where(live_rows, jnp.maximum(-gap[...], 0.0), 0.0)
        erecv[t, mine] = lanes_sum(depth * depth)
        to_all(erecv.at[t, mine], es_sem.at[slot], er_sem.at[slot])
        own = scatter([depth * geo[c, base : base + blocks] for c in range(3)])
        parts = cat(split(cat(own, 1), 2))
        if not t:
            wait_each(lrecv, ds_sem.at[1])
        if not last:
            far = apply(0, base, parts)
            respond(t + 1, lambda row, n: dots(row, n, [m[row : row + n] for m in far]))
        moved = apply(base, blocks if last else 2 * blocks, parts)
        near = cat([m[:blocks] for m in moved], 1)
        resid = jnp.sum(lanes_sum(near * near * first_col), axis=1, keepdims=True)
        rrecv[mine] = jnp.where(lane == t, resid, rrecv[mine])
        if last:
            to_all(rrecv.at[mine], es_sem.at[2], er_sem.at[2])
        if t:
            wait_all(erecv.at[t - 1], es_sem.at[1 - slot])
            responded(t)
            settle(scales[-1])
        else:
            wait_each(reqs, ds_sem.at[0])
        near_ref[...] = near
        if last:
            for c in range(3):
                cut = slice(c * bz, (c + 1) * bz)
                done = placed(acc_ref[:, cut])
                out_ref[c] = pos_ref[c] + done.reshape(bx, by, bz)
                step_ref[c] = placed(first_col * near[:, cut]).reshape(bx, by, bz)
        else:
            step = dots(base, 2 * blocks, moved)
            step = step[:blocks] + step[blocks:]
            more = received(t + 1)
        wait_all(erecv.at[t], er_sem.at[slot])
        energy = jnp.sum(jnp.sum(erecv[t], axis=0), axis=1, keepdims=True)
        scale = 1.0 / (1.0 + energy / (blocks * pairs * devices))
        energies.append(energy)
        scales.append(scale)
        if last:
            for c in range(3):
                out_ref[c] = out_ref[c] + scale[:, :, None] * step_ref[c]
        else:
            gap[0:outer, :] = gap[0:outer, :] + scale * step[:outer]
            gap[pl.ds(outer, outer), :] = gap[pl.ds(outer, outer), :] + scale * (
                step[outer:] + more
            )

    wait_all(erecv.at[SWEEPS - 1], es_sem.at[(SWEEPS - 1) % 2])
    energy, scale = jnp.zeros((1, 128), f32), jnp.zeros((1, 128), f32)
    for t in range(SWEEPS):
        energy = jnp.where(lane == t, energies[t], energy)
        scale = jnp.where(lane == t, scales[t], scale)
    hist_out[0:1, :] = jnp.sqrt(1.0 + energy / (blocks * pairs))[:, :SWEEPS]
    factor = scale * scale / (bx * by * bz)
    wait_all(rrecv, er_sem.at[2])
    resid = factor * jnp.sum(rrecv[...], axis=0)
    hist_out[1:2, :] = jnp.sqrt(1.0 + resid)[:, :SWEEPS]
    wait_all(rrecv, es_sem.at[2])


def finish(pos_ref, hist_ref, pos_out, hist_out, sem):
    copies = [
        pltpu.make_async_copy(pos_ref, pos_out, sem.at[0]),
        pltpu.make_async_copy(hist_ref, hist_out, sem.at[1]),
    ]
    for copy in copies:
        copy.start()
    for copy in copies:
        copy.wait()


def local(sizes, positions, pair_node, pair_line, pair_far, far_line, pair_geom, live_blocks):
    blocks, pairs = pair_node.shape[3:]
    blk = positions.shape[1:]
    devices = sizes[0] * sizes[1] * sizes[2]
    outer = blocks // 2
    rows = 2 * blocks + 6 * outer
    group = -(-3 * (blk[2] // 128) // 8) * 8
    dma = pltpu.SemaphoreType.DMA
    vmem = pl.BlockSpec(memory_space=pltpu.VMEM)
    hbm = functools.partial(pltpu.with_memory_space_constraint, memory_space=pltpu.HBM)
    moved, hist = pl.pallas_call(
        functools.partial(kernel, sizes, blk),
        out_shape=(
            pltpu.VMEM(positions.shape, f32),
            pltpu.VMEM((2, SWEEPS), f32),
        ),
        in_specs=[pl.BlockSpec(memory_space=pltpu.SMEM)]
        + [pl.BlockSpec(memory_space=pltpu.HBM)] * 3
        + [vmem]
        + [pl.BlockSpec(memory_space=pltpu.HBM)] * 2,
        out_specs=(vmem, vmem),
        scratch_shapes=[
            pltpu.VMEM(pair_node.shape, jnp.int32),
            pltpu.VMEM(pair_line.shape, jnp.int32),
            pltpu.VMEM(pair_far.shape, jnp.int32),
            pltpu.VMEM(pair_geom.shape, f32),
            pltpu.VMEM(positions.shape, f32),
            pltpu.VMEM((blocks, 3 * blk[2]), f32),
            pltpu.VMEM((blocks, 3 * blk[2]), f32),
            pltpu.VMEM(positions.shape, f32),
            pltpu.VMEM((3, 3, blk[0] * blk[1], blk[2]), bf16),
            pltpu.VMEM((outer, 128), f32),
            pltpu.VMEM((6, outer, 128), f32),
            pltpu.VMEM((6, 3, outer, blk[2]), f32),
            pltpu.VMEM((6, 3, outer, blk[2]), f32),
            pltpu.VMEM((4 * (pairs // 128), outer, 128), f32),
            pltpu.VMEM((2, blocks, pairs), f32),
            pltpu.VMEM((blocks * pairs, 128), bf16),
            pltpu.VMEM((1, 2 * blocks), f32),
            pltpu.VMEM((rows, 2 * blocks), bf16),
            pltpu.VMEM((rows, pairs), f32),
            pltpu.VMEM((3, rows, pairs), f32),
            pltpu.VMEM((rows, pairs), jnp.int32),
            pltpu.VMEM((rows, pairs), jnp.int32),
            pltpu.VMEM((blocks, pairs), f32),
            pltpu.VMEM((pairs // 128, blocks * group, 128), f32),
            pltpu.VMEM((blocks * group, 128), f32),
            pltpu.VMEM((6, 4 * (pairs // 128), outer, 128), f32),
            pltpu.VMEM((SWEEPS, 6, outer, pairs), f32),
            pltpu.VMEM((SWEEPS, 6, outer, pairs), f32),
            pltpu.VMEM((SWEEPS, devices, 1, 128), f32),
            pltpu.VMEM((devices, 1, 128), f32),
            pltpu.SemaphoreType.REGULAR((len(near_radii(sizes)),)),
            pltpu.SemaphoreType.REGULAR,
            dma((3,)),
            dma((3,)),
            dma((3,)),
            dma((3,)),
        ],
        compiler_params=pltpu.CompilerParams(
            collective_id=0, has_side_effects=True, vmem_limit_bytes=40 << 20
        ),
    )(
        live_blocks,
        hbm(pair_node),
        hbm(pair_line),
        hbm(pair_far),
        pltpu.with_memory_space_constraint(far_line, pltpu.VMEM),
        hbm(pair_geom),
        hbm(positions),
    )
    return pl.pallas_call(
        finish,
        out_shape=(
            jax.ShapeDtypeStruct(positions.shape, f32),
            jax.ShapeDtypeStruct((2, SWEEPS), f32),
        ),
        in_specs=[vmem] * 2,
        out_specs=[pl.BlockSpec(memory_space=pl.ANY)] * 2,
        scratch_shapes=[dma((2,))],
        compiler_params=pltpu.CompilerParams(vmem_limit_bytes=1 << 20),
    )(moved, hist)


def solution(mesh):
    sizes = tuple(mesh.shape[a] for a in AXES)
    return jax.shard_map(
        functools.partial(local, sizes),
        mesh=mesh,
        in_specs=(
            P(None, "gx", "gy", "gz"),
            P("gx", "gy", "gz", None, None),
            P("gx", "gy", "gz", None),
            P("gx", "gy", "gz", None, None),
            P("gx", "gy", "gz", None),
            P("gx", "gy", "gz", None, None, None),
            P("gx", "gy", "gz"),
        ),
        out_specs=(P(None, "gx", "gy", "gz"), P()),
        check_vma=False,
    )
```

```python
import functools
import itertools

import jax
import jax.numpy as jnp
from jax import lax
from jax.experimental import pallas as pl
from jax.experimental.pallas import tpu as pltpu
from jax.sharding import PartitionSpec as P

RIM = 3
SWEEPS = 5
RELAX = 0.9
AXES = ("gx", "gy", "gz")
MESH = pl.DeviceIdType.MESH
f32 = jnp.float32
bf16 = jnp.bfloat16


def split(x, parts):
    out = []
    for _ in range(parts - 1):
        hi = x.astype(bf16)
        out.append(hi)
        x = x - hi.astype(f32)
    out.append(x.astype(bf16))
    return out


def mm(a, b):
    return jnp.dot(a, b, preferred_element_type=f32)


def near_radii(sizes):
    need = max(sizes[0] - 1, sizes[1] + sizes[2] - 2)
    radii = [1]
    while 2 * radii[-1] < need:
        radii.append(2 * radii[-1])
    return radii


def take_lanes(xs, low, half):
    outs = [[] for _ in xs]
    for h in range(0, low.shape[1], 128):
        idx = low[:, h : h + 128]
        got = [None] * len(xs)
        for j in range(xs[0].shape[1] // 128):
            for i, x in enumerate(xs):
                more = jnp.take_along_axis(
                    x[:, 128 * j : 128 * (j + 1)], idx, axis=1, mode="promise_in_bounds"
                )
                got[i] = jnp.where(half[:, h : h + 128] == j, more, got[i]) if j else more
        for out, x in zip(outs, got):
            out.append(x)
    return [jnp.concatenate(out, axis=1) for out in outs]


def kernel(
    sizes,
    blk,
    live_ref,
    node_hbm,
    line_hbm,
    farpos_hbm,
    farline_ref,
    geom_hbm,
    pos_hbm,
    out_ref,
    hist_out,
    node_ref,
    line_ref,
    farpos_ref,
    geom_ref,
    pos_ref,
    acc_ref,
    near_ref,
    step_ref,
    pos3,
    code,
    codes,
    lsend,
    lrecv,
    req,
    cols,
    hot,
    two,
    amat,
    cinv,
    geo,
    low_ref,
    half_ref,
    gap,
    terms,
    sums,
    reqs,
    dsend,
    drecv,
    erecv,
    rrecv,
    near_sem,
    whole_sem,
    ds_sem,
    dr_sem,
    es_sem,
    er_sem,
):
    nx, ny, nz = sizes
    bx, by, bz = blk
    devices = nx * ny * nz
    blocks, pairs = gap.shape
    outer = blocks // 2
    lines = bx * by
    me = [lax.axis_index(a) for a in AXES]
    mine = (me[0] * ny + me[1]) * nz + me[2]
    dirs = [(a, s) for a in (1, 0, 2) for s in (1, -1)]

    def neighbour(axis, sign):
        to = list(me)
        to[axis] = lax.rem(me[axis] + sign + sizes[axis], sizes[axis])
        return tuple(to)

    def exists(axis, sign):
        return (me[axis] + sign >= 0) & (me[axis] + sign < sizes[axis])

    def coords(k):
        to = lax.rem(mine + k, devices)
        return (to // (ny * nz), lax.rem(to // nz, ny), lax.rem(to, nz))

    def moved_by(axis, k):
        if sizes[axis] & (sizes[axis] - 1) == 0:
            return lax.bitwise_xor(me[axis], k)
        to = me[axis] + k
        return jnp.where(to >= sizes[axis], to - sizes[axis], to)

    ids = [[moved_by(a, k) for k in range(sizes[a])] for a in range(3)]

    def sphere(r):
        steps = itertools.product(*[range(1 - n, n) for n in sizes])
        steps = [s for s in steps if sum(abs(x) for x in s) == r]
        return sorted(steps, key=lambda s: -abs(s[1]))

    def inside(step):
        ok = True
        for x, n, at in zip(step, sizes, me):
            if x > 0:
                ok = ok & (at < n - x)
            if x < 0:
                ok = ok & (at >= -x)
        return ok

    def signal_sphere(sem, r):
        for step in sphere(r):

            @pl.when(inside(step))
            def _():
                to = tuple(at + x for at, x in zip(me, step))
                pl.semaphore_signal(sem, inc=1, device_id=to, device_id_type=MESH)

    def wait_sphere(sem, r):
        pl.semaphore_wait(sem, sum(jnp.where(inside(s), 1, 0) for s in sphere(r)))

    radii = near_radii(sizes)
    barrier = pltpu.get_barrier_semaphore()
    signal_sphere(barrier, 1)
    inputs = [
        pltpu.make_async_copy(*copy)
        for copy in [
            (farpos_hbm, farpos_ref, ds_sem.at[0]),
            (geom_hbm, geom_ref, es_sem.at[0]),
            (node_hbm, node_ref, es_sem.at[1]),
            (line_hbm, line_ref, es_sem.at[2]),
            (pos_hbm, pos_ref, ds_sem.at[2]),
        ]
    ]
    for copy in inputs:
        copy.start()
    def column(ref):
        row = ref[0, 0].astype(f32)
        return jnp.transpose(jnp.broadcast_to(row, (pairs, blocks)))

    cols[1] = column(farline_ref)
    code[...] = cols[1, outer:, :128]

    def remote(src, dst, send_sem, recv_sem, to):
        return pltpu.make_async_remote_copy(
            src_ref=src,
            dst_ref=dst,
            send_sem=send_sem,
            recv_sem=recv_sem,
            device_id=neighbour(*to),
            device_id_type=MESH,
        )

    def ask_line(d, axis, sign):
        return remote(code, codes.at[d], ds_sem.at[1], dr_sem.at[1], (axis, sign))

    def ask_pairs(d, axis, sign):
        return remote(req, reqs.at[d], ds_sem.at[0], dr_sem.at[2], (axis, sign))

    def line_back(d, axis, sign):
        return remote(lsend.at[d], lrecv.at[d], ds_sem.at[1], dr_sem.at[0], (axis, -sign))

    def answer(t, d, axis, sign):
        sems = ds_sem.at[t % 2], dr_sem.at[t % 2]
        return remote(dsend.at[t, d], drecv.at[t, d], *sems, (axis, -sign))

    count = sum(jnp.where(exists(axis, sign), 1, 0) for axis, sign in dirs)

    def wait_each(ref, sem):
        for k in range(1, len(dirs) + 1):

            @pl.when(count == k)
            def _():
                some = ref.at[pl.ds(0, k)]
                pltpu.make_async_copy(some, some, sem).wait()

    def first_side(side):
        odd = lax.rem(me[1], 2) == 1
        return odd if side > 0 else jnp.logical_not(odd)

    def start_two(copy, way):
        for first in (True, False):
            for d in range(2):
                axis, sign = dirs[d]
                turn = first_side(way * sign)
                turn = turn if first else jnp.logical_not(turn)

                @pl.when(exists(axis, way * sign) & turn)
                def _():
                    copy(d, axis, sign).start()

    def start_rest(copy, way, d):
        axis, sign = dirs[d]

        @pl.when(exists(axis, way * sign))
        def _():
            copy(d, axis, sign).start()

    wait_sphere(barrier, 1)
    start_two(ask_line, 1)
    for d in range(2, len(dirs)):
        start_rest(ask_line, 1, d)
    for copy in inputs[:2]:
        copy.wait()
    wide = pairs // 128
    planes = [geom_ref[0, 0, 0, outer:, c, :] for c in range(3)]
    planes.append(farpos_ref[0, 0, 0, outer:, :].astype(f32))
    for c in range(4):
        for h in range(wide):
            req[c * wide + h] = planes[c][:, 128 * h : 128 * (h + 1)]
    start_two(ask_pairs, 1)
    for d in range(2, len(dirs)):
        start_rest(ask_pairs, 1, d)

    signal_sphere(near_sem.at[0], radii[0])
    for copy in inputs[2:4]:
        copy.wait()
    cols[0] = column(line_ref)

    for d, (axis, sign) in enumerate(dirs):

        @pl.when(jnp.logical_not(exists(axis, -sign)))
        def _():
            codes[d] = jnp.zeros(code.shape, f32)
            reqs[d] = jnp.zeros(req.shape, f32)

        @pl.when(jnp.logical_not(exists(axis, sign)))
        def _():
            lrecv[d] = jnp.zeros((3, outer, bz), f32)
            for t in range(1, SWEEPS):
                drecv[t, d] = jnp.zeros((outer, pairs), f32)

    def at_lanes(z):
        z = z.astype(jnp.int32)
        return lax.bitwise_and(z, 127), lax.shift_right_arithmetic(z, 7)

    live_rows = lax.broadcasted_iota(jnp.int32, (blocks, pairs), 0) < live_ref[0, 0, 0]
    node_low, node_half = at_lanes(node_ref[0, 0, 0])
    lane_node = lax.broadcasted_iota(jnp.int32, (pairs, 128), 1).astype(f32)
    node_t = jnp.transpose(node_low.astype(f32))
    group = terms.shape[1] // blocks
    terms[...] = jnp.zeros_like(terms)

    def mark(slots):
        for b in slots:
            hot[pl.ds(b * pairs, pairs), :] = jnp.where(
                node_t[:, b : b + 1] == lane_node, 1.0, 0.0
            ).astype(bf16)

    mark(range(outer))
    wait_sphere(near_sem.at[0], radii[0])
    if len(radii) > 1:
        signal_sphere(near_sem.at[1], radii[1])
    inputs[4].wait()
    for c in range(3):
        for k, part in enumerate(split(pos_ref[c].reshape(lines, bz), 3)):
            pos3[c, k] = part
    row_line = line_ref[0, 0].astype(f32)
    two[...] = jnp.concatenate([row_line, row_line], axis=1)
    row_mod = lax.broadcasted_iota(jnp.int32, (blocks, blocks), 0)
    col_mod = lax.broadcasted_iota(jnp.int32, (blocks, blocks), 1)
    line_b = cols[0]
    same = line_b[:, :blocks] == row_line
    first_col = 1.0 - jnp.max(
        jnp.where(same & (col_mod < row_mod), 1.0, 0.0), axis=1, keepdims=True
    )

    def cat(parts, axis=0):
        return jnp.concatenate(parts, axis=axis)

    def scatter(values, then=None):
        n = len(values)
        for h in range(bz // 128):
            for c in range(n):
                x = jnp.where(node_half == h, values[c], 0.0)
                for j in range(wide):
                    cut = x[:, 128 * j : 128 * (j + 1)]
                    terms[j, pl.ds(h * n + c, blocks, stride=group), :] = cut
        if then is not None:
            then()
        for b in range(blocks):
            slot = cat([terms[j, pl.ds(b * group, group), :] for j in range(wide)], 1)
            both = cat(split(slot, 2))
            both = mm(both, hot[pl.ds(b * pairs, pairs), :])
            sums[pl.ds(b * group, group), :] = both[:group] + both[group:]
        return [
            cat([sums[pl.ds(h * n + c, blocks, stride=group), :] for h in range(bz // 128)], 1)
            for c in range(n)
        ]

    def located(code, zpos, shift):
        e = jnp.floor((code + 0.5) / (by + 2 * RIM))
        f = code - e * (by + 2 * RIM)
        e = e - (RIM + shift[0] * bx)
        f = f - (RIM + shift[1] * by)
        z = zpos - (RIM + shift[2] * bz)
        ok_line = (e >= 0) & (e < bx) & (f >= 0) & (f < by)
        return jnp.where(ok_line, e * by + f, -1.0), z, ok_line & (z >= 0) & (z < bz)

    def setup(row, line, node, geom):
        n = line.shape[0]
        a = jnp.where(line[:, : 2 * blocks] == two[...], 1.0, 0.0).astype(bf16)
        amat[pl.ds(row, n), :] = a
        cinv[pl.ds(row, n), :] = RELAX / (1.0 + mm(a[:, :blocks], counts))
        low, half = at_lanes(node)
        low_ref[pl.ds(row, n), :] = low
        half_ref[pl.ds(row, n), :] = half
        for c in range(3):
            geo[c, pl.ds(row, n), :] = geom[c]

    def fetch(line):
        lane_line = lax.broadcasted_iota(jnp.int32, (line.shape[0], lines), 1).astype(f32)
        own = jnp.where(line == lane_line, 1.0, 0.0).astype(bf16)
        return [sum(mm(own, pos3[c, k]) for k in range(3)) for c in range(3)]

    base = len(dirs) * outer
    rows = base + 2 * blocks
    node = node_ref[0, 0, 0].astype(f32)
    far = farpos_ref[0, 0, 0].astype(f32)
    geom = [geom_ref[0, 0, 0, :, c, :] for c in range(4)]
    wait_each(codes, dr_sem.at[1])
    shifts = []
    for axis, sign in dirs:
        shifts.append([sign if a == axis else 0 for a in range(3)])
    asked = []
    for d in range(len(dirs)):
        there = jnp.concatenate([codes[d]] * wide, axis=1)
        asked.append(located(there, 0.0, shifts[d])[0])
    back = fetch(cat(asked))
    for d in range(len(dirs)):
        for c in range(3):
            lsend[d, c] = back[c][d * outer : (d + 1) * outer]
    wait_each(codes, ds_sem.at[1])
    start_two(line_back, -1)
    for d in range(2, len(dirs)):
        start_rest(line_back, -1, d)

    for i, r in enumerate(radii[1:], 1):
        wait_sphere(near_sem.at[i], r)
        if i + 1 < len(radii):
            signal_sphere(near_sem.at[i + 1], radii[i + 1])
    for k in range(1, nx):
        to = (ids[0][k], me[1], me[2])
        pl.semaphore_signal(whole_sem, inc=1, device_id=to, device_id_type=MESH)

    mark(range(outer, blocks))
    ones = jnp.where(live_rows, 1.0, 0.0)
    counts = scatter([ones, jnp.zeros_like(ones), jnp.zeros_like(ones)])[0].astype(bf16)
    line, z, ok = located(cols[1], far, (0, 0, 0))
    setup(
        base,
        cat([line_b, line]),
        cat([node, jnp.where(ok, z, 0.0)]),
        [cat([geom[c], jnp.where(ok, -geom[c], 0.0)]) for c in range(3)],
    )
    vals = fetch(cat([line_b, line]))
    start = take_lanes([v[:blocks] for v in vals], *at_lanes(node))
    inner = take_lanes([v[blocks : blocks + outer] for v in vals], *at_lanes(z[:outer]))
    gap[...] = sum(geom[c] * start[c] for c in range(3)) - geom[3]
    gap[0:outer, :] = gap[0:outer, :] - sum(geom[c][:outer] * inner[c] for c in range(3))

    wait_each(reqs, dr_sem.at[2])
    pairs_in = []
    for d in range(len(dirs)):
        got = [
            jnp.concatenate([reqs[d, c * wide + h] for h in range(wide)], axis=1) for c in range(4)
        ]
        there = jnp.concatenate([codes[d]] * wide, axis=1)
        _, at, ok = located(there, got[3], shifts[d])
        pairs_in.append([jnp.where(ok, at, 0.0)] + [jnp.where(ok, -got[c], 0.0) for c in range(3)])
    pairs_in = [cat([x[i] for x in pairs_in]) for i in range(4)]
    setup(0, cat(asked), pairs_in[0], pairs_in[1:])

    wait_each(lrecv, dr_sem.at[0])
    low, half = at_lanes(far[outer:] - RIM)
    reach = []
    for c in range(3):
        line = vals[c][blocks + outer :]
        for d, (axis, sign) in enumerate(dirs):
            if axis < 2:
                line = line + lrecv[d, c]
        below = lrecv[dirs.index((2, -1)), c][:, bz - 128 :]
        above = lrecv[dirs.index((2, 1)), c][:, :128]
        reach.append(jnp.concatenate([below, line, above], axis=1))
    reach = take_lanes(reach, low, half + 1)
    if nx > 1:
        pl.semaphore_wait(whole_sem, nx - 1)
    gap[pl.ds(outer, outer), :] = gap[pl.ds(outer, outer), :] - sum(
        geom[c][outer:] * reach[c] for c in range(3)
    )
    def respond(t, total):
        send = functools.partial(answer, t)
        for d in range(len(dirs)):
            dsend[t, d] = total(d * outer, outer)
            if d == 1:
                start_two(send, -1)
            if d > 1:
                start_rest(send, -1, d)

    def responded(t):
        wait_each(dsend.at[t], ds_sem.at[t % 2])

    def received(t):
        wait_each(drecv.at[t], dr_sem.at[t % 2])
        got = drecv[t, 0]
        for d in range(1, len(dirs)):
            got = got + drecv[t, d]
        return got

    acc_ref[...] = jnp.zeros_like(acc_ref)

    def to_all(ref, send_sem, recv_sem):
        def send(to):
            pltpu.make_async_remote_copy(
                src_ref=ref,
                dst_ref=ref,
                send_sem=send_sem,
                recv_sem=recv_sem,
                device_id=to,
                device_id_type=MESH,
            ).start()

        if devices <= 32:
            for a in reversed(range(nx)):
                for b in reversed(range(ny)):
                    for c in range(nz):
                        if a or b or c:
                            send((ids[0][a], ids[1][b], ids[2][c]))
        else:

            def step(k, carry):
                send(coords(k))
                return carry

            lax.fori_loop(1, devices, step, 0)

    def lanes_sum(x):
        x = jnp.sum(x, axis=0, keepdims=True)
        out = x[:, :128]
        for j in range(1, x.shape[1] // 128):
            out = out + x[:, 128 * j : 128 * (j + 1)]
        return out

    lane = lax.broadcasted_iota(jnp.int32, (1, 128), 1)
    at_line = lax.broadcasted_iota(jnp.int32, (lines, 2 * blocks), 0).astype(f32)
    place = jnp.where(at_line == two[...], 1.0, 0.0).astype(bf16)

    def placed(x):
        return mm(place, cat(split(x, 2)))

    def apply(row, n, parts):
        both = mm(amat[row : row + n, :], parts)
        return [both[:, c * bz : (c + 1) * bz] * cinv[row : row + n, :] for c in range(3)]

    def dots(row, n, moved):
        low = low_ref[row : row + n, :]
        half = half_ref[row : row + n, :]
        got = take_lanes(moved, low, half)
        return sum(geo[c, row : row + n] * got[c] for c in range(3))

    def wait_all(ref, sem):
        others = ref.at[pl.ds(0, devices - 1)]
        pltpu.make_async_copy(others, others, sem).wait()

    def settle(scale):
        acc_ref[...] = acc_ref[...] + (scale * first_col) * near_ref[...]

    rrecv[mine] = jnp.zeros((1, 128), f32)
    energies, scales = [], []
    for t in range(SWEEPS):
        last, slot = t == SWEEPS - 1, t % 2
        depth = jnp.where(live_rows, jnp.maximum(-gap[...], 0.0), 0.0)
        erecv[t, mine] = lanes_sum(depth * depth)
        send = functools.partial(to_all, erecv.at[t, mine], es_sem.at[slot], er_sem.at[slot])
        if not last:
            send()
        own = scatter(
            [depth * geo[c, base : base + blocks] for c in range(3)], send if last else None
        )
        parts = cat(split(cat(own, 1), 2))
        if not t:
            wait_each(lrecv, ds_sem.at[1])
        if not last:
            far = apply(0, base, parts)
            respond(t + 1, lambda row, n: dots(row, n, [m[row : row + n] for m in far]))
        moved = apply(base, blocks if last else 2 * blocks, parts)
        near = cat([m[:blocks] for m in moved], 1)
        resid = jnp.sum(lanes_sum(near * near * first_col), axis=1, keepdims=True)
        rrecv[mine] = jnp.where(lane == t, resid, rrecv[mine])
        if last:
            to_all(rrecv.at[mine], es_sem.at[2], er_sem.at[2])
        if t:
            wait_all(erecv.at[t - 1], es_sem.at[1 - slot])
            responded(t)
            settle(scales[-1])
        else:
            wait_each(reqs, ds_sem.at[0])
        near_ref[...] = near
        if last:
            for c in range(3):
                cut = slice(c * bz, (c + 1) * bz)
                done = placed(acc_ref[:, cut])
                out_ref[c] = pos_ref[c] + done.reshape(bx, by, bz)
                step_ref[c] = placed(first_col * near[:, cut]).reshape(bx, by, bz)
        else:
            step = dots(base, 2 * blocks, moved)
            step = step[:blocks] + step[blocks:]
            more = received(t + 1)
        wait_all(erecv.at[t], er_sem.at[slot])
        energy = jnp.sum(jnp.sum(erecv[t], axis=0), axis=1, keepdims=True)
        scale = 1.0 / (1.0 + energy / (blocks * pairs * devices))
        energies.append(energy)
        scales.append(scale)
        if last:
            for c in range(3):
                out_ref[c] = out_ref[c] + scale[:, :, None] * step_ref[c]
        else:
            gap[0:outer, :] = gap[0:outer, :] + scale * step[:outer]
            gap[pl.ds(outer, outer), :] = gap[pl.ds(outer, outer), :] + scale * (
                step[outer:] + more
            )

    wait_all(erecv.at[SWEEPS - 1], es_sem.at[(SWEEPS - 1) % 2])
    energy, scale = jnp.zeros((1, 128), f32), jnp.zeros((1, 128), f32)
    for t in range(SWEEPS):
        energy = jnp.where(lane == t, energies[t], energy)
        scale = jnp.where(lane == t, scales[t], scale)
    hist_out[0:1, :] = jnp.sqrt(1.0 + energy / (blocks * pairs))[:, :SWEEPS]
    factor = scale * scale / (bx * by * bz)
    wait_all(rrecv, er_sem.at[2])
    resid = factor * jnp.sum(rrecv[...], axis=0)
    hist_out[1:2, :] = jnp.sqrt(1.0 + resid)[:, :SWEEPS]
    wait_all(rrecv, es_sem.at[2])


def finish(pos_ref, hist_ref, pos_out, hist_out, sem):
    copies = [
        pltpu.make_async_copy(pos_ref, pos_out, sem.at[0]),
        pltpu.make_async_copy(hist_ref, hist_out, sem.at[1]),
    ]
    for copy in copies:
        copy.start()
    for copy in copies:
        copy.wait()


def local(sizes, positions, pair_node, pair_line, pair_far, far_line, pair_geom, live_blocks):
    blocks, pairs = pair_node.shape[3:]
    blk = positions.shape[1:]
    devices = sizes[0] * sizes[1] * sizes[2]
    outer = blocks // 2
    rows = 2 * blocks + 6 * outer
    group = -(-3 * (blk[2] // 128) // 8) * 8
    dma = pltpu.SemaphoreType.DMA
    vmem = pl.BlockSpec(memory_space=pltpu.VMEM)
    hbm = functools.partial(pltpu.with_memory_space_constraint, memory_space=pltpu.HBM)
    moved, hist = pl.pallas_call(
        functools.partial(kernel, sizes, blk),
        out_shape=(
            pltpu.VMEM(positions.shape, f32),
            pltpu.VMEM((2, SWEEPS), f32),
        ),
        in_specs=[pl.BlockSpec(memory_space=pltpu.SMEM)]
        + [pl.BlockSpec(memory_space=pltpu.HBM)] * 3
        + [vmem]
        + [pl.BlockSpec(memory_space=pltpu.HBM)] * 2,
        out_specs=(vmem, vmem),
        scratch_shapes=[
            pltpu.VMEM(pair_node.shape, jnp.int32),
            pltpu.VMEM(pair_line.shape, jnp.int32),
            pltpu.VMEM(pair_far.shape, jnp.int32),
            pltpu.VMEM(pair_geom.shape, f32),
            pltpu.VMEM(positions.shape, f32),
            pltpu.VMEM((blocks, 3 * blk[2]), f32),
            pltpu.VMEM((blocks, 3 * blk[2]), f32),
            pltpu.VMEM(positions.shape, f32),
            pltpu.VMEM((3, 3, blk[0] * blk[1], blk[2]), bf16),
            pltpu.VMEM((outer, 128), f32),
            pltpu.VMEM((6, outer, 128), f32),
            pltpu.VMEM((6, 3, outer, blk[2]), f32),
            pltpu.VMEM((6, 3, outer, blk[2]), f32),
            pltpu.VMEM((4 * (pairs // 128), outer, 128), f32),
            pltpu.VMEM((2, blocks, pairs), f32),
            pltpu.VMEM((blocks * pairs, 128), bf16),
            pltpu.VMEM((1, 2 * blocks), f32),
            pltpu.VMEM((rows, 2 * blocks), bf16),
            pltpu.VMEM((rows, pairs), f32),
            pltpu.VMEM((3, rows, pairs), f32),
            pltpu.VMEM((rows, pairs), jnp.int32),
            pltpu.VMEM((rows, pairs), jnp.int32),
            pltpu.VMEM((blocks, pairs), f32),
            pltpu.VMEM((pairs // 128, blocks * group, 128), f32),
            pltpu.VMEM((blocks * group, 128), f32),
            pltpu.VMEM((6, 4 * (pairs // 128), outer, 128), f32),
            pltpu.VMEM((SWEEPS, 6, outer, pairs), f32),
            pltpu.VMEM((SWEEPS, 6, outer, pairs), f32),
            pltpu.VMEM((SWEEPS, devices, 1, 128), f32),
            pltpu.VMEM((devices, 1, 128), f32),
            pltpu.SemaphoreType.REGULAR((len(near_radii(sizes)),)),
            pltpu.SemaphoreType.REGULAR,
            dma((3,)),
            dma((3,)),
            dma((3,)),
            dma((3,)),
        ],
        compiler_params=pltpu.CompilerParams(
            collective_id=0, has_side_effects=True, vmem_limit_bytes=40 << 20
        ),
    )(
        live_blocks,
        hbm(pair_node),
        hbm(pair_line),
        hbm(pair_far),
        pltpu.with_memory_space_constraint(far_line, pltpu.VMEM),
        hbm(pair_geom),
        hbm(positions),
    )
    return pl.pallas_call(
        finish,
        out_shape=(
            jax.ShapeDtypeStruct(positions.shape, f32),
            jax.ShapeDtypeStruct((2, SWEEPS), f32),
        ),
        in_specs=[vmem] * 2,
        out_specs=[pl.BlockSpec(memory_space=pl.ANY)] * 2,
        scratch_shapes=[dma((2,))],
        compiler_params=pltpu.CompilerParams(vmem_limit_bytes=1 << 20),
    )(moved, hist)


def solution(mesh):
    sizes = tuple(mesh.shape[a] for a in AXES)
    return jax.shard_map(
        functools.partial(local, sizes),
        mesh=mesh,
        in_specs=(
            P(None, "gx", "gy", "gz"),
            P("gx", "gy", "gz", None, None),
            P("gx", "gy", "gz", None),
            P("gx", "gy", "gz", None, None),
            P("gx", "gy", "gz", None),
            P("gx", "gy", "gz", None, None, None),
            P("gx", "gy", "gz"),
        ),
        out_specs=(P(None, "gx", "gy", "gz"), P()),
        check_vma=False,
    )
```
